8 devices in a mesh: dp: 1 (over z), col: 2 (over y), row: 4 (over x, core).
Axes of the slice: x: 2, y: 2, z: 1, core: 2. Of those that a mesh axis runs over, the one named last changes fastest.
Arguments:
- x_act: bfloat16 [96, 5120], P(('dp', 'row'), 'col')
- ln_gain: float32 [5120], P('col')
- w_in: bfloat16 [5120, 20480], P('row', 'col')
- w_out: bfloat16 [20480, 5120], P('row', 'col')
Outputs:
- output: bfloat16 [96, 5120], P(('dp', 'row'), 'col')
All inputs are finite; a program needn't handle non-finite values.
Results may differ from the reference program's by a relative error of at most 0.00117.
Values are sent between devices in bfloat16 or wider.
A program may use at most 1 GiB of HBM per device.

```python
import jax
import jax.numpy as jnp
from jax import lax

TOKENS = 96
D_MODEL = 5120
D_FF = 20480

NORM_EPS = 1e-5


def setup_inputs(seed: int = 0, part: int = 0) -> dict:
    key = jax.random.key(seed)
    part_key, shared_key = jax.random.split(key)
    part_key = jax.random.fold_in(part_key, part)
    key_noise, key_row, key_shift, key_scale = jax.random.split(part_key, 4)
    key_gain, key_in, key_out = jax.random.split(shared_key, 3)
    walk_norm = D_MODEL ** -0.5
    feat_shift = 0.8 * walk_norm * jnp.cumsum(jax.random.normal(key_shift, (D_MODEL,), jnp.float32))
    feat_scale = jnp.exp(0.5 * walk_norm * jnp.cumsum(jax.random.normal(key_scale, (D_MODEL,), jnp.float32)))
    row_shift = 0.5 * jax.random.normal(key_row, (TOKENS, 1), jnp.float32)
    noise = jax.random.normal(key_noise, (TOKENS, D_MODEL), jnp.float32)
    x_act = (noise * feat_scale + feat_shift + row_shift).astype(jnp.bfloat16)
    ln_gain = jax.random.uniform(key_gain, (D_MODEL,), jnp.float32, 0.5, 1.5)
    w_in = (D_MODEL ** -0.5 * jax.random.normal(key_in, (D_MODEL, D_FF), jnp.float32)).astype(jnp.bfloat16)
    w_out = (1.5 * D_FF ** -0.5 * jax.random.normal(key_out, (D_FF, D_MODEL), jnp.float32)).astype(jnp.bfloat16)
    return {"x_act": x_act, "ln_gain": ln_gain, "w_in": w_in, "w_out": w_out}


def reference(x_act, ln_gain, w_in, w_out):
    x_f32 = x_act.astype(jnp.float32)
    row_mean = jnp.mean(x_f32, axis=1, keepdims=True)
    row_var = jnp.mean(x_f32 * x_f32, axis=1, keepdims=True) - row_mean * row_mean
    z_norm = ((x_f32 - row_mean) * lax.rsqrt(row_var + NORM_EPS) * ln_gain).astype(jnp.bfloat16)
    hidden = jax.nn.gelu(jnp.dot(z_norm, w_in, preferred_element_type=jnp.float32), approximate=True).astype(jnp.bfloat16)
    branch = jnp.dot(hidden, w_out, preferred_element_type=jnp.float32)
    return (x_f32 + branch).astype(jnp.bfloat16)
```

```python
import jax
import jax.numpy as jnp
from jax import lax
from jax.experimental import pallas as pl
from jax.experimental.pallas import tpu as pltpu
from jax.sharding import PartitionSpec as P

NORM_EPS = 1e-5
MESH = pl.DeviceIdType.MESH
F32 = jnp.float32
BF16 = jnp.bfloat16

C = 256
NA = 12
NB = 8
N = NA + NB
TAIL = 5


def kernel(x_hbm, gain_hbm, w_in_hbm, w_out_hbm, out_hbm,
           x_v, gain_v, out_v, stat_s, stat_r, z_s, z_g, z_v, w_in_v, w_out_v, d_send, d_recv, own, x_recv, hall,
           acc, e_recv, f_send, f_recv,
           misc_sem, w_in_sem, w_out_sem, stat_sem, z_ssem, z_rsem, d_ssem, d_rsem, x_ssem, x_rsem, y_ssem, y_rsem,
           r_ssem, r_rsem, b_ssem, b_rsem, e_ssem, e_rsem, f_ssem, f_rsem):
    y = lax.axis_index("col")
    row = lax.axis_index("row")
    x = row // 2
    k = row % 2
    dp = lax.axis_index("dp")
    home = 1 - (x + y) % 2
    tok, half = x_v.shape
    feat = half // 2
    block = N * C
    sibling = (dp, y, 2 * x + 1 - k)
    x_next = (dp, y, 2 * (1 - x) + k)
    y_next = (dp, 1 - y, row)

    def remote(src, dst, ssem, rsem, dev):
        return pltpu.make_async_remote_copy(src_ref=src, dst_ref=dst, send_sem=ssem, recv_sem=rsem,
                                            device_id=dev, device_id_type=MESH)

    def col_b(j):
        return C * j

    def col_a(j):
        return C * (NB + j)

    def pos_col(p):
        j = p // 2
        q = p % 2
        is_b = (home + q) % 2
        return is_b * col_b(j) + (1 - is_b) * col_a(j)

    def w_in_copies(p, c):
        cs = pl.multiple_of((1 - k) * block + c, C)
        co = pl.multiple_of(k * block + c, C)
        return (pltpu.make_async_copy(w_in_hbm.at[:, pl.ds(cs, C)], w_in_v.at[p, :, pl.ds(0, C)], w_in_sem.at[p, 0]),
                pltpu.make_async_copy(w_in_hbm.at[:, pl.ds(co, C)], w_in_v.at[p, :, pl.ds(C, C)], w_in_sem.at[p, 1]))

    def w_out_copy(i):
        r = pl.multiple_of(i * C, C)
        return pltpu.make_async_copy(w_out_hbm.at[pl.ds(r, C), :], w_out_v.at[i], w_out_sem.at[i])

    x_copy = pltpu.make_async_copy(x_hbm, x_v, misc_sem.at[0])
    g_copy = pltpu.make_async_copy(gain_hbm, gain_v, misc_sem.at[1])
    x_copy.start()
    g_copy.start()

    def start_pair(p, _):
        for cp in w_in_copies(p, pos_col(p)):
            cp.start()
        return 0

    def start_rest(j, _):
        for cp in w_in_copies(NB + j, col_a(j)):
            cp.start()
        return 0

    lax.fori_loop(0, 2 * NB, start_pair, 0)
    lax.fori_loop(NB, NA, start_rest, 0)

    barrier = pltpu.get_barrier_semaphore()
    for dy in range(2):
        for dr in range(4):
            if dy or dr:
                pl.semaphore_signal(barrier, inc=1, device_id=(dp, (y + dy) % 2, (row + dr) % 4), device_id_type=MESH)

    x_copy.wait()
    g_copy.wait()
    x_f = x_v[...].astype(F32)
    s1 = jnp.sum(x_f, axis=1, keepdims=True)
    s2 = jnp.sum(x_f * x_f, axis=1, keepdims=True)
    lane = lax.broadcasted_iota(jnp.int32, (tok, 128), 1)
    stat_s[...] = jnp.where(lane < 64, s1, s2)
    pl.semaphore_wait(barrier, 7)

    stat_cp = remote(stat_s, stat_r, stat_sem.at[0], stat_sem.at[1], y_next)
    stat_cp.start()
    stat_cp.wait_recv()
    st = (stat_s[...] + stat_r[...]) * (1.0 / (2 * half))
    mean = st[:, 0:1]
    var = st[:, 64:65] - mean * mean
    z = ((x_v[...].astype(F32) - mean) * lax.rsqrt(var + NORM_EPS) * gain_v[...]).astype(BF16)
    z_s[0] = z[:, :feat]
    z_s[1] = z[:, feat:]

    for dy in range(2):
        for dk in range(2):
            ty = (y + dy) % 2
            tk = (k + dk) % 2
            cp = remote(z_s.at[tk], z_g.at[row], z_ssem.at[2 * dy + dk], z_rsem.at[row], (dp, ty, 2 * y + tk))
            if dy == 0 and dk == 0:
                @pl.when(home == 1)
                def _():
                    z_g[row] = z_s[k]

                @pl.when(home == 0)
                def _():
                    cp.start()
            else:
                cp.start()
    for sx in range(2):
        for sk in range(2):
            src = 2 * sx + sk
            cp = remote(z_s.at[0], z_g.at[src], z_ssem.at[0], z_rsem.at[src], y_next)

            @pl.when(1 - home * (1 - (src - row) * (src - row)) > 0)
            def _():
                cp.wait_recv()
    for src in range(4):
        z_v[pl.ds(tok * src, tok), :] = z_g[src]

    acc[...] = jnp.zeros_like(acc)

    def d_copy(p):
        return remote(d_send.at[p], d_recv.at[p], d_ssem.at[p], d_rsem.at[p], sibling)

    def x_copy_of(j, p):
        return remote(own.at[p], x_recv.at[j], x_ssem.at[j], x_rsem.at[j], x_next)

    def up(p, c):
        for cp in w_in_copies(p, c):
            cp.wait()
        part = jnp.dot(z_v[...], w_in_v[p], preferred_element_type=F32)
        d_send[p] = part[:, :C]
        own[p] = part[:, C:]
        d_copy(p).start()

    def pair_sum(p):
        d_copy(p).wait_recv()
        own[p] = own[p] + d_recv[p]

        @pl.when((p < 2 * NB) & (p % 2 == 0))
        def _():
            x_copy_of(p // 2, p).start()

        @pl.when((p >= 2 * NB) & (home == 0))
        def _():
            x_copy_of(p - NB, p).start()

    def up_step(p, _):
        is_pair = (p < 2 * NB).astype(jnp.int32)
        c = is_pair * pos_col(p) + (1 - is_pair) * col_a(p - NB)
        up(p, c)
        w_out_copy(p).start()

        @pl.when(p >= 2)
        def _():
            pair_sum(p - 2)
        return 0

    lax.fori_loop(0, N, up_step, 0)
    pair_sum(N - 2)
    pair_sum(N - 1)

    def y_copy(j):
        return remote(hall.at[j], hall.at[NA + j], y_ssem.at[j], y_rsem.at[j], y_next)

    def relay_copy(j):
        return remote(hall.at[NA + j], hall.at[2 * NA + j], r_ssem.at[j], r_rsem.at[j], x_next)

    def back_copy(j):
        return remote(hall.at[2 * NA + j], hall.at[2 * NA + j], b_ssem.at[j], b_rsem.at[j], y_next)

    def make_h(j):
        x_copy_of(j, 0).wait_recv()
        late = (j >= NB).astype(jnp.int32)
        p = late * (NB + j) + (1 - late) * (2 * j + 1)
        s = own[p] + x_recv[j]
        hall[j] = jax.nn.gelu(s, approximate=True).astype(BF16)
        y_copy(j).start()

    def down(slot, i):
        w_out_copy(i).wait()
        acc[...] += jnp.dot(hall[slot], w_out_v[i], preferred_element_type=F32)

    @pl.when(home == 1)
    def _():
        def relay(i):
            y_copy(i).wait_recv()
            relay_copy(i).start()

        def b_step(i, _):
            back_copy(i).wait_recv()
            down(2 * NA + i, i)
            return 0

        def a_step(j, _):
            @pl.when((j >= 2) & (j < NB + 2))
            def _():
                relay(j - 2)
            make_h(j)
            down(j, NB + j)
            return 0

        lax.fori_loop(0, 10, a_step, 0)

        def mix(m, _):
            lax.fori_loop(2 * m, 2 * m + 2, b_step, 0)
            a_step(10 + m, 0)
            return 0

        lax.fori_loop(0, 2, mix, 0)
        lax.fori_loop(4, NB, b_step, 0)

    @pl.when(home == 0)
    def _():
        def h_step(j, _):
            make_h(j)
            return 0

        def a_step(j, _):
            y_copy(j).wait_recv()
            down(NA + j, NB + j)
            return 0

        def b_step(i, _):
            relay_copy(i).wait_recv()
            back_copy(i).start()
            down(2 * NA + i, i)
            return 0

        def h_a_step(j, _):
            make_h(j + 2)
            a_step(j, 0)
            return 0

        lax.fori_loop(0, 2, h_step, 0)
        lax.fori_loop(0, 6, h_a_step, 0)

        def mix(g, _):
            a_step(6 + g, 0)
            lax.fori_loop(2 * g, 2 * g + 2, b_step, 0)
            return 0

        lax.fori_loop(0, 4, mix, 0)
        lax.fori_loop(10, NA, a_step, 0)

    width = half // TAIL

    def e_copy(t, s):
        tx = s * x + (1 - s) * (1 - x)
        r0 = pl.multiple_of(tok * (2 * tx + 1 - k), 8)
        cols = pl.ds(width * t, width)
        return remote(acc.at[pl.ds(r0, tok), cols], e_recv.at[s, :, cols], e_ssem.at[s, t], e_rsem.at[s, t], sibling)

    def f_copy(t):
        cols = pl.ds(width * t, width)
        return remote(f_send.at[:, cols], f_recv.at[:, cols], f_ssem.at[t], f_rsem.at[t], x_next)

    for t in range(TAIL):
        e_copy(t, 0).start()
    for t in range(TAIL):
        e_copy(t, 1).start()
    far = pl.multiple_of(tok * (2 * (1 - x) + k), 8)
    near = pl.multiple_of(tok * row, 8)
    for t in range(TAIL):
        cols = pl.ds(width * t, width)
        e_copy(t, 0).wait_recv()
        f_send[:, cols] = acc[pl.ds(far, tok), cols] + e_recv[0, :, cols]
        f_copy(t).start()
    for t in range(TAIL):
        cols = pl.ds(width * t, width)
        e_copy(t, 1).wait_recv()
        f_copy(t).wait_recv()
        total = acc[pl.ds(near, tok), cols] + e_recv[1, :, cols] + f_recv[:, cols]
        out_v[:, cols] = (x_v[:, cols].astype(F32) + total).astype(BF16)
    out_copy = pltpu.make_async_copy(out_v, out_hbm, misc_sem.at[2])
    out_copy.start()

    stat_cp.wait_send()
    for dy in range(2):
        for dk in range(2):
            tk = (k + dk) % 2
            cp = remote(z_s.at[tk], z_g.at[row], z_ssem.at[2 * dy + dk], z_rsem.at[row], y_next)
            if dy == 0 and dk == 0:
                @pl.when(home == 0)
                def _():
                    cp.wait_send()
            else:
                cp.wait_send()

    def drain_d(p, _):
        d_copy(p).wait_send()
        return 0

    def drain_xy(j, _):
        x_copy_of(j, 0).wait_send()
        y_copy(j).wait_send()

        @pl.when(home == 1)
        def _():
            relay_copy(j).wait_send()

        @pl.when(home == 0)
        def _():
            back_copy(j).wait_send()
        return 0

    def drain_late_x(j, _):
        @pl.when(home == 0)
        def _():
            x_copy_of(j, 0).wait_send()

        @pl.when(home == 1)
        def _():
            y_copy(j).wait_send()
        return 0

    lax.fori_loop(0, N, drain_d, 0)
    lax.fori_loop(0, NB, drain_xy, 0)
    lax.fori_loop(NB, NA, drain_late_x, 0)
    for t in range(TAIL):
        e_copy(t, 0).wait_send()
        e_copy(t, 1).wait_send()
        f_copy(t).wait_send()
    out_copy.wait()


def solution(mesh):
    def body(x_blk, gain_blk, w_in_blk, w_out_blk):
        tok, half = x_blk.shape
        feat = w_in_blk.shape[0]
        tokens = 4 * tok
        dma = pltpu.SemaphoreType.DMA
        return pl.pallas_call(
            kernel,
            out_shape=jax.ShapeDtypeStruct((tok, half), BF16),
            in_specs=[pl.BlockSpec(memory_space=pl.ANY)] * 4,
            out_specs=pl.BlockSpec(memory_space=pl.ANY),
            scratch_shapes=[
                pltpu.VMEM((tok, half), BF16),
                pltpu.VMEM((1, half), F32),
                pltpu.VMEM((tok, half), BF16),
                pltpu.VMEM((tok, 128), F32),
                pltpu.VMEM((tok, 128), F32),
                pltpu.VMEM((2, tok, feat), BF16),
                pltpu.VMEM((4, tok, feat), BF16),
                pltpu.VMEM((tokens, feat), BF16),
                pltpu.VMEM((N, feat, 2 * C), BF16),
                pltpu.VMEM((N, C, half), BF16),
                pltpu.VMEM((N, tokens, C), F32),
                pltpu.VMEM((N, tokens, C), F32),
                pltpu.VMEM((N, tokens, C), F32),
                pltpu.VMEM((NA, tokens, C), F32),
                pltpu.VMEM((2 * NA + NB, tokens, C), BF16),
                pltpu.VMEM((tokens, half), F32),
                pltpu.VMEM((2, tok, half), F32),
                pltpu.VMEM((tok, half), F32),
                pltpu.VMEM((tok, half), F32),
                dma((3,)),
                dma((N, 2)),
                dma((N,)),
                dma((2,)),
                dma((4,)),
                dma((4,)),
                dma((N,)),
                dma((N,)),
                dma((NA,)),
                dma((NA,)),
                dma((NA,)),
                dma((NA,)),
                dma((NB,)),
                dma((NB,)),
                dma((NB,)),
                dma((NB,)),
                dma((2, TAIL)),
                dma((2, TAIL)),
                dma((TAIL,)),
                dma((TAIL,)),
            ],
            compiler_params=pltpu.CompilerParams(
                collective_id=0, has_side_effects=True, vmem_limit_bytes=67_043_328
            ),
        )(x_blk, gain_blk.reshape(1, half), w_in_blk, w_out_blk)

    return jax.shard_map(
        body,
        mesh=mesh,
        in_specs=(P(("dp", "row"), "col"), P("col"), P("row", "col"), P("row", "col")),
        out_specs=P(("dp", "row"), "col"),
        check_vma=False,
    )
```

```python
import jax
import jax.numpy as jnp
from jax import lax
from jax.experimental import pallas as pl
from jax.experimental.pallas import tpu as pltpu
from jax.sharding import PartitionSpec as P

NORM_EPS = 1e-5
MESH = pl.DeviceIdType.MESH
F32 = jnp.float32
BF16 = jnp.bfloat16

C = 256
NA = 12
NB = 8
N = NA + NB
GROUP = 5
RING = 8
TAIL = 5


def kernel(x_hbm, gain_hbm, w_in_hbm, w_out_hbm, out_v,
           x_v, gain_v, stat_g, x_g, x_relay, z_v, w_in_v, w_out_v, d_send, d_recv, own, x_recv, hall,
           acc, e_recv, f_send, f_recv,
           misc_sem, w_in_sem, send_sem, d_rsem, x_rsem, y_rsem, b_rsem, e_rsem, f_rsem):
    w_out_sem, stat_rsem, z_rsem = misc_sem.at[4], misc_sem.at[5], misc_sem.at[6]
    stat_ssem, z_ssem, d_ssem, x_ssem, y_ssem, b_ssem, e_ssem, f_ssem = [send_sem.at[i] for i in range(8)]
    y = lax.axis_index("col")
    row = lax.axis_index("row")
    x = row // 2
    k = row % 2
    dp = lax.axis_index("dp")
    home = 1 - (x + y) % 2
    tok, half = x_v.shape
    feat = half // 2
    block = N * C
    sibling = (dp, y, 2 * x + 1 - k)
    x_next = (dp, y, 2 * (1 - x) + k)
    y_next = (dp, 1 - y, row)

    def remote(src, dst, ssem, rsem, dev):
        return pltpu.make_async_remote_copy(src_ref=src, dst_ref=dst, send_sem=ssem, recv_sem=rsem,
                                            device_id=dev, device_id_type=MESH)

    def col_b(j):
        return C * j

    def col_a(j):
        return C * (NB + j)

    def pos_col(p):
        j = p // 2
        q = p % 2
        is_b = (home + q) % 2
        return is_b * col_b(j) + (1 - is_b) * col_a(j)

    def w_in_copies(p, c):
        cs = pl.multiple_of((1 - k) * block + c, C)
        co = pl.multiple_of(k * block + c, C)
        return (pltpu.make_async_copy(w_in_hbm.at[:, pl.ds(cs, C)], w_in_v.at[p, :, pl.ds(0, C)], w_in_sem.at[p // GROUP]),
                pltpu.make_async_copy(w_in_hbm.at[:, pl.ds(co, C)], w_in_v.at[p, :, pl.ds(C, C)], w_in_sem.at[p // GROUP]))

    def w_out_copy(i):
        r = pl.multiple_of(i * C, C)
        return pltpu.make_async_copy(w_out_hbm.at[pl.ds(r, C), :], w_out_v.at[i], w_out_sem)

    x_copy = pltpu.make_async_copy(x_hbm, x_v, misc_sem.at[0])
    g_copy = pltpu.make_async_copy(gain_hbm, gain_v.at[0], misc_sem.at[1])
    x_copy.start()
    g_copy.start()

    def start_pair(p, _):
        for cp in w_in_copies(p, pos_col(p)):
            cp.start()
        return 0

    def start_rest(j, _):
        for cp in w_in_copies(NB + j, col_a(j)):
            cp.start()
        return 0

    lax.fori_loop(0, 2 * NB, start_pair, 0)
    lax.fori_loop(NB, NA, start_rest, 0)

    barrier = pltpu.get_barrier_semaphore()
    for dy in range(2):
        for dr in range(4):
            if dy or dr:
                pl.semaphore_signal(barrier, inc=1, device_id=(dp, (y + dy) % 2, (row + dr) % 4), device_id_type=MESH)

    x_copy.wait()
    g_copy.wait()
    x_f = x_v[...].astype(F32)
    s1 = jnp.sum(x_f, axis=1, keepdims=True)
    s2 = jnp.sum(x_f * x_f, axis=1, keepdims=True)
    lane = lax.broadcasted_iota(jnp.int32, (tok, 128), 1)
    me = 4 * y + row
    stat_g[me, :, :tok] = jnp.transpose(jnp.where(lane == 0, s1, s2))[:8]
    with jax.named_scope('barrier'):
        pl.semaphore_wait(barrier, 7)

    def tok_copy(dy, dk):
        ty = (y + dy) % 2
        tk = (k + dk) % 2
        cols = pl.ds(pl.multiple_of(feat * tk, 128), feat)
        return remote(x_v.at[:, cols], x_g.at[row], z_ssem, z_rsem, (dp, ty, 2 * y + tk))

    def stat_copy(d):
        ty = (y + d // 4) % 2
        tr = (row + d % 4) % 4
        return remote(stat_g.at[me], stat_g.at[me], stat_ssem, stat_rsem, (dp, ty, tr))

    gain_cp = remote(gain_v.at[0], gain_v.at[1], misc_sem.at[2], misc_sem.at[3], y_next)
    half_cols = pl.ds(pl.multiple_of(feat * (1 - k), 128), feat)
    to_relay = remote(x_v.at[:, half_cols], x_relay, z_ssem, misc_sem.at[7], y_next)
    from_relay = remote(x_relay, x_g.at[row], z_ssem, z_rsem, (dp, y, 2 * (1 - x) + 1 - k))

    for d in range(1, 8):
        stat_copy(d).start()

    @pl.when(home == 0)
    def _():
        to_relay.start()
        tok_copy(1, 0).start()
        tok_copy(0, 0).start()
        tok_copy(0, 1).start()

    @pl.when(home == 1)
    def _():
        gain_cp.start()
        tok_copy(0, 1).start()
        tok_copy(1, 0).start()
        tok_copy(1, 1).start()
        x_g[row] = jnp.where(k == 0, x_v[:, :feat], x_v[:, feat:])
        gain_v[1] = gain_v[0]
        with jax.named_scope('x_relay_wait'):
            to_relay.wait_recv()
        from_relay.start()

    @pl.when(home == 0)
    def _():
        with jax.named_scope('gain_wait'):
            gain_cp.wait_recv()
    gain = jnp.where(k == 0, gain_v[1, :feat], gain_v[1, feat:]).reshape(1, feat)
    acc[...] = jnp.zeros_like(acc)
    with jax.named_scope('stat_wait'):
        remote(stat_g.at[pl.ds(0, 7)], stat_g.at[pl.ds(0, 7)], stat_ssem, stat_rsem, y_next).wait_recv()

    @pl.when(home == 0)
    def _():
        with jax.named_scope('z_wait'):
            remote(x_g, x_g, z_ssem, z_rsem, y_next).wait_recv()

    @pl.when(home == 1)
    def _():
        with jax.named_scope('z_wait'):
            remote(x_g.at[pl.ds(0, 3)], x_g.at[pl.ds(0, 3)], z_ssem, z_rsem, y_next).wait_recv()
    for src in range(4):
        st = jnp.transpose(stat_g[src] + stat_g[4 + src])[:tok] * (1.0 / (2 * half))
        mean = st[:, 0:1]
        var = st[:, 1:2] - mean * mean
        z = (x_g[src].astype(F32) - mean) * lax.rsqrt(var + NORM_EPS) * gain
        z_v[pl.ds(tok * src, tok), :] = z.astype(BF16)

    def d_copy(p):
        return remote(d_send.at[p], d_recv.at[p], d_ssem, d_rsem.at[p % RING], sibling)

    def x_copy_of(j, p):
        return remote(own.at[p], x_recv.at[j], x_ssem, x_rsem.at[j], x_next)

    def up(p, c):
        @pl.when(p % GROUP == 0)
        def _():
            with jax.named_scope('w_in_wait'):
                group = w_in_v.at[pl.ds(p, GROUP)]
                pltpu.make_async_copy(group, group, w_in_sem.at[p // GROUP]).wait()

        part = jnp.dot(z_v[...], w_in_v[p], preferred_element_type=F32)
        d_send[p] = part[:, :C]
        own[p] = part[:, C:]
        d_copy(p).start()

    def pair_sum(p):
        with jax.named_scope('pair_wait'):
            d_copy(p).wait_recv()
        own[p] = own[p] + d_recv[p]

        @pl.when((p < 2 * NB) & (p % 2 == 0))
        def _():
            x_copy_of(p // 2, p).start()

        @pl.when((p >= 2 * NB) & (home == 0))
        def _():
            x_copy_of(p - NB, p).start()

    def up_step(p, _):
        is_pair = (p < 2 * NB).astype(jnp.int32)
        c = is_pair * pos_col(p) + (1 - is_pair) * col_a(p - NB)
        up(p, c)
        w_out_copy(p).start()

        @pl.when(p >= 2)
        def _():
            pair_sum(p - 2)
        return 0

    lax.fori_loop(0, N, up_step, 0)
    pair_sum(N - 2)
    pair_sum(N - 1)

    with jax.named_scope('w_out_wait'):
        pltpu.make_async_copy(w_out_v, w_out_v, w_out_sem).wait()

    def y_copy(j):
        return remote(hall.at[j], hall.at[NA + j], y_ssem, y_rsem.at[j], y_next)

    def relay_copy(j):
        return remote(hall.at[NA + j], hall.at[2 * NA + j], b_ssem, b_rsem.at[j], x_next)

    def back_copy(j):
        return remote(hall.at[2 * NA + j], hall.at[2 * NA + j], b_ssem, b_rsem.at[j], y_next)

    def make_h(j):
        with jax.named_scope('x_wait'):
            x_copy_of(j, 0).wait_recv()
        late = (j >= NB).astype(jnp.int32)
        p = late * (NB + j) + (1 - late) * (2 * j + 1)
        s = own[p] + x_recv[j]
        hall[j] = jax.nn.gelu(s, approximate=True).astype(BF16)
        y_copy(j).start()

    def down(slot, i):
        acc[...] += jnp.dot(hall[slot], w_out_v[i], preferred_element_type=F32)

    @pl.when(home == 1)
    def _():
        def relay(i):
            with jax.named_scope('relay_wait'):
                y_copy(i).wait_recv()
            relay_copy(i).start()

        def b_step(i, _):
            with jax.named_scope('b_wait'):
                back_copy(i).wait_recv()
            down(2 * NA + i, i)
            return 0

        def a_step(j, _):
            @pl.when((j >= 2) & (j < NB + 2))
            def _():
                relay(j - 2)
            make_h(j)
            down(j, NB + j)
            return 0

        lax.fori_loop(0, 10, a_step, 0)

        def mix(m, _):
            lax.fori_loop(2 * m, 2 * m + 2, b_step, 0)
            a_step(10 + m, 0)
            return 0

        lax.fori_loop(0, 2, mix, 0)
        lax.fori_loop(4, NB, b_step, 0)

    @pl.when(home == 0)
    def _():
        def h_step(j, _):
            make_h(j)
            return 0

        def a_step(j, _):
            with jax.named_scope('a_wait'):
                y_copy(j).wait_recv()
            down(NA + j, NB + j)
            return 0

        def b_step(i, _):
            with jax.named_scope('b_wait'):
                relay_copy(i).wait_recv()
            back_copy(i).start()
            down(2 * NA + i, i)
            return 0

        def h_a_step(j, _):
            make_h(j + 2)
            a_step(j, 0)
            return 0

        lax.fori_loop(0, 2, h_step, 0)
        lax.fori_loop(0, 6, h_a_step, 0)

        def mix(g, _):
            a_step(6 + g, 0)
            lax.fori_loop(2 * g, 2 * g + 2, b_step, 0)
            return 0

        lax.fori_loop(0, 4, mix, 0)
        lax.fori_loop(10, NA, a_step, 0)

    width = half // TAIL

    def e_copy(t, s):
        tx = s * x + (1 - s) * (1 - x)
        r0 = pl.multiple_of(tok * (2 * tx + 1 - k), 8)
        cols = pl.ds(width * t, width)
        return remote(acc.at[pl.ds(r0, tok), cols], e_recv.at[s, :, cols], e_ssem, e_rsem.at[s, t], sibling)

    def f_copy(t):
        cols = pl.ds(width * t, width)
        return remote(f_send.at[:, cols], f_recv.at[:, cols], f_ssem, f_rsem.at[t], x_next)

    for t in range(TAIL):
        e_copy(t, 0).start()
    for t in range(TAIL):
        e_copy(t, 1).start()
    far = pl.multiple_of(tok * (2 * (1 - x) + k), 8)
    near = pl.multiple_of(tok * row, 8)
    for t in range(TAIL):
        cols = pl.ds(width * t, width)
        with jax.named_scope('e0_wait'):
            e_copy(t, 0).wait_recv()
        f_send[:, cols] = acc[pl.ds(far, tok), cols] + e_recv[0, :, cols]
        f_copy(t).start()
    def sent(ref, sem):
        remote(ref, ref, sem, sem, y_next).wait_send()

    with jax.named_scope('drain'):
        sent(stat_g.at[pl.ds(0, 7)], stat_ssem)
        sent(x_g, z_ssem)
        sent(d_send, d_ssem)
        sent(hall.at[pl.ds(0, NB)], b_ssem)
        sent(e_recv, e_ssem)

        @pl.when(home == 0)
        def _():
            sent(own.at[pl.ds(0, NA)], x_ssem)
            sent(hall.at[pl.ds(0, NB)], y_ssem)

        @pl.when(home == 1)
        def _():
            gain_cp.wait_send()
            sent(own.at[pl.ds(0, NB)], x_ssem)
            sent(hall.at[pl.ds(0, NA)], y_ssem)

    for t in range(TAIL):
        cols = pl.ds(width * t, width)
        with jax.named_scope('e1_wait'):
            e_copy(t, 1).wait_recv()
        with jax.named_scope('f_wait'):
            f_copy(t).wait_recv()
        total = acc[pl.ds(near, tok), cols] + e_recv[1, :, cols] + f_recv[:, cols]
        out_v[:, cols] = (x_v[:, cols].astype(F32) + total).astype(BF16)
    sent(f_send, f_ssem)


def solution(mesh):
    def body(x_blk, gain_blk, w_in_blk, w_out_blk):
        tok, half = x_blk.shape
        feat = w_in_blk.shape[0]
        tokens = 4 * tok
        dma = pltpu.SemaphoreType.DMA
        return pl.pallas_call(
            kernel,
            out_shape=pltpu.VMEM((tok, half), BF16),
            in_specs=[pl.BlockSpec(memory_space=pl.ANY)] * 4,
            out_specs=pl.BlockSpec(memory_space=pltpu.VMEM),
            scratch_shapes=[
                pltpu.VMEM((tok, half), BF16),
                pltpu.VMEM((2, half), F32),
                pltpu.VMEM((8, 8, 128), F32),
                pltpu.VMEM((4, tok, feat), BF16),
                pltpu.VMEM((tok, feat), BF16),
                pltpu.VMEM((tokens, feat), BF16),
                pltpu.VMEM((N, feat, 2 * C), BF16),
                pltpu.VMEM((N, C, half), BF16),
                pltpu.VMEM((N, tokens, C), F32),
                pltpu.VMEM((N, tokens, C), F32),
                pltpu.VMEM((N, tokens, C), F32),
                pltpu.VMEM((NA, tokens, C), F32),
                pltpu.VMEM((2 * NA + NB, tokens, C), BF16),
                pltpu.VMEM((tokens, half), F32),
                pltpu.VMEM((2, tok, half), F32),
                pltpu.VMEM((tok, half), F32),
                pltpu.VMEM((tok, half), F32),
                dma((8,)),
                dma((N // GROUP,)),
                dma((8,)),
                dma((RING,)),
                dma((NA,)),
                dma((NA,)),
                dma((NB,)),
                dma((2, TAIL)),
                dma((TAIL,)),
            ],
            compiler_params=pltpu.CompilerParams(
                collective_id=0, has_side_effects=True, vmem_limit_bytes=66_500_000
            ),
        )(x_blk, gain_blk, w_in_blk, w_out_blk)

    return jax.shard_map(
        body,
        mesh=mesh,
        in_specs=(P(("dp", "row"), "col"), P("col"), P("row", "col"), P("row", "col")),
        out_specs=P(("dp", "row"), "col"),
        check_vma=False,
    )
```

```python
import jax
import jax.numpy as jnp
from jax import lax
from jax.experimental import pallas as pl
from jax.experimental.pallas import tpu as pltpu
from jax.sharding import PartitionSpec as P

NORM_EPS = 1e-5
MESH = pl.DeviceIdType.MESH
F32 = jnp.float32
BF16 = jnp.bfloat16

C = 256
NA = 12
NB = 8
N = NA + NB
NF = 4
GROUP = 5
RING = 8
TA = 16


def kernel(x_hbm, gain_hbm, w_in_hbm, w_out_hbm, out_v,
           x_v, gain_v, stat_g, x_g, x_relay, z_v, w_in_v, w_out_v, d_send, d_recv, own, x_recv, hall,
           acc, ea_recv, eb_recv, fa_send, fa_recv, fb_send, fb_recv,
           misc_sem, w_in_sem, send_sem, d_rsem, x_rsem, y_rsem, b_rsem, e_rsem, f_rsem):
    w_out_sem, stat_rsem, z_rsem = misc_sem.at[4], misc_sem.at[5], misc_sem.at[6]
    stat_ssem, z_ssem, d_ssem, x_ssem, y_ssem, b_ssem, e_ssem, f_ssem = [send_sem.at[i] for i in range(8)]
    y = lax.axis_index("col")
    row = lax.axis_index("row")
    x = row // 2
    k = row % 2
    dp = lax.axis_index("dp")
    home = 1 - (x + y) % 2
    tok, half = x_v.shape
    feat = half // 2
    block = N * C
    rows_a = 4 * TA
    tb = tok - TA
    rows_b = 4 * tb
    sibling = (dp, y, 2 * x + 1 - k)
    x_next = (dp, y, 2 * (1 - x) + k)
    y_next = (dp, 1 - y, row)

    def remote(src, dst, ssem, rsem, dev):
        return pltpu.make_async_remote_copy(src_ref=src, dst_ref=dst, send_sem=ssem, recv_sem=rsem,
                                            device_id=dev, device_id_type=MESH)

    def col_b(j):
        return C * j

    def col_a(j):
        return C * (NB + j)

    def pos_col(p):
        j = p // 2
        q = p % 2
        is_b = (home + q) % 2
        return is_b * col_b(j) + (1 - is_b) * col_a(j)

    def w_in_copies(p, c):
        cs = pl.multiple_of((1 - k) * block + c, C)
        co = pl.multiple_of(k * block + c, C)
        return (pltpu.make_async_copy(w_in_hbm.at[:, pl.ds(cs, C)], w_in_v.at[p, :, pl.ds(0, C)], w_in_sem.at[p // GROUP]),
                pltpu.make_async_copy(w_in_hbm.at[:, pl.ds(co, C)], w_in_v.at[p, :, pl.ds(C, C)], w_in_sem.at[p // GROUP]))

    def w_out_copy(i):
        r = pl.multiple_of(i * C, C)
        return pltpu.make_async_copy(w_out_hbm.at[pl.ds(r, C), :], w_out_v.at[i], w_out_sem)

    x_copy = pltpu.make_async_copy(x_hbm, x_v, misc_sem.at[0])
    g_copy = pltpu.make_async_copy(gain_hbm, gain_v.at[0], misc_sem.at[1])
    x_copy.start()
    g_copy.start()

    barrier = pltpu.get_barrier_semaphore()
    for dy in range(2):
        for dr in range(4):
            if dy or dr:
                pl.semaphore_signal(barrier, inc=1, device_id=(dp, (y + dy) % 2, (row + dr) % 4), device_id_type=MESH)

    def start_pair(p, _):
        for cp in w_in_copies(p, pos_col(p)):
            cp.start()
        return 0

    def start_rest(j, _):
        for cp in w_in_copies(NB + j, col_a(j)):
            cp.start()
        return 0

    lax.fori_loop(0, 2 * NB, start_pair, 0)
    lax.fori_loop(NB, NA, start_rest, 0)

    x_copy.wait()
    g_copy.wait()
    x_f = x_v[...].astype(F32)
    s1 = jnp.sum(x_f, axis=1, keepdims=True)
    s2 = jnp.sum(x_f * x_f, axis=1, keepdims=True)
    lane = lax.broadcasted_iota(jnp.int32, (tok, 128), 1)
    me = 4 * y + row
    stat_g[me, :, :tok] = jnp.transpose(jnp.where(lane == 0, s1, s2))[:8]
    with jax.named_scope('barrier'):
        pl.semaphore_wait(barrier, 7)

    def tok_copy(dy, dk):
        ty = (y + dy) % 2
        tk = (k + dk) % 2
        cols = pl.ds(pl.multiple_of(feat * tk, 128), feat)
        return remote(x_v.at[:, cols], x_g.at[row], z_ssem, z_rsem, (dp, ty, 2 * y + tk))

    def stat_copy(d):
        ty = (y + d // 4) % 2
        tr = (row + d % 4) % 4
        return remote(stat_g.at[me], stat_g.at[me], stat_ssem, stat_rsem, (dp, ty, tr))

    gain_cp = remote(gain_v.at[0], gain_v.at[1], misc_sem.at[2], misc_sem.at[3], y_next)
    half_cols = pl.ds(pl.multiple_of(feat * (1 - k), 128), feat)
    to_relay = remote(x_v.at[:, half_cols], x_relay, z_ssem, misc_sem.at[7], y_next)
    from_relay = remote(x_relay, x_g.at[row], z_ssem, z_rsem, (dp, y, 2 * (1 - x) + 1 - k))

    for d in range(1, 8):
        stat_copy(d).start()

    @pl.when(home == 0)
    def _():
        to_relay.start()
        tok_copy(1, 0).start()
        tok_copy(0, 0).start()
        tok_copy(0, 1).start()

    @pl.when(home == 1)
    def _():
        gain_cp.start()
        tok_copy(0, 1).start()
        tok_copy(1, 0).start()
        tok_copy(1, 1).start()
        x_g[row] = jnp.where(k == 0, x_v[:, :feat], x_v[:, feat:])
        gain_v[1] = gain_v[0]
        with jax.named_scope('x_relay_wait'):
            to_relay.wait_recv()
        from_relay.start()

    @pl.when(home == 0)
    def _():
        with jax.named_scope('gain_wait'):
            gain_cp.wait_recv()
    gain = jnp.where(k == 0, gain_v[1, :feat], gain_v[1, feat:]).reshape(1, feat)
    acc[...] = jnp.zeros_like(acc)
    with jax.named_scope('stat_wait'):
        remote(stat_g.at[pl.ds(0, 7)], stat_g.at[pl.ds(0, 7)], stat_ssem, stat_rsem, y_next).wait_recv()

    @pl.when(home == 0)
    def _():
        with jax.named_scope('z_wait'):
            remote(x_g, x_g, z_ssem, z_rsem, y_next).wait_recv()

    @pl.when(home == 1)
    def _():
        with jax.named_scope('z_wait'):
            remote(x_g.at[pl.ds(0, 3)], x_g.at[pl.ds(0, 3)], z_ssem, z_rsem, y_next).wait_recv()
    for src in range(4):
        st = jnp.transpose(stat_g[src] + stat_g[4 + src])[:tok] * (1.0 / (2 * half))
        mean = st[:, 0:1]
        var = st[:, 1:2] - mean * mean
        z = (x_g[src].astype(F32) - mean) * lax.rsqrt(var + NORM_EPS) * gain
        z = z.astype(BF16)
        z_v[pl.ds(TA * src, TA), :] = z[:TA]
        z_v[pl.ds(rows_a + tb * src, tb), :] = z[TA:]

    def d_copy(p):
        return remote(d_send.at[p], d_recv.at[p], d_ssem, d_rsem.at[p % RING], sibling)

    def slot_of(p):
        late = p // (2 * NB)
        return (1 - late) * (p // 2 + NA * (p % 2)) + late * (p - NB + NA * home)

    row_group = (pl.ds(0, rows_a), pl.ds(rows_a, rows_b))

    def part_of(ref, j, part):
        if part == 2:
            return ref.at[j]
        if part == 0:
            return ref.at[j, row_group[0]]
        return ref.at[pl.ds(j, 2), row_group[1]]

    def x_copy_of(j, part):
        sem = x_rsem.at[NA + j // 2] if part == 1 else x_rsem.at[j]
        return remote(part_of(own, j, part), part_of(x_recv, j, part), x_ssem, sem, x_next)

    def up(p, c):
        @pl.when(p % GROUP == 0)
        def _():
            with jax.named_scope('w_in_wait'):
                group = w_in_v.at[pl.ds(p, GROUP)]
                pltpu.make_async_copy(group, group, w_in_sem.at[p // GROUP]).wait()

        part = jnp.dot(z_v[...], w_in_v[p], preferred_element_type=F32)
        d_send[p] = part[:, :C]
        own[slot_of(p)] = part[:, C:]
        d_copy(p).start()

    def pair_sum(p):
        with jax.named_scope('pair_wait'):
            d_copy(p).wait_recv()
        slot = slot_of(p)
        own[slot] = own[slot] + d_recv[p]

        @pl.when((slot < NA) & ((home == 1) | (slot >= NF)))
        def _():
            x_copy_of(slot, 0).start()

        @pl.when((slot < NF) & (home == 0))
        def _():
            x_copy_of(slot, 2).start()

    def up_step(p, _):
        late = p // (2 * NB)
        up(p, (1 - late) * pos_col(p) + late * col_a(p - NB))
        w_out_copy(p).start()

        @pl.when(p >= 2)
        def _():
            pair_sum(p - 2)
        return 0

    lax.fori_loop(0, N, up_step, 0)
    pair_sum(N - 2)
    pair_sum(N - 1)

    first_b = NF * (1 - home)
    for m in range(NB // 2):
        x_copy_of(first_b + 2 * m, 1).start()

    with jax.named_scope('w_out_wait'):
        pltpu.make_async_copy(w_out_v, w_out_v, w_out_sem).wait()

    def y_copy(j, part):
        sem = y_rsem.at[NA + j // 2] if part == 1 else y_rsem.at[j]
        return remote(part_of(hall, j, part), part_of(hall, NA + j, part), y_ssem, sem, y_next)

    def b_sem(j, part):
        return b_rsem.at[NB + j // 2] if part == 1 else b_rsem.at[j]

    def relay_copy(j, part):
        return remote(part_of(hall, NA + j, part), part_of(hall, 2 * NA + j, part), b_ssem, b_sem(j, part), x_next)

    def back_copy(j, part):
        return remote(part_of(hall, 2 * NA + j, part), part_of(hall, 2 * NA + j, part), b_ssem, b_sem(j, part), y_next)

    def make_h(j, part):
        with jax.named_scope('x_wait'):
            x_copy_of(j, part).wait_recv()
        if part == 2:
            rows, chunks = pl.ds(0, rows_a + rows_b), (j,)
        elif part == 0:
            rows, chunks = row_group[0], (j,)
        else:
            rows, chunks = row_group[1], (j, j + 1)
        for c in chunks:
            total = own[NA + c, rows, :] + x_recv[c, rows, :]
            hall[c, rows, :] = jax.nn.gelu(total, approximate=True).astype(BF16)
        y_copy(j, part).start()

    def down(slot, i, part):
        if part == 2:
            acc[...] += jnp.dot(hall[slot], w_out_v[i], preferred_element_type=F32)
        elif part == 0:
            rows = row_group[0]
            acc[rows, :] += jnp.dot(hall[slot, rows, :], w_out_v[i], preferred_element_type=F32)
        else:
            rows = row_group[1]
            acc[rows, :] += (jnp.dot(hall[slot, rows, :], w_out_v[i], preferred_element_type=F32)
                             + jnp.dot(hall[slot + 1, rows, :], w_out_v[i + 1], preferred_element_type=F32))

    e_recv, f_send, f_recv = (ea_recv, eb_recv), (fa_send, fb_send), (fa_recv, fb_recv)

    def token_rows(group, r):
        n, base = ((TA, 0), (tb, rows_a))[group]
        return pl.ds(pl.multiple_of(base + n * r, 8), n)

    def e_copy(group, s):
        r = 2 * (s * x + (1 - s) * (1 - x)) + 1 - k
        return remote(acc.at[token_rows(group, r)], e_recv[group].at[s], e_ssem, e_rsem.at[2 * group + s], sibling)

    def f_copy(group):
        return remote(f_send[group], f_recv[group], f_ssem, f_rsem.at[group], x_next)

    def end_start(group):
        e_copy(group, 0).start()
        e_copy(group, 1).start()

    def end_send(group):
        with jax.named_scope('e0_wait'):
            e_copy(group, 0).wait_recv()
        f_send[group][...] = acc[token_rows(group, 2 * (1 - x) + k), :] + e_recv[group][0]
        f_copy(group).start()

    def end_sum(group):
        with jax.named_scope('e1_wait'):
            e_copy(group, 1).wait_recv()
        with jax.named_scope('f_wait'):
            f_copy(group).wait_recv()
        total = acc[token_rows(group, row), :] + e_recv[group][1] + f_recv[group][...]
        t0, n = ((0, TA), (TA, tb))[group]
        out_v[t0:t0 + n, :] = (x_v[t0:t0 + n, :].astype(F32) + total).astype(BF16)

    def loop(lo, hi, step):
        def body(i, _):
            step(i)
            return 0
        lax.fori_loop(lo, hi, body, 0)

    @pl.when(home == 1)
    def _():
        def relay(i, part):
            with jax.named_scope('relay_wait'):
                y_copy(i, part).wait_recv()
            relay_copy(i, part).start()

        def b_step(i, part):
            with jax.named_scope('b_wait'):
                back_copy(i, part).wait_recv()
            down(2 * NA + i, i, part)

        def a_step(j, part):
            make_h(j, part)
            down(j, NB + j, part)

        loop(0, NF, lambda j: a_step(j, 2))

        def step(t):
            @pl.when((t >= 1) & (t < 5))
            def _():
                relay(2 * t - 2, 0)
                relay(2 * t - 1, 0)

            @pl.when(t >= 5)
            def _():
                relay(2 * (t - 5), 1)
            a_step(NF + t, 0)

        loop(0, NA - NF, step)
        relay(NB - 2, 1)

        def step(m):
            b_step(2 * m, 0)
            a_step(NF + 2 * m, 1)
            b_step(2 * m + 1, 0)

        loop(0, NB // 2, step)
        end_start(0)
        loop(0, 1, lambda m: b_step(2 * m, 1))
        end_send(0)
        loop(1, NB // 2, lambda m: b_step(2 * m, 1))

    @pl.when(home == 0)
    def _():
        def a_step(j, part):
            with jax.named_scope('a_wait'):
                y_copy(j, part).wait_recv()
            down(NA + j, NB + j, part)

        def b_step(i, part):
            with jax.named_scope('b_wait'):
                relay_copy(i, part).wait_recv()
            back_copy(i, part).start()
            down(2 * NA + i, i, part)

        loop(0, NB, lambda j: make_h(j, 0))

        def step(t):
            a_step(2 * t, 2)
            a_step(2 * t + 1, 2)
            make_h(2 * t, 1)

        loop(0, 2, step)

        def step(t):
            a_step(NF + 2 * t, 0)
            make_h(4 + 2 * t, 1)
            a_step(NF + 2 * t + 1, 0)

        loop(0, 2, step)

        def step(t):
            b_step(2 * t, 0)
            b_step(2 * t + 1, 0)
            a_step(NF + 4 + t, 0)

        loop(0, 4, step)
        end_start(0)
        loop(0, 2, lambda m: b_step(2 * m, 1))
        end_send(0)

        def step(m):
            b_step(4 + 2 * m, 1)
            a_step(NF + 2 * m, 1)

        loop(0, 2, step)
        loop(2, 4, lambda m: a_step(NF + 2 * m, 1))

    end_start(1)
    end_send(1)

    def sent(ref, sem):
        remote(ref, ref, sem, sem, y_next).wait_send()

    with jax.named_scope('drain'):
        sent(stat_g.at[pl.ds(0, 7)], stat_ssem)
        sent(x_g, z_ssem)
        sent(d_send, d_ssem)
        sent(hall.at[pl.ds(0, NB)], b_ssem)
        sent(ea_recv, e_ssem)
        sent(eb_recv, e_ssem)

        @pl.when(home == 0)
        def _():
            sent(own.at[pl.ds(0, NA)], x_ssem)
            sent(hall.at[pl.ds(0, NB)], y_ssem)

        @pl.when(home == 1)
        def _():
            gain_cp.wait_send()
            sent(own.at[pl.ds(0, NB)], x_ssem)
            sent(hall.at[pl.ds(0, NA)], y_ssem)

    end_sum(0)
    end_sum(1)
    sent(fa_send, f_ssem)
    sent(fb_send, f_ssem)


def solution(mesh):
    def body(x_blk, gain_blk, w_in_blk, w_out_blk):
        tok, half = x_blk.shape
        feat = w_in_blk.shape[0]
        tokens = 4 * tok
        dma = pltpu.SemaphoreType.DMA
        return pl.pallas_call(
            kernel,
            out_shape=pltpu.VMEM((tok, half), BF16),
            in_specs=[pl.BlockSpec(memory_space=pl.ANY)] * 4,
            out_specs=pl.BlockSpec(memory_space=pltpu.VMEM),
            scratch_shapes=[
                pltpu.VMEM((tok, half), BF16),
                pltpu.VMEM((2, half), F32),
                pltpu.VMEM((8, 8, 128), F32),
                pltpu.VMEM((4, tok, feat), BF16),
                pltpu.VMEM((tok, feat), BF16),
                pltpu.VMEM((tokens, feat), BF16),
                pltpu.VMEM((N, feat, 2 * C), BF16),
                pltpu.VMEM((N, C, half), BF16),
                pltpu.VMEM((N, tokens, C), F32),
                pltpu.VMEM((N, tokens, C), F32),
                pltpu.VMEM((2 * NA, tokens, C), F32),
                pltpu.VMEM((NA, tokens, C), F32),
                pltpu.VMEM((2 * NA + NB, tokens, C), BF16),
                pltpu.VMEM((tokens, half), F32),
                pltpu.VMEM((2, TA, half), F32),
                pltpu.VMEM((2, tok - TA, half), F32),
                pltpu.VMEM((TA, half), F32),
                pltpu.VMEM((TA, half), F32),
                pltpu.VMEM((tok - TA, half), F32),
                pltpu.VMEM((tok - TA, half), F32),
                dma((8,)),
                dma((N // GROUP,)),
                dma((8,)),
                dma((RING,)),
                dma((NA + NA // 2,)),
                dma((NA + NA // 2,)),
                dma((NB + NB // 2,)),
                dma((4,)),
                dma((2,)),
            ],
            compiler_params=pltpu.CompilerParams(
                collective_id=0, has_side_effects=True, vmem_limit_bytes=66_500_000
            ),
        )(x_blk, gain_blk, w_in_blk, w_out_blk)

    return jax.shard_map(
        body,
        mesh=mesh,
        in_specs=(P(("dp", "row"), "col"), P("col"), P("row", "col"), P("row", "col")),
        out_specs=P(("dp", "row"), "col"),
        check_vma=False,
    )
```

```python
import jax
import jax.numpy as jnp
from jax import lax
from jax.experimental import pallas as pl
from jax.experimental.pallas import tpu as pltpu
from jax.sharding import PartitionSpec as P

NORM_EPS = 1e-5
MESH = pl.DeviceIdType.MESH
F32 = jnp.float32
BF16 = jnp.bfloat16

C = 256
NB = 4
NC = 5
NA = 11
N = NA + NB + NC
NF = 3
GROUP = 5
RING = 8
TA = 16


def kernel(x_hbm, gain_hbm, w_in_hbm, w_out_hbm, out_v,
           x_v, gain_v, stat_g, x_g, x_relay, z_v, w_in_v, w_out_v, d_send, d_recv, own, x_recv, c_recv, hall,
           acc, ea_recv, eb_recv, fa_send, fa_recv, fb_send, fb_recv,
           misc_sem, w_in_sem, send_sem, d_rsem, x_rsem, y_rsem, b_rsem, c_rsem, e_rsem, f_rsem):
    w_out_sem, stat_rsem, z_rsem = misc_sem.at[4], misc_sem.at[5], misc_sem.at[6]
    stat_ssem, z_ssem, d_ssem, x_ssem, y_ssem, b_ssem, c_ssem, e_ssem, f_ssem = [send_sem.at[i] for i in range(9)]
    y = lax.axis_index("col")
    row = lax.axis_index("row")
    x = row // 2
    k = row % 2
    dp = lax.axis_index("dp")
    home = 1 - (x + y) % 2
    tok, half = x_v.shape
    feat = half // 2
    block = N * C
    rows_a = 4 * TA
    tb = tok - TA
    rows_b = 4 * tb
    sibling = (dp, y, 2 * x + 1 - k)
    x_next = (dp, y, 2 * (1 - x) + k)
    y_next = (dp, 1 - y, row)

    def remote(src, dst, ssem, rsem, dev):
        return pltpu.make_async_remote_copy(src_ref=src, dst_ref=dst, send_sem=ssem, recv_sem=rsem,
                                            device_id=dev, device_id_type=MESH)

    c0, a0 = NB, NB + NC

    def chunk_of(p):
        u = p - 2 * NB - 1
        pair = jnp.where(p % 2 == 1, c0 + p // 2, p // 2 + (1 - home) * a0)
        mixed = jnp.where(u % 2 == 1, u // 2, a0 + NB + u // 2)
        late = jnp.where((home == 1) | (u >= 2 * NB), a0 + u, mixed)
        return jnp.where(p < 2 * NB, pair, jnp.where(u < 0, a0 - 1, late))

    def w_in_copies(p):
        c = C * chunk_of(p)
        cs = pl.multiple_of((1 - k) * block + c, C)
        co = pl.multiple_of(k * block + c, C)
        return (pltpu.make_async_copy(w_in_hbm.at[:, pl.ds(cs, C)], w_in_v.at[p, :, pl.ds(0, C)], w_in_sem.at[p // GROUP]),
                pltpu.make_async_copy(w_in_hbm.at[:, pl.ds(co, C)], w_in_v.at[p, :, pl.ds(C, C)], w_in_sem.at[p // GROUP]))

    def w_out_copy(i):
        r = pl.multiple_of(i * C, C)
        return pltpu.make_async_copy(w_out_hbm.at[pl.ds(r, C), :], w_out_v.at[i], w_out_sem)

    x_copy = pltpu.make_async_copy(x_hbm, x_v, misc_sem.at[0])
    g_copy = pltpu.make_async_copy(gain_hbm, gain_v.at[0], misc_sem.at[1])
    x_copy.start()
    g_copy.start()

    barrier = pltpu.get_barrier_semaphore()
    for dy in range(2):
        for dr in range(4):
            if dy or dr:
                pl.semaphore_signal(barrier, inc=1, device_id=(dp, (y + dy) % 2, (row + dr) % 4), device_id_type=MESH)

    def start_w_in(p, _):
        for cp in w_in_copies(p):
            cp.start()
        return 0

    lax.fori_loop(0, N, start_w_in, 0)

    x_copy.wait()
    g_copy.wait()
    x_f = x_v[...].astype(F32)
    s1 = jnp.sum(x_f, axis=1, keepdims=True)
    s2 = jnp.sum(x_f * x_f, axis=1, keepdims=True)
    lane = lax.broadcasted_iota(jnp.int32, (tok, 128), 1)
    me = 4 * y + row
    stat_g[me, :, :tok] = jnp.transpose(jnp.where(lane == 0, s1, s2))[:8]
    with jax.named_scope('barrier'):
        pl.semaphore_wait(barrier, 7)

    def tok_copy(dy, dk):
        ty = (y + dy) % 2
        tk = (k + dk) % 2
        cols = pl.ds(pl.multiple_of(feat * tk, 128), feat)
        return remote(x_v.at[:, cols], x_g.at[row], z_ssem, z_rsem, (dp, ty, 2 * y + tk))

    def stat_copy(d):
        ty = (y + d // 4) % 2
        tr = (row + d % 4) % 4
        return remote(stat_g.at[me], stat_g.at[me], stat_ssem, stat_rsem, (dp, ty, tr))

    gain_cp = remote(gain_v.at[0], gain_v.at[1], misc_sem.at[2], misc_sem.at[3], y_next)
    half_cols = pl.ds(pl.multiple_of(feat * (1 - k), 128), feat)
    to_relay = remote(x_v.at[:, half_cols], x_relay, z_ssem, misc_sem.at[7], y_next)
    from_relay = remote(x_relay, x_g.at[row], z_ssem, z_rsem, (dp, y, 2 * (1 - x) + 1 - k))

    for d in range(1, 8):
        stat_copy(d).start()

    @pl.when(home == 0)
    def _():
        to_relay.start()
        tok_copy(1, 0).start()
        tok_copy(0, 0).start()
        tok_copy(0, 1).start()

    @pl.when(home == 1)
    def _():
        gain_cp.start()
        tok_copy(0, 1).start()
        tok_copy(1, 0).start()
        tok_copy(1, 1).start()
        x_g[row] = jnp.where(k == 0, x_v[:, :feat], x_v[:, feat:])
        gain_v[1] = gain_v[0]
        with jax.named_scope('x_relay_wait'):
            to_relay.wait_recv()
        from_relay.start()

    @pl.when(home == 0)
    def _():
        with jax.named_scope('gain_wait'):
            gain_cp.wait_recv()
    gain = jnp.where(k == 0, gain_v[1, :feat], gain_v[1, feat:]).reshape(1, feat)
    acc[...] = jnp.zeros_like(acc)
    with jax.named_scope('stat_wait'):
        remote(stat_g.at[pl.ds(0, 7)], stat_g.at[pl.ds(0, 7)], stat_ssem, stat_rsem, y_next).wait_recv()

    @pl.when(home == 0)
    def _():
        with jax.named_scope('z_wait'):
            remote(x_g, x_g, z_ssem, z_rsem, y_next).wait_recv()

    @pl.when(home == 1)
    def _():
        with jax.named_scope('z_wait'):
            remote(x_g.at[pl.ds(0, 3)], x_g.at[pl.ds(0, 3)], z_ssem, z_rsem, y_next).wait_recv()
    for src in range(4):
        st = jnp.transpose(stat_g[src] + stat_g[4 + src])[:tok] * (1.0 / (2 * half))
        mean = st[:, 0:1]
        var = st[:, 1:2] - mean * mean
        z = (x_g[src].astype(F32) - mean) * lax.rsqrt(var + NORM_EPS) * gain
        z = z.astype(BF16)
        z_v[pl.ds(TA * src, TA), :] = z[:TA]
        z_v[pl.ds(rows_a + tb * src, tb), :] = z[TA:]

    def d_copy(p):
        return remote(d_send.at[p], d_recv.at[p], d_ssem, d_rsem.at[p % RING], sibling)

    row_group = (pl.ds(0, rows_a), pl.ds(rows_a, rows_b))

    def part_of(ref, j, part):
        if part == 2:
            return ref.at[j]
        if part == 0:
            return ref.at[j, row_group[0]]
        return ref.at[pl.ds(j, 2), row_group[1]]

    def x_copy_of(j, part, first):
        sem = x_rsem.at[NA + j // 2] if part == 1 else x_rsem.at[j]
        return remote(part_of(own, first + j, part), part_of(x_recv, j, part), x_ssem, sem, x_next)

    def c_copy(j):
        return remote(own.at[c0 + j], c_recv.at[0, j], c_ssem, c_rsem.at[j], y_next)

    def c_relay(j):
        return remote(c_recv.at[0, j], c_recv.at[1, j], c_ssem, c_rsem.at[NC + j], x_next)

    def pass_c(j):
        with jax.named_scope('c_wait'):
            c_copy(j).wait_recv()
        c_relay(j).start()

    def up(p):
        @pl.when(p % GROUP == 0)
        def _():
            with jax.named_scope('w_in_wait'):
                group = w_in_v.at[pl.ds(p, GROUP)]
                pltpu.make_async_copy(group, group, w_in_sem.at[p // GROUP]).wait()

        part = jnp.dot(z_v[...], w_in_v[p], preferred_element_type=F32)
        d_send[p] = part[:, :C]
        own[chunk_of(p)] = part[:, C:]
        d_copy(p).start()

    def pair_sum(p):
        with jax.named_scope('pair_wait'):
            d_copy(p).wait_recv()
        q = chunk_of(p)
        own[q] = own[q] + d_recv[p]

        @pl.when((q >= c0) & (q < a0))
        def _():
            c_copy(q - c0).start()

        @pl.when((home == 1) & (q < c0))
        def _():
            x_copy_of(q, 0, 0).start()

            @pl.when(q % 2 == 1)
            def _():
                x_copy_of(q - 1, 1, 0).start()

        @pl.when((home == 0) & (q >= a0 + NF))
        def _():
            x_copy_of(q - a0, 0, a0).start()

        @pl.when((home == 0) & (q >= a0) & (q < a0 + NF))
        def _():
            x_copy_of(q - a0, 2, a0).start()

    def up_step(p, _):
        up(p)
        w_out_copy(p).start()

        @pl.when(p >= 2)
        def _():
            pair_sum(p - 2)

        @pl.when((p == N - 2) & (home == 1))
        def _():
            pass_c(0)
        return 0

    lax.fori_loop(0, N, up_step, 0)
    pair_sum(N - 2)
    pair_sum(N - 1)

    @pl.when(home == 0)
    def _():
        for j in range(NF, NA, 2):
            x_copy_of(j, 1, a0).start()

    with jax.named_scope('w_out_wait'):
        pltpu.make_async_copy(w_out_v, w_out_v, w_out_sem).wait()

    def y_copy(j, part):
        sem = y_rsem.at[NA + j // 2] if part == 1 else y_rsem.at[j]
        return remote(part_of(hall, j, part), part_of(hall, NA + j, part), y_ssem, sem, y_next)

    def b_sem(j, part):
        return b_rsem.at[NB + j // 2] if part == 1 else b_rsem.at[j]

    def relay_copy(j, part):
        return remote(part_of(hall, NA + j, part), part_of(hall, 2 * NA + j, part), b_ssem, b_sem(j, part), x_next)

    def back_copy(j, part):
        return remote(part_of(hall, 2 * NA + j, part), part_of(hall, 2 * NA + j, part), b_ssem, b_sem(j, part), y_next)

    def make_h(j, part, first):
        with jax.named_scope('x_wait'):
            x_copy_of(j, part, 0).wait_recv()
        if part == 2:
            rows, chunks = pl.ds(0, rows_a + rows_b), (j,)
        elif part == 0:
            rows, chunks = row_group[0], (j,)
        else:
            rows, chunks = row_group[1], (j, j + 1)
        for c in chunks:
            total = own[first + c, rows, :] + x_recv[c, rows, :]
            hall[c, rows, :] = jax.nn.gelu(total, approximate=True).astype(BF16)
        y_copy(j, part).start()

    def make_h_c(j):
        with jax.named_scope('c_wait'):
            c_copy(j).wait_recv()
            c_relay(j).wait_recv()
        hall[c0 + j] = jax.nn.gelu(c_recv[0, j] + c_recv[1, j], approximate=True).astype(BF16)
        y_copy(c0 + j, 2).start()

    def down(slot, i, part):
        if part == 2:
            acc[...] += jnp.dot(hall[slot], w_out_v[i], preferred_element_type=F32)
        elif part == 0:
            rows = row_group[0]
            acc[rows, :] += jnp.dot(hall[slot, rows, :], w_out_v[i], preferred_element_type=F32)
        else:
            rows = row_group[1]
            acc[rows, :] += (jnp.dot(hall[slot, rows, :], w_out_v[i], preferred_element_type=F32)
                             + jnp.dot(hall[slot + 1, rows, :], w_out_v[i + 1], preferred_element_type=F32))

    e_recv, f_send, f_recv = (ea_recv, eb_recv), (fa_send, fb_send), (fa_recv, fb_recv)

    def token_rows(group, r):
        n, base = ((TA, 0), (tb, rows_a))[group]
        return pl.ds(pl.multiple_of(base + n * r, 8), n)

    def e_copy(group, s):
        r = 2 * (s * x + (1 - s) * (1 - x)) + 1 - k
        return remote(acc.at[token_rows(group, r)], e_recv[group].at[s], e_ssem, e_rsem.at[2 * group + s], sibling)

    def f_copy(group):
        return remote(f_send[group], f_recv[group], f_ssem, f_rsem.at[group], x_next)

    def end_start(group):
        e_copy(group, 0).start()
        e_copy(group, 1).start()

    def end_send(group):
        with jax.named_scope('e0_wait'):
            e_copy(group, 0).wait_recv()
        f_send[group][...] = acc[token_rows(group, 2 * (1 - x) + k), :] + e_recv[group][0]
        f_copy(group).start()

    def end_sum(group):
        with jax.named_scope('e1_wait'):
            e_copy(group, 1).wait_recv()
        with jax.named_scope('f_wait'):
            f_copy(group).wait_recv()
        total = acc[token_rows(group, row), :] + e_recv[group][1] + f_recv[group][...]
        t0, n = ((0, TA), (TA, tb))[group]
        out_v[t0:t0 + n, :] = (x_v[t0:t0 + n, :].astype(F32) + total).astype(BF16)

    def loop(lo, hi, step):
        def body(i, _):
            step(i)
            return 0
        lax.fori_loop(lo, hi, body, 0)

    @pl.when(home == 1)
    def _():
        def relay(i, part):
            with jax.named_scope('relay_wait'):
                y_copy(i, part).wait_recv()
            relay_copy(i, part).start()

        def b_step(i, part):
            with jax.named_scope('b_wait'):
                back_copy(i, part).wait_recv()
            down(2 * NA + i, i, part)

        def c_step(i):
            with jax.named_scope('ch_wait'):
                y_copy(c0 + i, 2).wait_recv()
            down(NA + c0 + i, c0 + i, 2)

        def a_step(j, part):
            make_h(j, part, a0)
            down(j, a0 + j, part)

        pass_c(1)
        loop(0, NF, lambda j: a_step(j, 2))

        def step(j):
            for t, i in ((3, 2), (5, 3), (6, 4)):
                @pl.when(j == t)
                def _():
                    pass_c(i)
            a_step(j, 0)

        loop(NF, 8, step)

        def step(t):
            @pl.when(t < 2)
            def _():
                relay(2 * t, 0)
                relay(2 * t + 1, 0)

            @pl.when(t == 2)
            def _():
                relay(0, 1)
                relay(2, 1)
            c_step(t)
            a_step(8 + t, 0)

        loop(0, 3, step)

        def step(t):
            a_step(NF + 2 * t, 1)
            c_step(3 + t)

        loop(0, 2, step)

        def step(t):
            a_step(NF + 4 + 2 * t, 1)
            b_step(2 * t, 0)
            b_step(2 * t + 1, 0)

        loop(0, 2, step)
        end_start(0)
        loop(0, 1, lambda m: b_step(2 * m, 1))
        end_send(0)
        loop(1, 2, lambda m: b_step(2 * m, 1))

    @pl.when(home == 0)
    def _():
        def a_step(j, part):
            with jax.named_scope('a_wait'):
                y_copy(j, part).wait_recv()
            down(NA + j, a0 + j, part)

        def b_step(i, part):
            with jax.named_scope('b_wait'):
                relay_copy(i, part).wait_recv()
            back_copy(i, part).start()
            down(2 * NA + i, i, part)

        def c_step(i):
            make_h_c(i)
            down(c0 + i, c0 + i, 2)

        loop(0, NB, lambda j: make_h(j, 0, 0))
        loop(0, NB // 2, lambda m: make_h(2 * m, 1, 0))
        c_step(0)
        a_step(0, 2)
        c_step(1)
        loop(1, NF, lambda j: a_step(j, 2))

        def step(t):
            c_step(2 + t)
            loop(NF + 3 * t, NF + 3 * t + 3, lambda j: a_step(j, 0))

        loop(0, 2, step)
        c_step(4)

        def step(t):
            b_step(2 * t, 0)
            a_step(NF + 6 + t, 0)
            b_step(2 * t + 1, 0)

        loop(0, 2, step)
        end_start(0)

        def step(t):
            b_step(2 * t, 1)
            a_step(NF + 2 * t, 1)

            @pl.when(t == 0)
            def _():
                end_send(0)

        loop(0, 2, step)
        loop(2, 4, lambda m: a_step(NF + 2 * m, 1))

    end_start(1)
    end_send(1)

    def sent(ref, sem):
        remote(ref, ref, sem, sem, y_next).wait_send()

    with jax.named_scope('drain'):
        sent(stat_g.at[pl.ds(0, 7)], stat_ssem)
        sent(x_g, z_ssem)
        sent(d_send, d_ssem)
        sent(hall.at[pl.ds(0, NB)], b_ssem)
        sent(c_recv.at[0], c_ssem)
        sent(ea_recv, e_ssem)
        sent(eb_recv, e_ssem)

        @pl.when(home == 0)
        def _():
            sent(own.at[pl.ds(0, NA)], x_ssem)
            sent(hall.at[pl.ds(0, NB + NC)], y_ssem)

        @pl.when(home == 1)
        def _():
            gain_cp.wait_send()
            sent(own.at[pl.ds(0, NB)], x_ssem)
            sent(c_recv.at[1], c_ssem)
            sent(hall.at[pl.ds(0, NA)], y_ssem)

    end_sum(0)
    end_sum(1)
    sent(fa_send, f_ssem)
    sent(fb_send, f_ssem)


def solution(mesh):
    def body(x_blk, gain_blk, w_in_blk, w_out_blk):
        tok, half = x_blk.shape
        feat = w_in_blk.shape[0]
        tokens = 4 * tok
        dma = pltpu.SemaphoreType.DMA
        return pl.pallas_call(
            kernel,
            out_shape=pltpu.VMEM((tok, half), BF16),
            in_specs=[pl.BlockSpec(memory_space=pl.ANY)] * 4,
            out_specs=pl.BlockSpec(memory_space=pltpu.VMEM),
            scratch_shapes=[
                pltpu.VMEM((tok, half), BF16),
                pltpu.VMEM((2, half), F32),
                pltpu.VMEM((8, 8, 128), F32),
                pltpu.VMEM((4, tok, feat), BF16),
                pltpu.VMEM((tok, feat), BF16),
                pltpu.VMEM((tokens, feat), BF16),
                pltpu.VMEM((N, feat, 2 * C), BF16),
                pltpu.VMEM((N, C, half), BF16),
                pltpu.VMEM((N, tokens, C), F32),
                pltpu.VMEM((N, tokens, C), F32),
                pltpu.VMEM((N, tokens, C), F32),
                pltpu.VMEM((NA, tokens, C), F32),
                pltpu.VMEM((2, NC, tokens, C), F32),
                pltpu.VMEM((2 * NA + NB, tokens, C), BF16),
                pltpu.VMEM((tokens, half), F32),
                pltpu.VMEM((2, TA, half), F32),
                pltpu.VMEM((2, tok - TA, half), F32),
                pltpu.VMEM((TA, half), F32),
                pltpu.VMEM((TA, half), F32),
                pltpu.VMEM((tok - TA, half), F32),
                pltpu.VMEM((tok - TA, half), F32),
                dma((8,)),
                dma((N // GROUP,)),
                dma((9,)),
                dma((RING,)),
                dma((NA + NA // 2,)),
                dma((NA + NA // 2,)),
                dma((NB + NB // 2,)),
                dma((2 * NC,)),
                dma((4,)),
                dma((2,)),
            ],
            compiler_params=pltpu.CompilerParams(
                collective_id=0, has_side_effects=True, vmem_limit_bytes=66_500_000
            ),
        )(x_blk, gain_blk, w_in_blk, w_out_blk)

    return jax.shard_map(
        body,
        mesh=mesh,
        in_specs=(P(("dp", "row"), "col"), P("col"), P("row", "col"), P("row", "col")),
        out_specs=P(("dp", "row"), "col"),
        check_vma=False,
    )
```

```python
import jax
import jax.numpy as jnp
from jax import lax
from jax.experimental import pallas as pl
from jax.experimental.pallas import tpu as pltpu
from jax.sharding import PartitionSpec as P

NORM_EPS = 1e-5
MESH = pl.DeviceIdType.MESH
F32 = jnp.float32
BF16 = jnp.bfloat16

C = 256
NB = 4
NC = 5
NA = 11
N = NA + NB + NC
NF = 3
GROUP = 5
RING = 8
TA = 16


def kernel(x_hbm, gain_hbm, w_in_hbm, w_out_hbm, out_v,
           xa_v, xb_v, gain_v, stat_g, x_ga, x_gb, x_relay, z_v, w_in_v, w_out_v, d_send, d_recv, own, x_recv, c_recv, hall,
           acc, ea_recv, eb_recv, fa_send, fa_recv, fb_send, fb_recv,
           misc_sem, w_in_sem, send_sem, d_rsem, x_rsem, y_rsem, b_rsem, c_rsem, e_rsem, f_rsem):
    w_out_sem, stat_rsem, za_rsem, zb_rsem = [misc_sem.at[i] for i in range(4, 8)]
    stat_ssem, z_ssem, d_ssem, x_ssem, y_ssem, b_ssem, c_ssem, e_ssem, f_ssem = [send_sem.at[i] for i in range(9)]
    y = lax.axis_index("col")
    row = lax.axis_index("row")
    x = row // 2
    k = row % 2
    dp = lax.axis_index("dp")
    home = 1 - (x + y) % 2
    tok, half = out_v.shape
    feat = half // 2
    block = N * C
    rows_a = 4 * TA
    tb = tok - TA
    rows_b = 4 * tb
    sibling = (dp, y, 2 * x + 1 - k)
    x_next = (dp, y, 2 * (1 - x) + k)
    y_next = (dp, 1 - y, row)

    def remote(src, dst, ssem, rsem, dev):
        return pltpu.make_async_remote_copy(src_ref=src, dst_ref=dst, send_sem=ssem, recv_sem=rsem,
                                            device_id=dev, device_id_type=MESH)

    c0, a0 = NB, NB + NC

    def chunk_of(p):
        u = p - 2 * NB - 1
        pair = jnp.where(p % 2 == 1, c0 + p // 2, p // 2 + (1 - home) * a0)
        mixed = jnp.where(u % 2 == 1, u // 2, a0 + NB + u // 2)
        late = jnp.where((home == 1) | (u >= 2 * NB), a0 + u, mixed)
        return jnp.where(p < 2 * NB, pair, jnp.where(u < 0, a0 - 1, late))

    def w_in_copies(p):
        c = C * chunk_of(p)
        cs = pl.multiple_of((1 - k) * block + c, C)
        co = pl.multiple_of(k * block + c, C)
        return (pltpu.make_async_copy(w_in_hbm.at[:, pl.ds(cs, C)], w_in_v.at[p, :, pl.ds(0, C)], w_in_sem.at[p // GROUP]),
                pltpu.make_async_copy(w_in_hbm.at[:, pl.ds(co, C)], w_in_v.at[p, :, pl.ds(C, C)], w_in_sem.at[p // GROUP]))

    def w_out_copy(i):
        r = pl.multiple_of(i * C, C)
        return pltpu.make_async_copy(w_out_hbm.at[pl.ds(r, C), :], w_out_v.at[i], w_out_sem)

    xa_copy = pltpu.make_async_copy(x_hbm.at[pl.ds(0, TA)], xa_v, misc_sem.at[0])
    xb_copy = pltpu.make_async_copy(x_hbm.at[pl.ds(TA, tb)], xb_v, misc_sem.at[8])
    g_copy = pltpu.make_async_copy(gain_hbm, gain_v.at[0], misc_sem.at[1])
    xa_copy.start()
    xb_copy.start()
    g_copy.start()

    barrier = pltpu.get_barrier_semaphore()
    for dy in range(2):
        for dr in range(4):
            if dy or dr:
                pl.semaphore_signal(barrier, inc=1, device_id=(dp, (y + dy) % 2, (row + dr) % 4), device_id_type=MESH)

    def start_w_in(p, _):
        for cp in w_in_copies(p):
            cp.start()
        return 0

    lax.fori_loop(0, N, start_w_in, 0)

    xa_copy.wait()
    xb_copy.wait()
    g_copy.wait()

    def row_sums(ref):
        v = ref[...].astype(F32)
        lane = lax.broadcasted_iota(jnp.int32, (v.shape[0], 128), 1)
        return jnp.where(lane == 0, jnp.sum(v, axis=1, keepdims=True), jnp.sum(v * v, axis=1, keepdims=True))

    me = 4 * y + row
    stat_g[me, :, :tok] = jnp.transpose(jnp.concatenate([row_sums(xa_v), row_sums(xb_v)], axis=0))[:8]
    with jax.named_scope('barrier'):
        pl.semaphore_wait(barrier, 7)

    def tok_copy(group, dy, dk):
        tk = (k + dk) % 2
        cols = pl.ds(pl.multiple_of(feat * tk, 128), feat)
        src, dst, sem = ((xa_v, x_ga, za_rsem), (xb_v, x_gb, zb_rsem))[group]
        return remote(src.at[:, cols], dst.at[row], z_ssem, sem, (dp, (y + dy) % 2, 2 * y + tk))

    def stat_copy(d):
        ty = (y + d // 4) % 2
        tr = (row + d % 4) % 4
        return remote(stat_g.at[me], stat_g.at[me], stat_ssem, stat_rsem, (dp, ty, tr))

    gain_cp = remote(gain_v.at[0], gain_v.at[1], misc_sem.at[2], misc_sem.at[3], y_next)
    def to_relay(tk):
        return remote(xb_v.at[:, pl.ds(feat * tk, feat)], x_relay.at[tk], z_ssem, misc_sem.at[9], y_next)

    def from_relay(tk):
        return remote(x_relay.at[tk], x_gb.at[row], z_ssem, zb_rsem, (dp, y, 2 * (1 - x) + tk))

    for d in range(1, 8):
        stat_copy(d).start()

    @pl.when(home == 0)
    def _():
        to_relay(0).start()
        to_relay(1).start()
        tok_copy(0, 1, 0).start()
        tok_copy(0, 1, 1).start()
        for group in range(2):
            tok_copy(group, 0, 0).start()
            tok_copy(group, 0, 1).start()

    @pl.when(home == 1)
    def _():
        gain_cp.start()
        for group in range(2):
            tok_copy(group, 0, 1).start()
            tok_copy(group, 1, 0).start()
            tok_copy(group, 1, 1).start()
        x_ga[row] = jnp.where(k == 0, xa_v[:, :feat], xa_v[:, feat:])
        x_gb[row] = jnp.where(k == 0, xb_v[:, :feat], xb_v[:, feat:])
        gain_v[1] = gain_v[0]
        with jax.named_scope('x_relay_wait'):
            remote(x_relay, x_relay, z_ssem, misc_sem.at[9], y_next).wait_recv()
        from_relay(0).start()
        from_relay(1).start()

    @pl.when(home == 0)
    def _():
        with jax.named_scope('gain_wait'):
            gain_cp.wait_recv()
    gain = jnp.where(k == 0, gain_v[1, :feat], gain_v[1, feat:]).reshape(1, feat)
    acc[...] = jnp.zeros_like(acc)
    with jax.named_scope('stat_wait'):
        remote(stat_g.at[pl.ds(0, 7)], stat_g.at[pl.ds(0, 7)], stat_ssem, stat_rsem, y_next).wait_recv()

    def make_z(group):
        ref, sem = ((x_ga, za_rsem), (x_gb, zb_rsem))[group]

        @pl.when(home == 0)
        def _():
            with jax.named_scope('z_wait'):
                remote(ref, ref, z_ssem, sem, y_next).wait_recv()

        @pl.when(home == 1)
        def _():
            with jax.named_scope('z_wait'):
                remote(ref.at[pl.ds(0, 3)], ref.at[pl.ds(0, 3)], z_ssem, sem, y_next).wait_recv()

        t0, n, base = ((0, TA, 0), (TA, tb, rows_a))[group]
        for src in range(4):
            st = jnp.transpose(stat_g[src] + stat_g[4 + src])[t0:t0 + n] * (1.0 / (2 * half))
            mean = st[:, 0:1]
            var = st[:, 1:2] - mean * mean
            z = (ref[src].astype(F32) - mean) * lax.rsqrt(var + NORM_EPS) * gain
            z_v[pl.ds(base + n * src, n), :] = z.astype(BF16)

    row_group = (pl.ds(0, rows_a), pl.ds(rows_a, rows_b))

    def part_of(ref, j, part):
        if part == 2:
            return ref.at[j]
        if part == 1:
            return ref.at[pl.ds(j, 2), row_group[1]]
        return ref.at[j, row_group[part // 3]]

    def d_copy(p, part, seq):
        return remote(part_of(d_send, p, part), part_of(d_recv, p, part), d_ssem, d_rsem.at[seq % RING], sibling)

    def x_copy_of(j, part, first):
        sem = x_rsem.at[NA + j // 2] if part == 1 else x_rsem.at[j]
        return remote(part_of(own, first + j, part), part_of(x_recv, j, part), x_ssem, sem, x_next)

    def c_copy(j, part):
        return remote(part_of(own, c0 + j, part), part_of(c_recv.at[0], j, part), c_ssem, c_rsem.at[j], y_next)

    def c_relay(j):
        return remote(c_recv.at[0, j], c_recv.at[1, j], c_ssem, c_rsem.at[NC + j], x_next)

    def pass_c(j):
        with jax.named_scope('c_wait'):
            c_copy(j, 2).wait_recv()
        c_relay(j).start()

    def rows_of(part):
        return pl.ds(0, rows_a + rows_b) if part == 2 else row_group[part // 3]

    def up(p, part, seq):
        rows = rows_of(part)
        sums = jnp.dot(z_v[rows, :], w_in_v[p], preferred_element_type=F32)
        d_send[p, rows, :] = sums[:, :C]
        own[chunk_of(p), rows, :] = sums[:, C:]
        d_copy(p, part, seq).start()

    def pair_add(p, part, seq):
        with jax.named_scope('pair_wait'):
            d_copy(p, part, seq).wait_recv()
        q, rows = chunk_of(p), rows_of(part)
        own[q, rows, :] = own[q, rows, :] + d_recv[p, rows, :]

    def wait_w_in(p):
        with jax.named_scope('w_in_wait'):
            group = w_in_v.at[pl.ds(p, GROUP)]
            pltpu.make_async_copy(group, group, w_in_sem.at[p // GROUP]).wait()

    def pair_sum(p):
        pair_add(p, 2, p + 2)
        q = chunk_of(p)

        @pl.when((q >= c0) & (q < a0))
        def _():
            c_copy(q - c0, 2).start()

        @pl.when((home == 1) & (q < c0))
        def _():
            x_copy_of(q, 0, 0).start()

            @pl.when(q % 2 == 1)
            def _():
                x_copy_of(q - 1, 1, 0).start()

        @pl.when((home == 0) & (q >= a0 + NF))
        def _():
            x_copy_of(q - a0, 0, a0).start()

        @pl.when((home == 0) & (q >= a0) & (q < a0 + NF))
        def _():
            x_copy_of(q - a0, 2, a0).start()

    def up_step(p, _):
        @pl.when(p % GROUP == 0)
        def _():
            wait_w_in(p)
        up(p, 2, p + 2)
        w_out_copy(p).start()

        @pl.when(p >= 4)
        def _():
            pair_sum(p - 2)

        @pl.when((p >= 2) & (p < 4))
        def _():
            pair_add(p - 2, 3, p)

            @pl.when(p == 3)
            def _():
                c_copy(0, 3).start()

            @pl.when((p == 2) & (home == 0))
            def _():
                x_copy_of(0, 3, a0).start()

        @pl.when((p == N - 2) & (home == 1))
        def _():
            pass_c(0)
        return 0

    make_z(0)
    wait_w_in(0)
    up(0, 0, 0)
    up(1, 0, 1)
    make_z(1)
    up(0, 3, 2)
    w_out_copy(0).start()
    pair_add(0, 0, 0)

    @pl.when(home == 1)
    def _():
        x_copy_of(0, 0, 0).start()

    @pl.when(home == 0)
    def _():
        x_copy_of(0, 0, a0).start()

    up(1, 3, 3)
    w_out_copy(1).start()
    pair_add(1, 0, 1)
    c_copy(0, 0).start()
    lax.fori_loop(2, N, up_step, 0)
    pair_sum(N - 2)
    pair_sum(N - 1)

    @pl.when(home == 0)
    def _():
        for j in range(NF, NA, 2):
            x_copy_of(j, 1, a0).start()

    with jax.named_scope('w_out_wait'):
        pltpu.make_async_copy(w_out_v, w_out_v, w_out_sem).wait()

    def y_copy(j, part):
        sem = y_rsem.at[NA + j // 2] if part == 1 else y_rsem.at[j]
        return remote(part_of(hall, j, part), part_of(hall, NA + j, part), y_ssem, sem, y_next)

    def b_sem(j, part):
        return b_rsem.at[NB + j // 2] if part == 1 else b_rsem.at[j]

    def relay_copy(j, part):
        return remote(part_of(hall, NA + j, part), part_of(hall, 2 * NA + j, part), b_ssem, b_sem(j, part), x_next)

    def back_copy(j, part):
        return remote(part_of(hall, 2 * NA + j, part), part_of(hall, 2 * NA + j, part), b_ssem, b_sem(j, part), y_next)

    def make_h(j, part, first):
        with jax.named_scope('x_wait'):
            x_copy_of(j, part, 0).wait_recv()
        if part == 2:
            rows, chunks = pl.ds(0, rows_a + rows_b), (j,)
        elif part == 0:
            rows, chunks = row_group[0], (j,)
        else:
            rows, chunks = row_group[1], (j, j + 1)
        for c in chunks:
            total = own[first + c, rows, :] + x_recv[c, rows, :]
            hall[c, rows, :] = jax.nn.gelu(total, approximate=True).astype(BF16)
        y_copy(j, part).start()

    def make_h_c(j):
        with jax.named_scope('c_wait'):
            c_copy(j, 2).wait_recv()
            c_relay(j).wait_recv()
        hall[c0 + j] = jax.nn.gelu(c_recv[0, j] + c_recv[1, j], approximate=True).astype(BF16)
        y_copy(c0 + j, 2).start()

    def down(slot, i, part):
        if part == 2:
            acc[...] += jnp.dot(hall[slot], w_out_v[i], preferred_element_type=F32)
        elif part == 0:
            rows = row_group[0]
            acc[rows, :] += jnp.dot(hall[slot, rows, :], w_out_v[i], preferred_element_type=F32)
        else:
            rows = row_group[1]
            acc[rows, :] += (jnp.dot(hall[slot, rows, :], w_out_v[i], preferred_element_type=F32)
                             + jnp.dot(hall[slot + 1, rows, :], w_out_v[i + 1], preferred_element_type=F32))

    e_recv, f_send, f_recv = (ea_recv, eb_recv), (fa_send, fb_send), (fa_recv, fb_recv)

    def token_rows(group, r):
        n, base = ((TA, 0), (tb, rows_a))[group]
        return pl.ds(pl.multiple_of(base + n * r, 8), n)

    def e_copy(group, s):
        r = 2 * (s * x + (1 - s) * (1 - x)) + 1 - k
        return remote(acc.at[token_rows(group, r)], e_recv[group].at[s], e_ssem, e_rsem.at[2 * group + s], sibling)

    def f_copy(group):
        return remote(f_send[group], f_recv[group], f_ssem, f_rsem.at[group], x_next)

    def end_start(group):
        e_copy(group, 0).start()
        e_copy(group, 1).start()

    def end_send(group):
        with jax.named_scope('e0_wait'):
            e_copy(group, 0).wait_recv()
        f_send[group][...] = acc[token_rows(group, 2 * (1 - x) + k), :] + e_recv[group][0]
        f_copy(group).start()

    def end_sum(group):
        with jax.named_scope('e1_wait'):
            e_copy(group, 1).wait_recv()
        with jax.named_scope('f_wait'):
            f_copy(group).wait_recv()
        total = acc[token_rows(group, row), :] + e_recv[group][1] + f_recv[group][...]
        t0, n = ((0, TA), (TA, tb))[group]
        out_v[t0:t0 + n, :] = ((xa_v, xb_v)[group][...].astype(F32) + total).astype(BF16)

    def loop(lo, hi, step):
        def body(i, _):
            step(i)
            return 0
        lax.fori_loop(lo, hi, body, 0)

    @pl.when(home == 1)
    def _():
        def relay(i, part):
            with jax.named_scope('relay_wait'):
                y_copy(i, part).wait_recv()
            relay_copy(i, part).start()

        def b_step(i, part):
            with jax.named_scope('b_wait'):
                back_copy(i, part).wait_recv()
            down(2 * NA + i, i, part)

        def c_step(i):
            with jax.named_scope('ch_wait'):
                y_copy(c0 + i, 2).wait_recv()
            down(NA + c0 + i, c0 + i, 2)

        def a_step(j, part):
            make_h(j, part, a0)
            down(j, a0 + j, part)

        pass_c(1)
        loop(0, NF, lambda j: a_step(j, 2))

        def step(j):
            for t, i in ((3, 2), (5, 3), (6, 4)):
                @pl.when(j == t)
                def _():
                    pass_c(i)
            a_step(j, 0)

        loop(NF, 8, step)

        def step(t):
            relay(2 * t, 0)
            relay(2 * t + 1, 0)

            @pl.when(t == 1)
            def _():
                relay(0, 1)
                relay(2, 1)
            a_step(8 + t, 0)

        loop(0, 2, step)
        c_step(0)
        a_step(10, 0)
        loop(1, 3, c_step)
        a_step(NF, 1)
        c_step(3)
        a_step(NF + 2, 1)
        make_h(NF + 4, 1, a0)
        c_step(4)
        loop(0, 2, lambda i: b_step(i, 0))
        make_h(NF + 6, 1, a0)
        loop(2, 4, lambda i: b_step(i, 0))
        end_start(0)
        loop(2, 4, lambda m: down(NF + 2 * m, a0 + NF + 2 * m, 1))
        end_send(0)
        loop(0, 2, lambda m: b_step(2 * m, 1))

    @pl.when(home == 0)
    def _():
        def a_step(j, part):
            with jax.named_scope('a_wait'):
                y_copy(j, part).wait_recv()
            down(NA + j, a0 + j, part)

        def b_step(i, part):
            with jax.named_scope('b_wait'):
                relay_copy(i, part).wait_recv()
            back_copy(i, part).start()
            down(2 * NA + i, i, part)

        def c_step(i):
            make_h_c(i)
            down(c0 + i, c0 + i, 2)

        loop(0, NB, lambda j: make_h(j, 0, 0))
        loop(0, NB // 2, lambda m: make_h(2 * m, 1, 0))
        c_step(0)
        a_step(0, 2)
        c_step(1)
        loop(1, NF, lambda j: a_step(j, 2))

        def step(t):
            c_step(2 + t)
            loop(NF + 3 * t, NF + 3 * t + 3, lambda j: a_step(j, 0))

        loop(0, 2, step)
        c_step(4)

        def step(t):
            b_step(2 * t, 0)
            a_step(NF + 6 + t, 0)
            b_step(2 * t + 1, 0)

        loop(0, 2, step)
        end_start(0)

        def step(t):
            b_step(2 * t, 1)
            a_step(NF + 2 * t, 1)

            @pl.when(t == 0)
            def _():
                end_send(0)

        loop(0, 2, step)
        loop(2, 4, lambda m: a_step(NF + 2 * m, 1))

    end_start(1)
    end_send(1)

    def sent(ref, sem):
        remote(ref, ref, sem, sem, y_next).wait_send()

    with jax.named_scope('drain'):
        sent(stat_g.at[pl.ds(0, 7)], stat_ssem)
        sent(d_send, d_ssem)
        sent(hall.at[pl.ds(0, NB)], b_ssem)
        sent(c_recv.at[0], c_ssem)
        sent(ea_recv, e_ssem)
        sent(eb_recv, e_ssem)

        @pl.when(home == 0)
        def _():
            sent(x_ga, z_ssem)
            sent(x_gb, z_ssem)
            sent(own.at[pl.ds(0, NA)], x_ssem)
            sent(hall.at[pl.ds(0, NB + NC)], y_ssem)

        @pl.when(home == 1)
        def _():
            gain_cp.wait_send()
            sent(x_ga.at[pl.ds(0, 3)], z_ssem)
            sent(x_gb, z_ssem)
            sent(x_gb.at[0], z_ssem)
            sent(own.at[pl.ds(0, NB)], x_ssem)
            sent(c_recv.at[1], c_ssem)
            sent(hall.at[pl.ds(0, NA)], y_ssem)

    end_sum(0)
    end_sum(1)
    sent(fa_send, f_ssem)
    sent(fb_send, f_ssem)


def solution(mesh):
    def body(x_blk, gain_blk, w_in_blk, w_out_blk):
        tok, half = x_blk.shape
        feat = w_in_blk.shape[0]
        tokens = 4 * tok
        dma = pltpu.SemaphoreType.DMA
        return pl.pallas_call(
            kernel,
            out_shape=pltpu.VMEM((tok, half), BF16),
            in_specs=[pl.BlockSpec(memory_space=pl.ANY)] * 4,
            out_specs=pl.BlockSpec(memory_space=pltpu.VMEM),
            scratch_shapes=[
                pltpu.VMEM((TA, half), BF16),
                pltpu.VMEM((tok - TA, half), BF16),
                pltpu.VMEM((2, half), F32),
                pltpu.VMEM((8, 8, 128), F32),
                pltpu.VMEM((4, TA, feat), BF16),
                pltpu.VMEM((4, tok - TA, feat), BF16),
                pltpu.VMEM((2, tok - TA, feat), BF16),
                pltpu.VMEM((tokens, feat), BF16),
                pltpu.VMEM((N, feat, 2 * C), BF16),
                pltpu.VMEM((N, C, half), BF16),
                pltpu.VMEM((N, tokens, C), F32),
                pltpu.VMEM((N, tokens, C), F32),
                pltpu.VMEM((N, tokens, C), F32),
                pltpu.VMEM((NA, tokens, C), F32),
                pltpu.VMEM((2, NC, tokens, C), F32),
                pltpu.VMEM((2 * NA + NB, tokens, C), BF16),
                pltpu.VMEM((tokens, half), F32),
                pltpu.VMEM((2, TA, half), F32),
                pltpu.VMEM((2, tok - TA, half), F32),
                pltpu.VMEM((TA, half), F32),
                pltpu.VMEM((TA, half), F32),
                pltpu.VMEM((tok - TA, half), F32),
                pltpu.VMEM((tok - TA, half), F32),
                dma((10,)),
                dma((N // GROUP,)),
                dma((9,)),
                dma((RING,)),
                dma((NA + NA // 2,)),
                dma((NA + NA // 2,)),
                dma((NB + NB // 2,)),
                dma((2 * NC,)),
                dma((4,)),
                dma((2,)),
            ],
            compiler_params=pltpu.CompilerParams(
                collective_id=0, has_side_effects=True, vmem_limit_bytes=66_500_000
            ),
        )(x_blk, gain_blk, w_in_blk, w_out_blk)

    return jax.shard_map(
        body,
        mesh=mesh,
        in_specs=(P(("dp", "row"), "col"), P("col"), P("row", "col"), P("row", "col")),
        out_specs=P(("dp", "row"), "col"),
        check_vma=False,
    )
```

```python
import jax
import jax.numpy as jnp
from jax import lax
from jax.experimental import pallas as pl
from jax.experimental.pallas import tpu as pltpu
from jax.sharding import PartitionSpec as P

NORM_EPS = 1e-5
MESH = pl.DeviceIdType.MESH
WHOLE, FIRST = -1, 0
F32 = jnp.float32
BF16 = jnp.bfloat16

C = 256
NB = 4
NC = 5
NA = 11
N = NA + NB + NC
NF = 3
GROUP = 5
RING = 8
TA = 16


def kernel(x_hbm, gain_hbm, w_in_hbm, w_out_hbm, out_v,
           xa_v, xb_v, gain_v, stat_g, x_ga, x_gb, x_relay, z_v, w_in_v, w_out_v, d_send, d_recv, own, x_recv, c_recv, hall,
           acc, ea_recv, eb_recv, fa_send, fa_recv, fb_send, fb_recv,
           misc_sem, w_in_sem, send_sem, d_rsem, x_rsem, y_rsem, b_rsem, c_rsem, e_rsem, f_rsem):
    w_out_sem, stat_rsem, za_rsem, zb_rsem = [misc_sem.at[i] for i in range(4, 8)]
    stat_ssem, z_ssem, d_ssem, x_ssem, y_ssem, b_ssem, c_ssem, e_ssem, f_ssem = [send_sem.at[i] for i in range(9)]
    y = lax.axis_index("col")
    row = lax.axis_index("row")
    x = row // 2
    k = row % 2
    dp = lax.axis_index("dp")
    home = 1 - (x + y) % 2
    tok, half = out_v.shape
    feat = half // 2
    block = N * C
    rows_a = 4 * TA
    tb = tok - TA
    rows_b = 4 * tb
    sibling = (dp, y, 2 * x + 1 - k)
    x_next = (dp, y, 2 * (1 - x) + k)
    y_next = (dp, 1 - y, row)

    def remote(src, dst, ssem, rsem, dev):
        return pltpu.make_async_remote_copy(src_ref=src, dst_ref=dst, send_sem=ssem, recv_sem=rsem,
                                            device_id=dev, device_id_type=MESH)

    c0, a0 = NB, NB + NC

    def chunk_of(p):
        u = p - 2 * NB - 1
        pair = jnp.where(p % 2 == 1, c0 + p // 2, p // 2 + (1 - home) * a0)
        mixed = jnp.where(u % 2 == 1, u // 2, a0 + NB + u // 2)
        late = jnp.where((home == 1) | (u >= 2 * NB), a0 + u, mixed)
        return jnp.where(p < 2 * NB, pair, jnp.where(u < 0, a0 - 1, late))

    def w_in_copies(p):
        c = C * chunk_of(p)
        cs = pl.multiple_of((1 - k) * block + c, C)
        co = pl.multiple_of(k * block + c, C)
        return (pltpu.make_async_copy(w_in_hbm.at[:, pl.ds(cs, C)], w_in_v.at[p, :, pl.ds(0, C)], w_in_sem.at[p // GROUP]),
                pltpu.make_async_copy(w_in_hbm.at[:, pl.ds(co, C)], w_in_v.at[p, :, pl.ds(C, C)], w_in_sem.at[p // GROUP]))

    def w_out_copy(i):
        r = pl.multiple_of(i * C, C)
        return pltpu.make_async_copy(w_out_hbm.at[pl.ds(r, C), :], w_out_v.at[i], w_out_sem)

    xa_copy = pltpu.make_async_copy(x_hbm.at[pl.ds(0, TA)], xa_v, misc_sem.at[0])
    xb_copy = pltpu.make_async_copy(x_hbm.at[pl.ds(TA, tb)], xb_v, misc_sem.at[8])
    g_copy = pltpu.make_async_copy(gain_hbm, gain_v.at[0], misc_sem.at[1])
    xa_copy.start()
    xb_copy.start()
    g_copy.start()

    barrier = pltpu.get_barrier_semaphore()
    for dy in range(2):
        for dr in range(4):
            if dy or dr:
                pl.semaphore_signal(barrier, inc=1, device_id=(dp, (y + dy) % 2, (row + dr) % 4), device_id_type=MESH)

    def start_w_in(p, _):
        for cp in w_in_copies(p):
            cp.start()
        return 0

    lax.fori_loop(0, N, start_w_in, 0)

    xa_copy.wait()
    xb_copy.wait()
    g_copy.wait()

    def row_sums(ref):
        v = ref[...].astype(F32)
        lane = lax.broadcasted_iota(jnp.int32, (v.shape[0], 128), 1)
        return jnp.where(lane == 0, jnp.sum(v, axis=1, keepdims=True), jnp.sum(v * v, axis=1, keepdims=True))

    me = 4 * y + row
    stat_g[me, :, :tok] = jnp.transpose(jnp.concatenate([row_sums(xa_v), row_sums(xb_v)], axis=0))[:8]
    with jax.named_scope('barrier'):
        pl.semaphore_wait(barrier, 7)

    def tok_copy(group, dy, dk):
        tk = (k + dk) % 2
        cols = pl.ds(pl.multiple_of(feat * tk, 128), feat)
        src, dst, sem = ((xa_v, x_ga, za_rsem), (xb_v, x_gb, zb_rsem))[group]
        return remote(src.at[:, cols], dst.at[row], z_ssem, sem, (dp, (y + dy) % 2, 2 * y + tk))

    def stat_copy(d):
        ty = (y + d // 4) % 2
        tr = (row + d % 4) % 4
        return remote(stat_g.at[me], stat_g.at[me], stat_ssem, stat_rsem, (dp, ty, tr))

    gain_cp = remote(gain_v.at[0], gain_v.at[1], misc_sem.at[2], misc_sem.at[3], y_next)
    def to_relay(tk):
        return remote(xb_v.at[:, pl.ds(feat * tk, feat)], x_relay.at[tk], z_ssem, misc_sem.at[9], y_next)

    def from_relay(tk):
        return remote(x_relay.at[tk], x_gb.at[row], z_ssem, zb_rsem, (dp, y, 2 * (1 - x) + tk))

    for d in range(1, 8):
        stat_copy(d).start()

    @pl.when(home == 0)
    def _():
        to_relay(0).start()
        to_relay(1).start()
        tok_copy(0, 1, 0).start()
        tok_copy(0, 1, 1).start()
        for group in range(2):
            tok_copy(group, 0, 0).start()
            tok_copy(group, 0, 1).start()

    @pl.when(home == 1)
    def _():
        gain_cp.start()
        for group in range(2):
            tok_copy(group, 0, 1).start()
            tok_copy(group, 1, 0).start()
            tok_copy(group, 1, 1).start()
        x_ga[row] = jnp.where(k == 0, xa_v[:, :feat], xa_v[:, feat:])
        x_gb[row] = jnp.where(k == 0, xb_v[:, :feat], xb_v[:, feat:])
        gain_v[1] = gain_v[0]
        with jax.named_scope('x_relay_wait'):
            remote(x_relay, x_relay, z_ssem, misc_sem.at[9], y_next).wait_recv()
        from_relay(0).start()
        from_relay(1).start()

    @pl.when(home == 0)
    def _():
        with jax.named_scope('gain_wait'):
            gain_cp.wait_recv()
    gain = jnp.where(k == 0, gain_v[1, :feat], gain_v[1, feat:]).reshape(1, feat)
    acc[...] = jnp.zeros_like(acc)
    with jax.named_scope('stat_wait'):
        remote(stat_g.at[pl.ds(0, 7)], stat_g.at[pl.ds(0, 7)], stat_ssem, stat_rsem, y_next).wait_recv()

    def make_z(group):
        ref, sem = ((x_ga, za_rsem), (x_gb, zb_rsem))[group]

        @pl.when(home == 0)
        def _():
            with jax.named_scope('z_wait'):
                remote(ref, ref, z_ssem, sem, y_next).wait_recv()

        @pl.when(home == 1)
        def _():
            with jax.named_scope('z_wait'):
                remote(ref.at[pl.ds(0, 3)], ref.at[pl.ds(0, 3)], z_ssem, sem, y_next).wait_recv()

        t0, n, base = ((0, TA, 0), (TA, tb, rows_a))[group]
        for src in range(4):
            st = jnp.transpose(stat_g[src] + stat_g[4 + src])[t0:t0 + n] * (1.0 / (2 * half))
            mean = st[:, 0:1]
            var = st[:, 1:2] - mean * mean
            z = (ref[src].astype(F32) - mean) * lax.rsqrt(var + NORM_EPS) * gain
            z_v[pl.ds(base + n * src, n), :] = z.astype(BF16)

    row_group = (pl.ds(0, rows_a), pl.ds(rows_a, rows_b))

    def part_of(ref, j, part):
        if part == WHOLE:
            return ref.at[j]
        if part == FIRST:
            return ref.at[j, row_group[0]]
        return ref.at[pl.ds(j, part), row_group[1]]

    def d_copy(p):
        return remote(d_send.at[p], d_recv.at[p], d_ssem, d_rsem.at[p % RING], sibling)

    def x_copy_of(j, part, first):
        sem = x_rsem.at[NA + j // 2] if part > 0 else x_rsem.at[j]
        return remote(part_of(own, first + j, part), part_of(x_recv, j, part), x_ssem, sem, x_next)

    def c_copy(j):
        return remote(own.at[c0 + j], c_recv.at[0, j], c_ssem, c_rsem.at[j], y_next)

    def c_relay(j, part):
        sem = c_rsem.at[2 * NC + j // 3] if part > 0 else c_rsem.at[NC + j]
        return remote(part_of(c_recv.at[0], j, part), part_of(c_recv.at[1], j, part), c_ssem, sem, x_next)

    def pass_c(j):
        with jax.named_scope('c_wait'):
            c_copy(j).wait_recv()
        c_relay(j, FIRST).start()

    def up(p):
        sums = jnp.dot(z_v[...], w_in_v[p], preferred_element_type=F32)
        d_send[p] = sums[:, :C]
        own[chunk_of(p)] = sums[:, C:]
        d_copy(p).start()

    def pair_sum(p):
        with jax.named_scope('pair_wait'):
            d_copy(p).wait_recv()
        q = chunk_of(p)
        own[q] = own[q] + d_recv[p]

        @pl.when((q >= c0) & (q < a0))
        def _():
            c_copy(q - c0).start()

        @pl.when((home == 1) & (q < c0))
        def _():
            x_copy_of(q, FIRST, 0).start()

            @pl.when(q % 2 == 1)
            def _():
                x_copy_of(q - 1, 2, 0).start()

        @pl.when((home == 0) & (q >= a0 + NF))
        def _():
            x_copy_of(q - a0, FIRST, a0).start()

        @pl.when((home == 0) & (q >= a0) & (q < a0 + NF))
        def _():
            x_copy_of(q - a0, WHOLE, a0).start()

    def up_step(p, _):
        @pl.when(p % GROUP == 0)
        def _():
            with jax.named_scope('w_in_wait'):
                group = w_in_v.at[pl.ds(p, GROUP)]
                pltpu.make_async_copy(group, group, w_in_sem.at[p // GROUP]).wait()
        up(p)
        w_out_copy(p).start()

        @pl.when(p >= 2)
        def _():
            pair_sum(p - 2)

        @pl.when((p == 13) & (home == 1))
        def _():
            pass_c(0)

        @pl.when((p == 18) & (home == 1))
        def _():
            pass_c(1)
        return 0

    make_z(0)
    make_z(1)
    lax.fori_loop(0, N, up_step, 0)
    pair_sum(N - 2)
    pair_sum(N - 1)

    @pl.when(home == 0)
    def _():
        for j in range(NF, NA, 2):
            x_copy_of(j, 2, a0).start()

    with jax.named_scope('w_out_wait'):
        pltpu.make_async_copy(w_out_v, w_out_v, w_out_sem).wait()

    def y_copy(j, part):
        sem = y_rsem.at[NA + j // 2] if part > 0 else y_rsem.at[j]
        return remote(part_of(hall, j, part), part_of(hall, NA + j, part), y_ssem, sem, y_next)

    def b_sem(j, part):
        return b_rsem.at[NB + j // 2] if part > 0 else b_rsem.at[j]

    def relay_copy(j, part):
        return remote(part_of(hall, NA + j, part), part_of(hall, 2 * NA + j, part), b_ssem, b_sem(j, part), x_next)

    def back_copy(j, part):
        return remote(part_of(hall, 2 * NA + j, part), part_of(hall, 2 * NA + j, part), b_ssem, b_sem(j, part), y_next)

    def rows_of(part):
        return pl.ds(0, rows_a + rows_b) if part == WHOLE else row_group[int(part > 0)]

    def put_h(j, part, left, right):
        rows = rows_of(part)
        for c in range(max(part, 1)):
            total = left(c)[rows, :] + right(c)[rows, :]
            hall[j + c, rows, :] = jax.nn.gelu(total, approximate=True).astype(BF16)

    def make_h(j, part, first):
        with jax.named_scope('x_wait'):
            x_copy_of(j, part, 0).wait_recv()
        put_h(j, part, lambda c: own.at[first + j + c], lambda c: x_recv.at[j + c])
        y_copy(j, part).start()

    def make_h_c(j, part):
        with jax.named_scope('c_wait'):
            if part == FIRST:
                c_copy(j).wait_recv()
            c_relay(j, part).wait_recv()
        put_h(c0 + j, part, lambda c: c_recv.at[0, j + c], lambda c: c_recv.at[1, j + c])
        yc_copy(j, part).start()

    def yc_copy(j, part):
        sem = y_rsem.at[NA + 2 + j // 3] if part > 0 else y_rsem.at[c0 + j]
        return remote(part_of(hall, c0 + j, part), part_of(hall, NA + c0 + j, part), y_ssem, sem, y_next)

    def down(slot, i, part):
        rows = rows_of(part)
        parts = [jnp.dot(hall[slot + c, rows, :], w_out_v[i + c], preferred_element_type=F32)
                 for c in range(max(part, 1))]
        acc[rows, :] += sum(parts[1:], parts[0])

    e_recv, f_send, f_recv = (ea_recv, eb_recv), (fa_send, fb_send), (fa_recv, fb_recv)

    def token_rows(group, r):
        n, base = ((TA, 0), (tb, rows_a))[group]
        return pl.ds(pl.multiple_of(base + n * r, 8), n)

    def e_copy(group, s):
        r = 2 * (s * x + (1 - s) * (1 - x)) + 1 - k
        return remote(acc.at[token_rows(group, r)], e_recv[group].at[s], e_ssem, e_rsem.at[2 * group + s], sibling)

    def f_copy(group):
        return remote(f_send[group], f_recv[group], f_ssem, f_rsem.at[group], x_next)

    def end_start(group):
        e_copy(group, 0).start()
        e_copy(group, 1).start()

    def end_send(group):
        with jax.named_scope('e0_wait'):
            e_copy(group, 0).wait_recv()
        f_send[group][...] = acc[token_rows(group, 2 * (1 - x) + k), :] + e_recv[group][0]
        f_copy(group).start()

    def end_sum(group):
        with jax.named_scope('e1_wait'):
            e_copy(group, 1).wait_recv()
        with jax.named_scope('f_wait'):
            f_copy(group).wait_recv()
        total = acc[token_rows(group, row), :] + e_recv[group][1] + f_recv[group][...]
        t0, n = ((0, TA), (TA, tb))[group]
        out_v[t0:t0 + n, :] = ((xa_v, xb_v)[group][...].astype(F32) + total).astype(BF16)

    def loop(lo, hi, step):
        def body(i, _):
            step(i)
            return 0
        lax.fori_loop(lo, hi, body, 0)

    @pl.when(home == 1)
    def _():
        def relay(i, part):
            with jax.named_scope('relay_wait'):
                y_copy(i, part).wait_recv()
            relay_copy(i, part).start()

        def b_step(i, part):
            with jax.named_scope('b_wait'):
                back_copy(i, part).wait_recv()
            down(2 * NA + i, i, part)

        def c_step(i, part):
            with jax.named_scope('ch_wait'):
                yc_copy(i, part).wait_recv()
            down(NA + c0 + i, c0 + i, part)

        def a_step(j, part):
            make_h(j, part, a0)
            down(j, a0 + j, part)

        loop(0, NF, lambda j: a_step(j, WHOLE))

        def step(j):
            for t, i in ((3, 2), (4, 3), (6, 4)):
                @pl.when(j == t)
                def _():
                    pass_c(i)

            @pl.when(j == 7)
            def _():
                relay(0, FIRST)
                relay(1, FIRST)

            @pl.when(j == 8)
            def _():
                relay(2, FIRST)
                relay(3, FIRST)
                c_relay(0, 3).start()
                c_relay(3, 2).start()
                relay(0, 2)
                relay(2, 2)
            a_step(j, FIRST)

        loop(NF, 9, step)

        def step(t):
            c_step(2 * t, FIRST)
            a_step(9 + t, FIRST)
            c_step(2 * t + 1, FIRST)

        loop(0, 2, step)
        c_step(4, FIRST)

        def step(t):
            a_step(NF + 2 * t, 2)
            b_step(2 * t, FIRST)
            b_step(2 * t + 1, FIRST)

        loop(0, 2, step)
        end_start(0)
        a_step(NF + 4, 2)
        end_send(0)
        a_step(NF + 6, 2)
        c_step(0, 3)
        c_step(3, 2)
        loop(0, 2, lambda m: b_step(2 * m, 2))

    @pl.when(home == 0)
    def _():
        def a_step(j, part):
            with jax.named_scope('a_wait'):
                y_copy(j, part).wait_recv()
            down(NA + j, a0 + j, part)

        def b_step(i, part):
            with jax.named_scope('b_wait'):
                relay_copy(i, part).wait_recv()
            back_copy(i, part).start()
            down(2 * NA + i, i, part)

        def c_step(i, part):
            make_h_c(i, part)
            down(c0 + i, c0 + i, part)

        loop(0, NB, lambda j: make_h(j, FIRST, 0))
        loop(0, NB // 2, lambda m: make_h(2 * m, 2, 0))
        c_step(0, FIRST)

        def step(t):
            c_step(1 + t, FIRST)
            a_step(t, WHOLE)

        loop(0, NF, step)
        a_step(NF, FIRST)
        c_step(4, FIRST)

        def step(t):
            a_step(NF + 1 + t, FIRST)
            b_step(t, FIRST)

        loop(0, 4, step)
        loop(NF + 5, NA, lambda j: a_step(j, FIRST))
        end_start(0)
        c_step(0, 3)
        end_send(0)
        c_step(3, 2)

        def step(t):
            b_step(2 * t, 2)
            a_step(NF + 2 * t, 2)

        loop(0, 2, step)
        loop(2, 4, lambda m: a_step(NF + 2 * m, 2))

    end_start(1)
    end_send(1)

    def sent(ref, sem):
        remote(ref, ref, sem, sem, y_next).wait_send()

    with jax.named_scope('drain'):
        sent(stat_g.at[pl.ds(0, 7)], stat_ssem)
        sent(d_send, d_ssem)
        sent(hall.at[pl.ds(0, NB)], b_ssem)
        sent(c_recv.at[0], c_ssem)
        sent(ea_recv, e_ssem)
        sent(eb_recv, e_ssem)

        @pl.when(home == 0)
        def _():
            sent(x_ga, z_ssem)
            sent(x_gb, z_ssem)
            sent(own.at[pl.ds(0, NA)], x_ssem)
            sent(hall.at[pl.ds(0, NB + NC)], y_ssem)

        @pl.when(home == 1)
        def _():
            gain_cp.wait_send()
            sent(x_ga.at[pl.ds(0, 3)], z_ssem)
            sent(x_gb, z_ssem)
            sent(x_gb.at[0], z_ssem)
            sent(own.at[pl.ds(0, NB)], x_ssem)
            sent(c_recv.at[1], c_ssem)
            sent(hall.at[pl.ds(0, NA)], y_ssem)

    end_sum(0)
    end_sum(1)
    sent(fa_send, f_ssem)
    sent(fb_send, f_ssem)


def solution(mesh):
    def body(x_blk, gain_blk, w_in_blk, w_out_blk):
        tok, half = x_blk.shape
        feat = w_in_blk.shape[0]
        tokens = 4 * tok
        dma = pltpu.SemaphoreType.DMA
        return pl.pallas_call(
            kernel,
            out_shape=pltpu.VMEM((tok, half), BF16),
            in_specs=[pl.BlockSpec(memory_space=pl.ANY)] * 4,
            out_specs=pl.BlockSpec(memory_space=pltpu.VMEM),
            scratch_shapes=[
                pltpu.VMEM((TA, half), BF16),
                pltpu.VMEM((tok - TA, half), BF16),
                pltpu.VMEM((2, half), F32),
                pltpu.VMEM((8, 8, 128), F32),
                pltpu.VMEM((4, TA, feat), BF16),
                pltpu.VMEM((4, tok - TA, feat), BF16),
                pltpu.VMEM((2, tok - TA, feat), BF16),
                pltpu.VMEM((tokens, feat), BF16),
                pltpu.VMEM((N, feat, 2 * C), BF16),
                pltpu.VMEM((N, C, half), BF16),
                pltpu.VMEM((N, tokens, C), F32),
                pltpu.VMEM((N, tokens, C), F32),
                pltpu.VMEM((N, tokens, C), F32),
                pltpu.VMEM((NA, tokens, C), F32),
                pltpu.VMEM((2, NC, tokens, C), F32),
                pltpu.VMEM((2 * NA + NB, tokens, C), BF16),
                pltpu.VMEM((tokens, half), F32),
                pltpu.VMEM((2, TA, half), F32),
                pltpu.VMEM((2, tok - TA, half), F32),
                pltpu.VMEM((TA, half), F32),
                pltpu.VMEM((TA, half), F32),
                pltpu.VMEM((tok - TA, half), F32),
                pltpu.VMEM((tok - TA, half), F32),
                dma((10,)),
                dma((N // GROUP,)),
                dma((9,)),
                dma((RING,)),
                dma((NA + NA // 2,)),
                dma((NA + NA // 2,)),
                dma((NB + NB // 2,)),
                dma((2 * NC + 2,)),
                dma((4,)),
                dma((2,)),
            ],
            compiler_params=pltpu.CompilerParams(
                collective_id=0, has_side_effects=True, vmem_limit_bytes=66_500_000
            ),
        )(x_blk, gain_blk, w_in_blk, w_out_blk)

    return jax.shard_map(
        body,
        mesh=mesh,
        in_specs=(P(("dp", "row"), "col"), P("col"), P("row", "col"), P("row", "col")),
        out_specs=P(("dp", "row"), "col"),
        check_vma=False,
    )
```

```python
import jax
import jax.numpy as jnp
from jax import lax
from jax.experimental import pallas as pl
from jax.experimental.pallas import tpu as pltpu
from jax.sharding import PartitionSpec as P

NORM_EPS = 1e-5
MESH = pl.DeviceIdType.MESH
WHOLE, FIRST = -1, 0
F32 = jnp.float32
BF16 = jnp.bfloat16

C = 256
NB = 4
NC = 5
NA = 11
N = NA + NB + NC
NF = 3
GROUP = 5
RING = 8
TA = 16


def kernel(x_hbm, gain_hbm, w_in_hbm, w_out_hbm, out_v,
           xa_v, xb_v, gain_v, stat_g, x_ga, x_gb, x_relay, z_v, w_in_v, w_out_v, d_send, d_recv, own, x_recv, c_recv, hall,
           acc, ea_recv, eb_recv, fa_send, fa_recv, fb_send, fb_recv,
           misc_sem, w_in_sem, send_sem, d_rsem, x_rsem, y_rsem, b_rsem, c_rsem, e_rsem, f_rsem):
    w_out_sem, stat_rsem, za_rsem, zb_rsem = [misc_sem.at[i] for i in range(4, 8)]
    stat_ssem, z_ssem, d_ssem, x_ssem, y_ssem, b_ssem, c_ssem, e_ssem, f_ssem = [send_sem.at[i] for i in range(9)]
    y = lax.axis_index("col")
    row = lax.axis_index("row")
    x = row // 2
    k = row % 2
    dp = lax.axis_index("dp")
    home = 1 - (x + y) % 2
    tok, half = out_v.shape
    feat = half // 2
    block = N * C
    rows_a = 4 * TA
    tb = tok - TA
    rows_b = 4 * tb
    sibling = (dp, y, 2 * x + 1 - k)
    x_next = (dp, y, 2 * (1 - x) + k)
    y_next = (dp, 1 - y, row)

    def remote(src, dst, ssem, rsem, dev):
        return pltpu.make_async_remote_copy(src_ref=src, dst_ref=dst, send_sem=ssem, recv_sem=rsem,
                                            device_id=dev, device_id_type=MESH)

    c0, a0 = NB, NB + NC

    def chunk_of(p):
        u = p - 2 * NB - 1
        pair = jnp.where(p % 2 == 1, c0 + p // 2, p // 2 + (1 - home) * a0)
        mixed = jnp.where(u % 2 == 1, u // 2, a0 + NB + u // 2)
        late = jnp.where((home == 1) | (u >= 2 * NB), a0 + u, mixed)
        return jnp.where(p < 2 * NB, pair, jnp.where(u < 0, a0 - 1, late))

    def w_in_copies(p):
        c = C * chunk_of(p)
        cs = pl.multiple_of((1 - k) * block + c, C)
        co = pl.multiple_of(k * block + c, C)
        return (pltpu.make_async_copy(w_in_hbm.at[:, pl.ds(cs, C)], w_in_v.at[p, :, pl.ds(0, C)], w_in_sem.at[p // GROUP]),
                pltpu.make_async_copy(w_in_hbm.at[:, pl.ds(co, C)], w_in_v.at[p, :, pl.ds(C, C)], w_in_sem.at[p // GROUP]))

    def w_out_copy(i):
        r = pl.multiple_of(i * C, C)
        return pltpu.make_async_copy(w_out_hbm.at[pl.ds(r, C), :], w_out_v.at[i], w_out_sem)

    xa_copy = pltpu.make_async_copy(x_hbm.at[pl.ds(0, TA)], xa_v, misc_sem.at[0])
    xb_copy = pltpu.make_async_copy(x_hbm.at[pl.ds(TA, tb)], xb_v, misc_sem.at[8])
    g_copy = pltpu.make_async_copy(gain_hbm, gain_v.at[0], misc_sem.at[1])
    xa_copy.start()
    xb_copy.start()
    g_copy.start()

    barrier = pltpu.get_barrier_semaphore()
    for dy in range(2):
        for dr in range(4):
            if dy or dr:
                pl.semaphore_signal(barrier, inc=1, device_id=(dp, (y + dy) % 2, (row + dr) % 4), device_id_type=MESH)

    def start_w_in(p, _):
        for cp in w_in_copies(p):
            cp.start()
        return 0

    lax.fori_loop(0, N, start_w_in, 0)

    xa_copy.wait()
    xb_copy.wait()
    g_copy.wait()

    def row_sums(ref):
        v = ref[...].astype(F32)
        lane = lax.broadcasted_iota(jnp.int32, (v.shape[0], 128), 1)
        return jnp.where(lane == 0, jnp.sum(v, axis=1, keepdims=True), jnp.sum(v * v, axis=1, keepdims=True))

    me = 4 * y + row
    with jax.named_scope('barrier'):
        pl.semaphore_wait(barrier, 7)

    def tok_copy(group, dy, dk):
        tk = (k + dk) % 2
        cols = pl.ds(pl.multiple_of(feat * tk, 128), feat)
        src, dst, sem = ((xa_v, x_ga, za_rsem), (xb_v, x_gb, zb_rsem))[group]
        return remote(src.at[:, cols], dst.at[row], z_ssem, sem, (dp, (y + dy) % 2, 2 * y + tk))

    def stat_copy(d):
        ty = (y + d // 4) % 2
        tr = (row + d % 4) % 4
        return remote(stat_g.at[me], stat_g.at[me], stat_ssem, stat_rsem, (dp, ty, tr))

    gain_cp = remote(gain_v.at[0], gain_v.at[1], misc_sem.at[2], misc_sem.at[3], y_next)
    def to_relay(tk):
        return remote(xb_v.at[:, pl.ds(feat * tk, feat)], x_relay.at[tk], z_ssem, misc_sem.at[9], y_next)

    def from_relay(tk):
        return remote(x_relay.at[tk], x_gb.at[row], z_ssem, zb_rsem, (dp, y, 2 * (1 - x) + tk))

    @pl.when(home == 0)
    def _():
        to_relay(0).start()
        to_relay(1).start()
        tok_copy(0, 1, 0).start()

    @pl.when(home == 1)
    def _():
        gain_cp.start()
        tok_copy(0, 0, 1).start()
        tok_copy(0, 1, 0).start()

    stat_g[me, :, :tok] = jnp.transpose(jnp.concatenate([row_sums(xa_v), row_sums(xb_v)], axis=0))[:8]
    for d in range(1, 8):
        stat_copy(d).start()

    @pl.when(home == 0)
    def _():
        tok_copy(0, 1, 1).start()
        for group in range(2):
            tok_copy(group, 0, 0).start()
            tok_copy(group, 0, 1).start()

    @pl.when(home == 1)
    def _():
        tok_copy(0, 1, 1).start()
        tok_copy(1, 0, 1).start()
        tok_copy(1, 1, 0).start()
        tok_copy(1, 1, 1).start()
        x_ga[row] = jnp.where(k == 0, xa_v[:, :feat], xa_v[:, feat:])
        x_gb[row] = jnp.where(k == 0, xb_v[:, :feat], xb_v[:, feat:])
        gain_v[1] = gain_v[0]
        with jax.named_scope('x_relay_wait'):
            remote(x_relay, x_relay, z_ssem, misc_sem.at[9], y_next).wait_recv()
        from_relay(0).start()
        from_relay(1).start()

    @pl.when(home == 0)
    def _():
        with jax.named_scope('gain_wait'):
            gain_cp.wait_recv()
    gain = jnp.where(k == 0, gain_v[1, :feat], gain_v[1, feat:]).reshape(1, feat)
    acc[...] = jnp.zeros_like(acc)
    with jax.named_scope('stat_wait'):
        remote(stat_g.at[pl.ds(0, 7)], stat_g.at[pl.ds(0, 7)], stat_ssem, stat_rsem, y_next).wait_recv()

    def make_z(group):
        ref, sem = ((x_ga, za_rsem), (x_gb, zb_rsem))[group]

        @pl.when(home == 0)
        def _():
            with jax.named_scope('z_wait'):
                remote(ref, ref, z_ssem, sem, y_next).wait_recv()

        @pl.when(home == 1)
        def _():
            with jax.named_scope('z_wait'):
                remote(ref.at[pl.ds(0, 3)], ref.at[pl.ds(0, 3)], z_ssem, sem, y_next).wait_recv()

        t0, n, base = ((0, TA, 0), (TA, tb, rows_a))[group]
        for src in range(4):
            st = jnp.transpose(stat_g[src] + stat_g[4 + src])[t0:t0 + n] * (1.0 / (2 * half))
            mean = st[:, 0:1]
            var = st[:, 1:2] - mean * mean
            z = (ref[src].astype(F32) - mean) * lax.rsqrt(var + NORM_EPS) * gain
            z_v[pl.ds(base + n * src, n), :] = z.astype(BF16)

    row_group = (pl.ds(0, rows_a), pl.ds(rows_a, rows_b))

    def part_of(ref, j, part):
        if part == WHOLE:
            return ref.at[j]
        if part == FIRST:
            return ref.at[j, row_group[0]]
        return ref.at[pl.ds(j, part), row_group[1]]

    def rows_of(part):
        return pl.ds(0, rows_a + rows_b) if part == WHOLE else row_group[int(part > 0)]

    def d_copy(p, part, seq):
        return remote(part_of(d_send, p, part), part_of(d_recv, p, part), d_ssem, d_rsem.at[seq % RING], sibling)

    def x_copy_of(j, part, first):
        sem = x_rsem.at[NA + j // 2] if part > 0 else x_rsem.at[j]
        return remote(part_of(own, first + j, part), part_of(x_recv, j, part), x_ssem, sem, x_next)

    def c_copy(j):
        return c_part(j, WHOLE)

    def c_part(j, part):
        return remote(part_of(own, c0 + j, part), part_of(c_recv.at[0], j, part), c_ssem, c_rsem.at[j], y_next)

    def c_relay(j, part):
        sem = c_rsem.at[2 * NC + j // 3] if part > 0 else c_rsem.at[NC + j]
        return remote(part_of(c_recv.at[0], j, part), part_of(c_recv.at[1], j, part), c_ssem, sem, x_next)

    def pass_c(j):
        with jax.named_scope('c_wait'):
            c_copy(j).wait_recv()
        c_relay(j, FIRST).start()

    def up(p, part, seq):
        rows = rows_of(part)
        sums = jnp.dot(z_v[rows, :], w_in_v[p], preferred_element_type=F32)
        d_send[p, rows, :] = sums[:, :C]
        own[chunk_of(p), rows, :] = sums[:, C:]
        d_copy(p, part, seq).start()

    def pair_add(p, part, seq):
        with jax.named_scope('pair_wait'):
            d_copy(p, part, seq).wait_recv()
        q, rows = chunk_of(p), rows_of(part)
        own[q, rows, :] = own[q, rows, :] + d_recv[p, rows, :]

    def wait_w_in(p):
        with jax.named_scope('w_in_wait'):
            group = w_in_v.at[pl.ds(p, GROUP)]
            pltpu.make_async_copy(group, group, w_in_sem.at[p // GROUP]).wait()

    def pair_sum(p):
        pair_add(p, WHOLE, p + 2)
        q = chunk_of(p)

        @pl.when((q >= c0) & (q < a0))
        def _():
            c_copy(q - c0).start()

        @pl.when((home == 1) & (q < c0))
        def _():
            x_copy_of(q, FIRST, 0).start()

            @pl.when(q % 2 == 1)
            def _():
                x_copy_of(q - 1, 2, 0).start()

        @pl.when((home == 0) & (q >= a0 + NF))
        def _():
            x_copy_of(q - a0, FIRST, a0).start()

        @pl.when((home == 0) & (q >= a0) & (q < a0 + NF))
        def _():
            x_copy_of(q - a0, WHOLE, a0).start()

    def up_step(p, _):
        @pl.when(p % GROUP == 0)
        def _():
            wait_w_in(p)
        up(p, WHOLE, p + 2)
        w_out_copy(p).start()

        @pl.when(p >= 4)
        def _():
            pair_sum(p - 2)

        @pl.when((p >= 2) & (p < 4))
        def _():
            pair_add(p - 2, 1, p)

            @pl.when(p == 3)
            def _():
                c_part(0, 1).start()

            @pl.when((p == 2) & (home == 0))
            def _():
                first_b_part().start()

        @pl.when((p == 13) & (home == 1))
        def _():
            pass_c(0)

        @pl.when((p == 18) & (home == 1))
        def _():
            pass_c(1)
        return 0

    def first_b_part():
        return remote(part_of(own, a0, 1), part_of(x_recv, 0, 1), x_ssem, x_rsem.at[0], x_next)

    make_z(0)
    wait_w_in(0)
    up(0, FIRST, 0)
    up(1, FIRST, 1)
    make_z(1)
    up(0, 1, 2)
    w_out_copy(0).start()
    pair_add(0, FIRST, 0)

    @pl.when(home == 1)
    def _():
        x_copy_of(0, FIRST, 0).start()

    @pl.when(home == 0)
    def _():
        x_copy_of(0, FIRST, a0).start()

    up(1, 1, 3)
    w_out_copy(1).start()
    pair_add(1, FIRST, 1)
    c_part(0, FIRST).start()
    lax.fori_loop(2, N, up_step, 0)
    pair_sum(N - 2)
    pair_sum(N - 1)

    @pl.when(home == 0)
    def _():
        for j in range(NF, NA - 2, 2):
            x_copy_of(j, 2, a0).start()
        x_copy_of(NA - 2, 1, a0).start()
        x_copy_of(NA - 1, 1, a0).start()

    with jax.named_scope('w_out_wait'):
        pltpu.make_async_copy(w_out_v, w_out_v, w_out_sem).wait()

    def y_copy(j, part):
        sem = y_rsem.at[NA + j // 2] if part > 0 else y_rsem.at[j]
        return remote(part_of(hall, j, part), part_of(hall, NA + j, part), y_ssem, sem, y_next)

    def b_sem(j, part):
        return b_rsem.at[NB + j // 2] if part > 0 else b_rsem.at[j]

    def relay_copy(j, part):
        return remote(part_of(hall, NA + j, part), part_of(hall, 2 * NA + j, part), b_ssem, b_sem(j, part), x_next)

    def back_copy(j, part):
        return remote(part_of(hall, 2 * NA + j, part), part_of(hall, 2 * NA + j, part), b_ssem, b_sem(j, part), y_next)

    def put_h(j, part, left, right):
        rows = rows_of(part)
        for c in range(max(part, 1)):
            total = left(c)[rows, :] + right(c)[rows, :]
            hall[j + c, rows, :] = jax.nn.gelu(total, approximate=True).astype(BF16)

    def make_h(j, part, first):
        with jax.named_scope('x_wait'):
            x_copy_of(j, part, 0).wait_recv()
        put_h(j, part, lambda c: own.at[first + j + c], lambda c: x_recv.at[j + c])
        y_copy(j, part).start()

    def make_h_c(j, part):
        with jax.named_scope('c_wait'):
            if part == FIRST:
                c_copy(j).wait_recv()
            c_relay(j, part).wait_recv()
        put_h(c0 + j, part, lambda c: c_recv.at[0, j + c], lambda c: c_recv.at[1, j + c])
        yc_copy(j, part).start()

    def yc_copy(j, part):
        sem = y_rsem.at[NA + 2 + j // 3] if part > 0 else y_rsem.at[c0 + j]
        return remote(part_of(hall, c0 + j, part), part_of(hall, NA + c0 + j, part), y_ssem, sem, y_next)

    def down(slot, i, part):
        rows = rows_of(part)
        parts = [jnp.dot(hall[slot + c, rows, :], w_out_v[i + c], preferred_element_type=F32)
                 for c in range(max(part, 1))]
        acc[rows, :] += sum(parts[1:], parts[0])

    e_recv, f_send, f_recv = (ea_recv, eb_recv), (fa_send, fb_send), (fa_recv, fb_recv)

    def token_rows(group, r):
        n, base = ((TA, 0), (tb, rows_a))[group]
        return pl.ds(pl.multiple_of(base + n * r, 8), n)

    def e_copy(group, s):
        r = 2 * (s * x + (1 - s) * (1 - x)) + 1 - k
        return remote(acc.at[token_rows(group, r)], e_recv[group].at[s], e_ssem, e_rsem.at[2 * group + s], sibling)

    def f_copy(group):
        return remote(f_send[group], f_recv[group], f_ssem, f_rsem.at[group], x_next)

    def end_start(group):
        e_copy(group, 0).start()
        e_copy(group, 1).start()

    def end_send(group):
        with jax.named_scope('e0_wait'):
            e_copy(group, 0).wait_recv()
        f_send[group][...] = acc[token_rows(group, 2 * (1 - x) + k), :] + e_recv[group][0]
        f_copy(group).start()

    def end_sum(group):
        with jax.named_scope('e1_wait'):
            e_copy(group, 1).wait_recv()
        with jax.named_scope('f_wait'):
            f_copy(group).wait_recv()
        total = acc[token_rows(group, row), :] + e_recv[group][1] + f_recv[group][...]
        t0, n = ((0, TA), (TA, tb))[group]
        out_v[t0:t0 + n, :] = ((xa_v, xb_v)[group][...].astype(F32) + total).astype(BF16)

    def loop(lo, hi, step):
        def body(i, _):
            step(i)
            return 0
        lax.fori_loop(lo, hi, body, 0)

    @pl.when(home == 1)
    def _():
        def relay(i, part):
            with jax.named_scope('relay_wait'):
                y_copy(i, part).wait_recv()
            relay_copy(i, part).start()

        def b_step(i, part):
            with jax.named_scope('b_wait'):
                back_copy(i, part).wait_recv()
            down(2 * NA + i, i, part)

        def c_step(i, part):
            with jax.named_scope('ch_wait'):
                yc_copy(i, part).wait_recv()
            down(NA + c0 + i, c0 + i, part)

        def a_step(j, part):
            make_h(j, part, a0)
            down(j, a0 + j, part)

        loop(0, NF, lambda j: a_step(j, WHOLE))

        def step(j):
            for t, i in ((3, 2), (4, 3), (6, 4)):
                @pl.when(j == t)
                def _():
                    pass_c(i)

            @pl.when(j == 8)
            def _():
                relay(0, FIRST)
                relay(1, FIRST)
            a_step(j, FIRST)

        loop(NF, 9, step)
        relay(2, FIRST)
        relay(3, FIRST)
        c_relay(0, 3).start()
        c_relay(3, 2).start()

        def step(t):
            a_step(9 + t, FIRST)

            @pl.when(t == 0)
            def _():
                relay(0, 2)
                relay(2, 2)
            c_step(2 * t, FIRST)
            c_step(2 * t + 1, FIRST)

        loop(0, 2, step)
        a_step(NF, 2)
        c_step(4, FIRST)
        b_step(0, FIRST)
        a_step(NF + 2, 2)
        loop(1, NB, lambda i: b_step(i, FIRST))
        end_start(0)
        a_step(NF + 4, 2)
        end_send(0)
        loop(NA - 2, NA, lambda j: a_step(j, 1))
        c_step(0, 3)
        c_step(3, 2)
        loop(0, 2, lambda m: b_step(2 * m, 2))

    @pl.when(home == 0)
    def _():
        def a_step(j, part):
            with jax.named_scope('a_wait'):
                y_copy(j, part).wait_recv()
            down(NA + j, a0 + j, part)

        def b_step(i, part):
            with jax.named_scope('b_wait'):
                relay_copy(i, part).wait_recv()
            back_copy(i, part).start()
            down(2 * NA + i, i, part)

        def c_step(i, part):
            make_h_c(i, part)
            down(c0 + i, c0 + i, part)

        loop(0, NB, lambda j: make_h(j, FIRST, 0))
        loop(0, NB // 2, lambda m: make_h(2 * m, 2, 0))
        c_step(0, FIRST)

        def step(t):
            c_step(1 + t, FIRST)
            a_step(t, WHOLE)

        loop(0, NF, step)
        a_step(NF, FIRST)
        c_step(4, FIRST)

        def step(t):
            a_step(NF + 1 + t, FIRST)
            b_step(t, FIRST)

        loop(0, 4, step)
        loop(NF + 5, NA, lambda j: a_step(j, FIRST))
        end_start(0)
        c_step(0, 3)
        c_step(3, 2)
        b_step(0, 2)
        end_send(0)
        a_step(NF, 2)
        b_step(2, 2)
        loop(1, 3, lambda m: a_step(NF + 2 * m, 2))
        loop(NA - 2, NA, lambda j: a_step(j, 1))

    end_start(1)
    end_send(1)

    def sent(ref, sem):
        remote(ref, ref, sem, sem, y_next).wait_send()

    with jax.named_scope('drain'):
        sent(stat_g.at[pl.ds(0, 7)], stat_ssem)
        sent(d_send, d_ssem)
        sent(hall.at[pl.ds(0, NB)], b_ssem)
        sent(c_recv.at[0], c_ssem)
        sent(ea_recv, e_ssem)
        sent(eb_recv, e_ssem)

        @pl.when(home == 0)
        def _():
            sent(x_ga, z_ssem)
            sent(x_gb, z_ssem)
            sent(own.at[pl.ds(0, NA)], x_ssem)
            sent(hall.at[pl.ds(0, NB + NC)], y_ssem)

        @pl.when(home == 1)
        def _():
            gain_cp.wait_send()
            sent(x_ga.at[pl.ds(0, 3)], z_ssem)
            sent(x_gb, z_ssem)
            sent(x_gb.at[0], z_ssem)
            sent(own.at[pl.ds(0, NB)], x_ssem)
            sent(c_recv.at[1], c_ssem)
            sent(hall.at[pl.ds(0, NA)], y_ssem)

    end_sum(0)
    end_sum(1)
    sent(fa_send, f_ssem)
    sent(fb_send, f_ssem)


def solution(mesh):
    def body(x_blk, gain_blk, w_in_blk, w_out_blk):
        tok, half = x_blk.shape
        feat = w_in_blk.shape[0]
        tokens = 4 * tok
        dma = pltpu.SemaphoreType.DMA
        return pl.pallas_call(
            kernel,
            out_shape=pltpu.VMEM((tok, half), BF16),
            in_specs=[pl.BlockSpec(memory_space=pl.ANY)] * 4,
            out_specs=pl.BlockSpec(memory_space=pltpu.VMEM),
            scratch_shapes=[
                pltpu.VMEM((TA, half), BF16),
                pltpu.VMEM((tok - TA, half), BF16),
                pltpu.VMEM((2, half), F32),
                pltpu.VMEM((8, 8, 128), F32),
                pltpu.VMEM((4, TA, feat), BF16),
                pltpu.VMEM((4, tok - TA, feat), BF16),
                pltpu.VMEM((2, tok - TA, feat), BF16),
                pltpu.VMEM((tokens, feat), BF16),
                pltpu.VMEM((N, feat, 2 * C), BF16),
                pltpu.VMEM((N, C, half), BF16),
                pltpu.VMEM((N, tokens, C), F32),
                pltpu.VMEM((N, tokens, C), F32),
                pltpu.VMEM((N, tokens, C), F32),
                pltpu.VMEM((NA, tokens, C), F32),
                pltpu.VMEM((2, NC, tokens, C), F32),
                pltpu.VMEM((2 * NA + NB, tokens, C), BF16),
                pltpu.VMEM((tokens, half), F32),
                pltpu.VMEM((2, TA, half), F32),
                pltpu.VMEM((2, tok - TA, half), F32),
                pltpu.VMEM((TA, half), F32),
                pltpu.VMEM((TA, half), F32),
                pltpu.VMEM((tok - TA, half), F32),
                pltpu.VMEM((tok - TA, half), F32),
                dma((10,)),
                dma((N // GROUP,)),
                dma((9,)),
                dma((RING,)),
                dma((NA + NA // 2 + 1,)),
                dma((NA + NA // 2 + 1,)),
                dma((NB + NB // 2,)),
                dma((2 * NC + 2,)),
                dma((4,)),
                dma((2,)),
            ],
            compiler_params=pltpu.CompilerParams(
                collective_id=0, has_side_effects=True, vmem_limit_bytes=66_500_000
            ),
        )(x_blk, gain_blk, w_in_blk, w_out_blk)

    return jax.shard_map(
        body,
        mesh=mesh,
        in_specs=(P(("dp", "row"), "col"), P("col"), P("row", "col"), P("row", "col")),
        out_specs=P(("dp", "row"), "col"),
        check_vma=False,
    )
```

```python
import jax
import jax.numpy as jnp
from jax import lax
from jax.experimental import pallas as pl
from jax.experimental.pallas import tpu as pltpu
from jax.sharding import PartitionSpec as P

NORM_EPS = 1e-5
MESH = pl.DeviceIdType.MESH
WHOLE, FIRST = -1, 0
F32 = jnp.float32
BF16 = jnp.bfloat16

C = 256
NB = 4
NC = 5
NA = 11
N = NA + NB + NC
NF = 3
GROUP = 5
RING = 8
TA = 16


def kernel(x_hbm, gain_hbm, w_in_hbm, w_out_hbm, out_v,
           xa_v, xb_v, gain_v, stat_g, x_ga, x_gb, x_relay, z_v, w_in_v, w_out_v, d_send, d_recv, own, x_recv, c_recv, hall,
           acc, ea_recv, eb_recv, fa_send, fa_recv, fb_send, fb_recv,
           misc_sem, w_in_sem, send_sem, d_rsem, x_rsem, y_rsem, b_rsem, c_rsem, e_rsem, f_rsem):
    w_out_sem, stat_rsem, za_rsem, zb_rsem = [misc_sem.at[i] for i in range(4, 8)]
    stat_ssem, z_ssem, d_ssem, x_ssem, y_ssem, b_ssem, c_ssem, e_ssem, f_ssem = [send_sem.at[i] for i in range(9)]
    y = lax.axis_index("col")
    row = lax.axis_index("row")
    x = row // 2
    k = row % 2
    dp = lax.axis_index("dp")
    home = 1 - (x + y) % 2
    tok, half = out_v.shape
    feat = half // 2
    block = N * C
    rows_a = 4 * TA
    tb = tok - TA
    rows_b = 4 * tb
    sibling = (dp, y, 2 * x + 1 - k)
    x_next = (dp, y, 2 * (1 - x) + k)
    y_next = (dp, 1 - y, row)

    def remote(src, dst, ssem, rsem, dev):
        return pltpu.make_async_remote_copy(src_ref=src, dst_ref=dst, send_sem=ssem, recv_sem=rsem,
                                            device_id=dev, device_id_type=MESH)

    c0, a0 = NB, NB + NC

    def chunk_of(p):
        u = p - 2 * NB - 1
        pair = jnp.where(p % 2 == 1, c0 + p // 2, p // 2 + (1 - home) * a0)
        mixed = jnp.where(u % 2 == 1, u // 2, a0 + NB + u // 2)
        late = jnp.where((home == 1) | (u >= 2 * NB), a0 + u, mixed)
        return jnp.where(p < 2 * NB, pair, jnp.where(u < 0, a0 - 1, late))

    def w_in_copies(p):
        c = C * chunk_of(p)
        cs = pl.multiple_of((1 - k) * block + c, C)
        co = pl.multiple_of(k * block + c, C)
        return (pltpu.make_async_copy(w_in_hbm.at[:, pl.ds(cs, C)], w_in_v.at[p, :, pl.ds(0, C)], w_in_sem.at[p // GROUP]),
                pltpu.make_async_copy(w_in_hbm.at[:, pl.ds(co, C)], w_in_v.at[p, :, pl.ds(C, C)], w_in_sem.at[p // GROUP]))

    def w_out_copy(i):
        r = pl.multiple_of(i * C, C)
        return pltpu.make_async_copy(w_out_hbm.at[pl.ds(r, C), :], w_out_v.at[i], w_out_sem)

    xa_copy = pltpu.make_async_copy(x_hbm.at[pl.ds(0, TA)], xa_v, misc_sem.at[0])
    xb_copy = pltpu.make_async_copy(x_hbm.at[pl.ds(TA, tb)], xb_v, misc_sem.at[8])
    g_copy = pltpu.make_async_copy(gain_hbm, gain_v.at[0], misc_sem.at[1])
    xa_copy.start()
    xb_copy.start()
    g_copy.start()

    barrier = pltpu.get_barrier_semaphore()
    for dy in range(2):
        for dr in range(4):
            if dy or dr:
                pl.semaphore_signal(barrier, inc=1, device_id=(dp, (y + dy) % 2, (row + dr) % 4), device_id_type=MESH)

    def start_w_in(p, _):
        for cp in w_in_copies(p):
            cp.start()
        return 0

    lax.fori_loop(0, N, start_w_in, 0)

    xa_copy.wait()
    xb_copy.wait()
    g_copy.wait()

    def row_sums(ref):
        v = ref[...].astype(F32)
        lane = lax.broadcasted_iota(jnp.int32, (v.shape[0], 128), 1)
        return jnp.where(lane == 0, jnp.sum(v, axis=1, keepdims=True), jnp.sum(v * v, axis=1, keepdims=True))

    me = 4 * y + row
    with jax.named_scope('barrier'):
        pl.semaphore_wait(barrier, 7)

    def tok_copy(group, dy, dk):
        tk = (k + dk) % 2
        cols = pl.ds(pl.multiple_of(feat * tk, 128), feat)
        src, dst, sem = ((xa_v, x_ga, za_rsem), (xb_v, x_gb, zb_rsem))[group]
        return remote(src.at[:, cols], dst.at[row], z_ssem, sem, (dp, (y + dy) % 2, 2 * y + tk))

    def stat_copy(d):
        ty = (y + d // 4) % 2
        tr = (row + d % 4) % 4
        return remote(stat_g.at[me], stat_g.at[me], stat_ssem, stat_rsem, (dp, ty, tr))

    gain_cp = remote(gain_v.at[0], gain_v.at[1], misc_sem.at[2], misc_sem.at[3], y_next)
    def to_relay(tk):
        return remote(xb_v.at[:, pl.ds(feat * tk, feat)], x_relay.at[tk], z_ssem, misc_sem.at[9], y_next)

    def from_relay(tk):
        return remote(x_relay.at[tk], x_gb.at[row], z_ssem, zb_rsem, (dp, y, 2 * (1 - x) + tk))

    @pl.when(home == 0)
    def _():
        to_relay(0).start()
        to_relay(1).start()
        tok_copy(0, 1, 0).start()

    @pl.when(home == 1)
    def _():
        gain_cp.start()
        tok_copy(0, 0, 1).start()
        tok_copy(0, 1, 0).start()

    stat_g[me, :, :tok] = jnp.transpose(jnp.concatenate([row_sums(xa_v), row_sums(xb_v)], axis=0))[:8]
    for d in range(1, 8):
        stat_copy(d).start()

    @pl.when(home == 0)
    def _():
        tok_copy(0, 1, 1).start()
        for group in range(2):
            tok_copy(group, 0, 0).start()
            tok_copy(group, 0, 1).start()

    @pl.when(home == 1)
    def _():
        tok_copy(0, 1, 1).start()
        tok_copy(1, 0, 1).start()
        tok_copy(1, 1, 0).start()
        tok_copy(1, 1, 1).start()
        x_ga[row] = jnp.where(k == 0, xa_v[:, :feat], xa_v[:, feat:])
        x_gb[row] = jnp.where(k == 0, xb_v[:, :feat], xb_v[:, feat:])
        gain_v[1] = gain_v[0]
        with jax.named_scope('x_relay_wait'):
            remote(x_relay, x_relay, z_ssem, misc_sem.at[9], y_next).wait_recv()
        from_relay(0).start()
        from_relay(1).start()

    @pl.when(home == 0)
    def _():
        with jax.named_scope('gain_wait'):
            gain_cp.wait_recv()
    gain = jnp.where(k == 0, gain_v[1, :feat], gain_v[1, feat:]).reshape(1, feat)
    acc[...] = jnp.zeros_like(acc)
    with jax.named_scope('stat_wait'):
        remote(stat_g.at[pl.ds(0, 7)], stat_g.at[pl.ds(0, 7)], stat_ssem, stat_rsem, y_next).wait_recv()

    def make_z(group):
        ref, sem = ((x_ga, za_rsem), (x_gb, zb_rsem))[group]

        @pl.when(home == 0)
        def _():
            with jax.named_scope('z_wait'):
                remote(ref, ref, z_ssem, sem, y_next).wait_recv()

        @pl.when(home == 1)
        def _():
            with jax.named_scope('z_wait'):
                remote(ref.at[pl.ds(0, 3)], ref.at[pl.ds(0, 3)], z_ssem, sem, y_next).wait_recv()

        t0, n, base = ((0, TA, 0), (TA, tb, rows_a))[group]
        for src in range(4):
            st = jnp.transpose(stat_g[src] + stat_g[4 + src])[t0:t0 + n] * (1.0 / (2 * half))
            mean = st[:, 0:1]
            var = st[:, 1:2] - mean * mean
            z = (ref[src].astype(F32) - mean) * lax.rsqrt(var + NORM_EPS) * gain
            z_v[pl.ds(base + n * src, n), :] = z.astype(BF16)

    row_group = (pl.ds(0, rows_a), pl.ds(rows_a, rows_b))

    def part_of(ref, j, part):
        if part == WHOLE:
            return ref.at[j]
        if part == FIRST:
            return ref.at[j, row_group[0]]
        return ref.at[pl.ds(j, part), row_group[1]]

    def rows_of(part):
        return pl.ds(0, rows_a + rows_b) if part == WHOLE else row_group[int(part > 0)]

    def d_copy(p, part, seq):
        return remote(part_of(d_send, p, part), part_of(d_recv, p, part), d_ssem, d_rsem.at[seq % RING], sibling)

    def x_copy_of(j, part, first):
        sem = x_rsem.at[NA + j // 2] if part > 0 else x_rsem.at[j]
        return remote(part_of(own, first + j, part), part_of(x_recv, j, part), x_ssem, sem, x_next)

    def c_copy(j):
        return c_part(j, WHOLE)

    def c_part(j, part):
        return remote(part_of(own, c0 + j, part), part_of(c_recv.at[0], j, part), c_ssem, c_rsem.at[j], y_next)

    def c_relay(j, part):
        sem = c_rsem.at[2 * NC + j // 3] if part > 0 else c_rsem.at[NC + j]
        return remote(part_of(c_recv.at[0], j, part), part_of(c_recv.at[1], j, part), c_ssem, sem, x_next)

    def pass_c(j):
        with jax.named_scope('c_wait'):
            c_copy(j).wait_recv()
        c_relay(j, FIRST).start()

    def up(p, part, seq):
        rows = rows_of(part)
        sums = jnp.dot(z_v[rows, :], w_in_v[p], preferred_element_type=F32)
        d_send[p, rows, :] = sums[:, :C]
        own[chunk_of(p), rows, :] = sums[:, C:]
        d_copy(p, part, seq).start()

    def pair_add(p, part, seq):
        with jax.named_scope('pair_wait'):
            d_copy(p, part, seq).wait_recv()
        q, rows = chunk_of(p), rows_of(part)
        own[q, rows, :] = own[q, rows, :] + d_recv[p, rows, :]

    def wait_w_in(p):
        with jax.named_scope('w_in_wait'):
            group = w_in_v.at[pl.ds(p, GROUP)]
            pltpu.make_async_copy(group, group, w_in_sem.at[p // GROUP]).wait()

    def pair_sum(p):
        pair_add(p, WHOLE, p + 2)
        q = chunk_of(p)

        @pl.when((q >= c0) & (q < a0))
        def _():
            c_copy(q - c0).start()

        @pl.when((home == 1) & (q < c0))
        def _():
            x_copy_of(q, FIRST, 0).start()

            @pl.when(q % 2 == 1)
            def _():
                x_copy_of(q - 1, 2, 0).start()

        @pl.when((home == 0) & (q >= a0 + NF))
        def _():
            x_copy_of(q - a0, FIRST, a0).start()

        @pl.when((home == 0) & (q >= a0) & (q < a0 + NF))
        def _():
            x_copy_of(q - a0, WHOLE, a0).start()

    def up_step(p, _):
        @pl.when(p % GROUP == 0)
        def _():
            wait_w_in(p)
        up(p, WHOLE, p + 2)
        w_out_copy(p).start()

        @pl.when(p >= 4)
        def _():
            pair_sum(p - 2)

        @pl.when((p >= 2) & (p < 4))
        def _():
            pair_add(p - 2, 1, p)

            @pl.when(p == 3)
            def _():
                c_part(0, 1).start()

            @pl.when((p == 2) & (home == 0))
            def _():
                first_b_part().start()

        @pl.when((p == 13) & (home == 1))
        def _():
            pass_c(0)

        @pl.when((p == 18) & (home == 1))
        def _():
            pass_c(1)
        return 0

    def first_b_part():
        return remote(part_of(own, a0, 1), part_of(x_recv, 0, 1), x_ssem, x_rsem.at[0], x_next)

    make_z(0)
    wait_w_in(0)
    up(0, FIRST, 0)
    up(1, FIRST, 1)
    make_z(1)
    up(0, 1, 2)
    w_out_copy(0).start()
    pair_add(0, FIRST, 0)

    @pl.when(home == 1)
    def _():
        x_copy_of(0, FIRST, 0).start()

    @pl.when(home == 0)
    def _():
        x_copy_of(0, FIRST, a0).start()

    up(1, 1, 3)
    w_out_copy(1).start()
    pair_add(1, FIRST, 1)
    c_part(0, FIRST).start()
    lax.fori_loop(2, N, up_step, 0)
    pair_sum(N - 2)
    pair_sum(N - 1)

    @pl.when(home == 0)
    def _():
        for j in range(NF, NA - 2, 2):
            x_copy_of(j, 2, a0).start()
        x_copy_of(NA - 2, 1, a0).start()
        x_copy_of(NA - 1, 1, a0).start()

    with jax.named_scope('w_out_wait'):
        pltpu.make_async_copy(w_out_v, w_out_v, w_out_sem).wait()

    def y_copy(j, part):
        sem = y_rsem.at[NA + j // 2] if part > 0 else y_rsem.at[j]
        return remote(part_of(hall, j, part), part_of(hall, NA + j, part), y_ssem, sem, y_next)

    def b_sem(j, part):
        return b_rsem.at[NB + j // 2] if part > 0 else b_rsem.at[j]

    def relay_copy(j, part):
        return remote(part_of(hall, NA + j, part), part_of(hall, 2 * NA + j, part), b_ssem, b_sem(j, part), x_next)

    def back_copy(j, part):
        return remote(part_of(hall, 2 * NA + j, part), part_of(hall, 2 * NA + j, part), b_ssem, b_sem(j, part), y_next)

    def put_h(j, part, left, right):
        rows = rows_of(part)
        for c in range(max(part, 1)):
            total = left(c)[rows, :] + right(c)[rows, :]
            hall[j + c, rows, :] = jax.nn.gelu(total, approximate=True).astype(BF16)

    def make_h(j, part, first):
        with jax.named_scope('x_wait'):
            x_copy_of(j, part, 0).wait_recv()
        put_h(j, part, lambda c: own.at[first + j + c], lambda c: x_recv.at[j + c])
        y_copy(j, part).start()

    def make_h_c(j, part):
        with jax.named_scope('c_wait'):
            if part == FIRST:
                c_copy(j).wait_recv()
            c_relay(j, part).wait_recv()
        put_h(c0 + j, part, lambda c: c_recv.at[0, j + c], lambda c: c_recv.at[1, j + c])
        yc_copy(j, part).start()

    def yc_copy(j, part):
        sem = y_rsem.at[NA + 2 + j // 3] if part > 0 else y_rsem.at[c0 + j]
        return remote(part_of(hall, c0 + j, part), part_of(hall, NA + c0 + j, part), y_ssem, sem, y_next)

    def down(slot, i, part):
        rows = rows_of(part)
        parts = [jnp.dot(hall[slot + c, rows, :], w_out_v[i + c], preferred_element_type=F32)
                 for c in range(max(part, 1))]
        acc[rows, :] += sum(parts[1:], parts[0])

    e_recv, f_send, f_recv = (ea_recv, eb_recv), (fa_send, fb_send), (fa_recv, fb_recv)

    def token_rows(group, r):
        n, base = ((TA, 0), (tb, rows_a))[group]
        return pl.ds(pl.multiple_of(base + n * r, 8), n)

    def e_copy(group, s):
        r = 2 * (s * x + (1 - s) * (1 - x)) + 1 - k
        return remote(acc.at[token_rows(group, r)], e_recv[group].at[s], e_ssem, e_rsem.at[2 * group + s], sibling)

    def f_copy(group):
        return remote(f_send[group], f_recv[group], f_ssem, f_rsem.at[group], x_next)

    def end_start(group):
        e_copy(group, 0).start()
        e_copy(group, 1).start()

    def end_send(group):
        with jax.named_scope('e0_wait'):
            e_copy(group, 0).wait_recv()
        f_send[group][...] = acc[token_rows(group, 2 * (1 - x) + k), :] + e_recv[group][0]
        f_copy(group).start()

    def end_sum(group):
        with jax.named_scope('e1_wait'):
            e_copy(group, 1).wait_recv()
        with jax.named_scope('f_wait'):
            f_copy(group).wait_recv()
        total = acc[token_rows(group, row), :] + e_recv[group][1] + f_recv[group][...]
        t0, n = ((0, TA), (TA, tb))[group]
        out_v[t0:t0 + n, :] = ((xa_v, xb_v)[group][...].astype(F32) + total).astype(BF16)

    def loop(lo, hi, step):
        def body(i, _):
            step(i)
            return 0
        lax.fori_loop(lo, hi, body, 0)

    @pl.when(home == 1)
    def _():
        def relay(i, part):
            with jax.named_scope('relay_wait'):
                y_copy(i, part).wait_recv()
            relay_copy(i, part).start()

        def b_step(i, part):
            with jax.named_scope('b_wait'):
                back_copy(i, part).wait_recv()
            down(2 * NA + i, i, part)

        def c_step(i, part):
            with jax.named_scope('ch_wait'):
                yc_copy(i, part).wait_recv()
            down(NA + c0 + i, c0 + i, part)

        def a_step(j, part):
            make_h(j, part, a0)
            down(j, a0 + j, part)

        loop(0, NF, lambda j: a_step(j, WHOLE))

        def step(j):
            for t, i in ((3, 2), (4, 3), (6, 4)):
                @pl.when(j == t)
                def _():
                    pass_c(i)

            @pl.when(j == 8)
            def _():
                relay(0, FIRST)
                relay(1, FIRST)
            a_step(j, FIRST)

        loop(NF, 9, step)
        relay(2, FIRST)
        relay(3, FIRST)
        c_relay(0, 3).start()
        c_relay(3, 2).start()

        def step(t):
            a_step(9 + t, FIRST)

            @pl.when(t == 0)
            def _():
                relay(0, 2)
                relay(2, 2)
            c_step(2 * t, FIRST)
            c_step(2 * t + 1, FIRST)

        loop(0, 2, step)
        a_step(NF, 2)
        c_step(4, FIRST)
        b_step(0, FIRST)
        a_step(NF + 2, 2)
        loop(1, NB - 1, lambda i: b_step(i, FIRST))
        make_h(NF + 4, 2, a0)
        b_step(NB - 1, FIRST)
        end_start(0)
        make_h(NA - 2, 1, a0)
        down(NF + 4, a0 + NF + 4, 2)
        make_h(NA - 1, 1, a0)
        end_send(0)
        loop(NA - 2, NA, lambda j: down(j, a0 + j, 1))
        c_step(0, 3)
        c_step(3, 2)
        loop(0, 2, lambda m: b_step(2 * m, 2))

    @pl.when(home == 0)
    def _():
        def a_step(j, part):
            with jax.named_scope('a_wait'):
                y_copy(j, part).wait_recv()
            down(NA + j, a0 + j, part)

        def b_step(i, part):
            with jax.named_scope('b_wait'):
                relay_copy(i, part).wait_recv()
            back_copy(i, part).start()
            down(2 * NA + i, i, part)

        def c_step(i, part):
            make_h_c(i, part)
            down(c0 + i, c0 + i, part)

        loop(0, NB, lambda j: make_h(j, FIRST, 0))
        loop(0, NB // 2, lambda m: make_h(2 * m, 2, 0))
        c_step(0, FIRST)

        def step(t):
            c_step(1 + t, FIRST)
            a_step(t, WHOLE)

        loop(0, NF, step)
        a_step(NF, FIRST)
        c_step(4, FIRST)

        def step(t):
            a_step(NF + 1 + t, FIRST)
            b_step(t, FIRST)

        loop(0, 4, step)
        loop(NF + 5, NA, lambda j: a_step(j, FIRST))
        end_start(0)
        c_step(0, 3)
        c_step(3, 2)
        end_send(0)
        b_step(0, 2)
        a_step(NF, 2)
        b_step(2, 2)
        loop(1, 3, lambda m: a_step(NF + 2 * m, 2))
        loop(NA - 2, NA, lambda j: a_step(j, 1))

    end_start(1)
    end_send(1)

    def sent(ref, sem):
        remote(ref, ref, sem, sem, y_next).wait_send()

    with jax.named_scope('drain'):
        sent(stat_g.at[pl.ds(0, 7)], stat_ssem)
        sent(d_send, d_ssem)
        sent(hall.at[pl.ds(0, NB)], b_ssem)
        sent(c_recv.at[0], c_ssem)
        sent(ea_recv, e_ssem)
        sent(eb_recv, e_ssem)

        @pl.when(home == 0)
        def _():
            sent(x_ga, z_ssem)
            sent(x_gb, z_ssem)
            sent(own.at[pl.ds(0, NA)], x_ssem)
            sent(hall.at[pl.ds(0, NB + NC)], y_ssem)

        @pl.when(home == 1)
        def _():
            gain_cp.wait_send()
            sent(x_ga.at[pl.ds(0, 3)], z_ssem)
            sent(x_gb, z_ssem)
            sent(x_gb.at[0], z_ssem)
            sent(own.at[pl.ds(0, NB)], x_ssem)
            sent(c_recv.at[1], c_ssem)
            sent(hall.at[pl.ds(0, NA)], y_ssem)

    end_sum(0)
    end_sum(1)
    sent(fa_send, f_ssem)
    sent(fb_send, f_ssem)


def solution(mesh):
    def body(x_blk, gain_blk, w_in_blk, w_out_blk):
        tok, half = x_blk.shape
        feat = w_in_blk.shape[0]
        tokens = 4 * tok
        dma = pltpu.SemaphoreType.DMA
        return pl.pallas_call(
            kernel,
            out_shape=pltpu.VMEM((tok, half), BF16),
            in_specs=[pl.BlockSpec(memory_space=pl.ANY)] * 4,
            out_specs=pl.BlockSpec(memory_space=pltpu.VMEM),
            scratch_shapes=[
                pltpu.VMEM((TA, half), BF16),
                pltpu.VMEM((tok - TA, half), BF16),
                pltpu.VMEM((2, half), F32),
                pltpu.VMEM((8, 8, 128), F32),
                pltpu.VMEM((4, TA, feat), BF16),
                pltpu.VMEM((4, tok - TA, feat), BF16),
                pltpu.VMEM((2, tok - TA, feat), BF16),
                pltpu.VMEM((tokens, feat), BF16),
                pltpu.VMEM((N, feat, 2 * C), BF16),
                pltpu.VMEM((N, C, half), BF16),
                pltpu.VMEM((N, tokens, C), F32),
                pltpu.VMEM((N, tokens, C), F32),
                pltpu.VMEM((N, tokens, C), F32),
                pltpu.VMEM((NA, tokens, C), F32),
                pltpu.VMEM((2, NC, tokens, C), F32),
                pltpu.VMEM((2 * NA + NB, tokens, C), BF16),
                pltpu.VMEM((tokens, half), F32),
                pltpu.VMEM((2, TA, half), F32),
                pltpu.VMEM((2, tok - TA, half), F32),
                pltpu.VMEM((TA, half), F32),
                pltpu.VMEM((TA, half), F32),
                pltpu.VMEM((tok - TA, half), F32),
                pltpu.VMEM((tok - TA, half), F32),
                dma((10,)),
                dma((N // GROUP,)),
                dma((9,)),
                dma((RING,)),
                dma((NA + NA // 2 + 1,)),
                dma((NA + NA // 2 + 1,)),
                dma((NB + NB // 2,)),
                dma((2 * NC + 2,)),
                dma((4,)),
                dma((2,)),
            ],
            compiler_params=pltpu.CompilerParams(
                collective_id=0, has_side_effects=True, vmem_limit_bytes=66_500_000
            ),
        )(x_blk, gain_blk, w_in_blk, w_out_blk)

    return jax.shard_map(
        body,
        mesh=mesh,
        in_specs=(P(("dp", "row"), "col"), P("col"), P("row", "col"), P("row", "col")),
        out_specs=P(("dp", "row"), "col"),
        check_vma=False,
    )
```

```python
import jax
import jax.numpy as jnp
from jax import lax
from jax.experimental import pallas as pl
from jax.experimental.pallas import tpu as pltpu
from jax.sharding import PartitionSpec as P

NORM_EPS = 1e-5
MESH = pl.DeviceIdType.MESH
WHOLE, FIRST = -1, 0
F32 = jnp.float32
BF16 = jnp.bfloat16

C = 256
NB = 4
NC = 5
NA = 11
N = NA + NB + NC
NF = 4
EARLY = 2 * NB
GROUP = 5
RING = 8
TA = 16


def kernel(x_hbm, gain_hbm, w_in_hbm, w_out_hbm, out_v,
           xa_v, xb_v, gain_v, stat_g, x_ga, x_gb, x_relay, z_v, w_in_v, w_out_v, d_send, d_recv, own, x_recv, c_recv, hall,
           acc, ea_recv, eb_recv, fa_send, fa_recv, fb_send, fb_recv,
           misc_sem, w_in_sem, send_sem, d_rsem, x_rsem, y_rsem, b_rsem, c_rsem, e_rsem, f_rsem):
    w_out_sem, stat_rsem, za_rsem, zb_rsem = [misc_sem.at[i] for i in range(4, 8)]
    stat_ssem, z_ssem, d_ssem, x_ssem, y_ssem, b_ssem, c_ssem, e_ssem, f_ssem = [send_sem.at[i] for i in range(9)]
    y = lax.axis_index("col")
    row = lax.axis_index("row")
    x = row // 2
    k = row % 2
    dp = lax.axis_index("dp")
    home = 1 - (x + y) % 2
    tok, half = out_v.shape
    feat = half // 2
    block = N * C
    rows_a = 4 * TA
    tb = tok - TA
    rows_b = 4 * tb
    sibling = (dp, y, 2 * x + 1 - k)
    x_next = (dp, y, 2 * (1 - x) + k)
    y_next = (dp, 1 - y, row)

    def remote(src, dst, ssem, rsem, dev):
        return pltpu.make_async_remote_copy(src_ref=src, dst_ref=dst, send_sem=ssem, recv_sem=rsem,
                                            device_id=dev, device_id_type=MESH)

    c0, a0 = NB, NB + NC

    def chunk_of(p):
        u = p - 2 * NB - 1
        pair = jnp.where(p % 2 == 1, c0 + p // 2, p // 2 + (1 - home) * a0)
        mixed = jnp.where(u % 2 == 1, u // 2, a0 + NB + u // 2)
        late = jnp.where((home == 1) | (u >= 2 * NB), a0 + u, mixed)
        return jnp.where(p < 2 * NB, pair, jnp.where(u < 0, a0 - 1, late))

    def w_in_copies(p):
        c = C * chunk_of(p)
        cs = pl.multiple_of((1 - k) * block + c, C)
        co = pl.multiple_of(k * block + c, C)
        return (pltpu.make_async_copy(w_in_hbm.at[:, pl.ds(cs, C)], w_in_v.at[p, :, pl.ds(0, C)], w_in_sem.at[p // GROUP]),
                pltpu.make_async_copy(w_in_hbm.at[:, pl.ds(co, C)], w_in_v.at[p, :, pl.ds(C, C)], w_in_sem.at[p // GROUP]))

    def w_out_copy(i):
        r = pl.multiple_of(i * C, C)
        return pltpu.make_async_copy(w_out_hbm.at[pl.ds(r, C), :], w_out_v.at[i], w_out_sem)

    xa_copy = pltpu.make_async_copy(x_hbm.at[pl.ds(0, TA)], xa_v, misc_sem.at[0])
    xb_copy = pltpu.make_async_copy(x_hbm.at[pl.ds(TA, tb)], xb_v, misc_sem.at[8])
    g_copy = pltpu.make_async_copy(gain_hbm, gain_v.at[0], misc_sem.at[1])
    xa_copy.start()
    xb_copy.start()
    g_copy.start()

    barrier = pltpu.get_barrier_semaphore()
    for dy in range(2):
        for dr in range(4):
            if dy or dr:
                pl.semaphore_signal(barrier, inc=1, device_id=(dp, (y + dy) % 2, (row + dr) % 4), device_id_type=MESH)

    def start_w_in(p, _):
        for cp in w_in_copies(p):
            cp.start()
        return 0

    lax.fori_loop(0, N, start_w_in, 0)

    xa_copy.wait()
    xb_copy.wait()
    g_copy.wait()

    def row_sums(ref):
        v = ref[...].astype(F32)
        lane = lax.broadcasted_iota(jnp.int32, (v.shape[0], 128), 1)
        return jnp.where(lane == 0, jnp.sum(v, axis=1, keepdims=True), jnp.sum(v * v, axis=1, keepdims=True))

    me = 4 * y + row
    stat_g[me, :, :tok] = jnp.transpose(jnp.concatenate([row_sums(xa_v), row_sums(xb_v)], axis=0))[:8]
    with jax.named_scope('barrier'):
        pl.semaphore_wait(barrier, 7)

    def tok_copy(group, dy, dk):
        tk = (k + dk) % 2
        cols = pl.ds(pl.multiple_of(feat * tk, 128), feat)
        src, dst, sem = ((xa_v, x_ga, za_rsem), (xb_v, x_gb, zb_rsem))[group]
        return remote(src.at[:, cols], dst.at[row], z_ssem, sem, (dp, (y + dy) % 2, 2 * y + tk))

    def stat_copy(d):
        ty = (y + d // 4) % 2
        tr = (row + d % 4) % 4
        return remote(stat_g.at[me], stat_g.at[me], stat_ssem, stat_rsem, (dp, ty, tr))

    gain_cp = remote(gain_v.at[0], gain_v.at[1], misc_sem.at[2], misc_sem.at[3], y_next)
    half_cols = pl.ds(pl.multiple_of(feat * (1 - k), 128), feat)
    to_relay = remote(xa_v.at[:, half_cols], x_relay, z_ssem, misc_sem.at[9], y_next)
    from_relay = remote(x_relay, x_ga.at[row], z_ssem, za_rsem, (dp, y, 2 * (1 - x) + 1 - k))

    for d in range(1, 8):
        stat_copy(d).start()

    @pl.when(home == 0)
    def _():
        to_relay.start()
        tok_copy(1, 1, 0).start()
        tok_copy(1, 1, 1).start()
        tok_copy(1, 0, 0).start()
        tok_copy(1, 0, 1).start()
        tok_copy(0, 1, 0).start()
        tok_copy(0, 0, 0).start()
        tok_copy(0, 0, 1).start()

    @pl.when(home == 1)
    def _():
        gain_cp.start()
        for group in (1, 0):
            tok_copy(group, 0, 1).start()
            tok_copy(group, 1, 0).start()
            tok_copy(group, 1, 1).start()
        x_ga[row] = jnp.where(k == 0, xa_v[:, :feat], xa_v[:, feat:])
        x_gb[row] = jnp.where(k == 0, xb_v[:, :feat], xb_v[:, feat:])
        gain_v[1] = gain_v[0]
        with jax.named_scope('x_relay_wait'):
            to_relay.wait_recv()
        from_relay.start()

    @pl.when(home == 0)
    def _():
        with jax.named_scope('gain_wait'):
            gain_cp.wait_recv()
    gain = jnp.where(k == 0, gain_v[1, :feat], gain_v[1, feat:]).reshape(1, feat)
    acc[...] = jnp.zeros_like(acc)
    with jax.named_scope('stat_wait'):
        remote(stat_g.at[pl.ds(0, 7)], stat_g.at[pl.ds(0, 7)], stat_ssem, stat_rsem, y_next).wait_recv()

    def make_z(group):
        ref, sem = ((x_ga, za_rsem), (x_gb, zb_rsem))[group]

        @pl.when(home == 0)
        def _():
            with jax.named_scope('z_wait'):
                remote(ref, ref, z_ssem, sem, y_next).wait_recv()

        @pl.when(home == 1)
        def _():
            with jax.named_scope('z_wait'):
                remote(ref.at[pl.ds(0, 3)], ref.at[pl.ds(0, 3)], z_ssem, sem, y_next).wait_recv()

        t0, n, base = ((0, TA, 0), (TA, tb, rows_a))[group]
        for src in range(4):
            st = jnp.transpose(stat_g[src] + stat_g[4 + src])[t0:t0 + n] * (1.0 / (2 * half))
            mean = st[:, 0:1]
            var = st[:, 1:2] - mean * mean
            z = (ref[src].astype(F32) - mean) * lax.rsqrt(var + NORM_EPS) * gain
            z_v[pl.ds(base + n * src, n), :] = z.astype(BF16)

    row_group = (pl.ds(0, rows_a), pl.ds(rows_a, rows_b))

    def part_of(ref, j, part):
        if part == WHOLE:
            return ref.at[j]
        if part == FIRST:
            return ref.at[j, row_group[0]]
        return ref.at[pl.ds(j, part), row_group[1]]

    def rows_of(part):
        return pl.ds(0, rows_a + rows_b) if part == WHOLE else row_group[int(part > 0)]

    def d_copy(p, part, seq):
        return remote(part_of(d_send, p, part), part_of(d_recv, p, part), d_ssem, d_rsem.at[seq % RING], sibling)

    def b_index(j, part):
        return NA + j // 2 if part == 2 else j + 7

    def x_group(j, part, first, sem):
        return remote(part_of(own, first + j, part), part_of(x_recv, j, part), x_ssem, x_rsem.at[sem], x_next)

    def x_copy_of(j, part, first):
        sem = x_rsem.at[b_index(j, part)] if part > 0 else x_rsem.at[j]
        return remote(part_of(own, first + j, part), part_of(x_recv, j, part), x_ssem, sem, x_next)

    def c_copy(j):
        return c_part(j, WHOLE)

    def c_part(j, part):
        return remote(part_of(own, c0 + j, part), part_of(c_recv.at[0], j, part), c_ssem, c_rsem.at[j], y_next)

    def c_relay(j, part):
        sem = c_rsem.at[2 * NC + j // 3] if part > 0 else c_rsem.at[NC + j]
        return remote(part_of(c_recv.at[0], j, part), part_of(c_recv.at[1], j, part), c_ssem, sem, x_next)

    def pass_c(j):
        with jax.named_scope('c_wait'):
            c_copy(j).wait_recv()
        c_relay(j, FIRST).start()

    def up(p, part, seq):
        rows = rows_of(part)
        sums = jnp.dot(z_v[rows, :], w_in_v[p], preferred_element_type=F32)
        d_send[p, rows, :] = sums[:, :C]
        own[chunk_of(p), rows, :] = sums[:, C:]
        d_copy(p, part, seq).start()

    def pair_add(p, part, seq):
        with jax.named_scope('pair_wait'):
            d_copy(p, part, seq).wait_recv()
        q, rows = chunk_of(p), rows_of(part)
        own[q, rows, :] = own[q, rows, :] + d_recv[p, rows, :]

    def wait_w_in(p):
        with jax.named_scope('w_in_wait'):
            group = w_in_v.at[pl.ds(p, GROUP)]
            pltpu.make_async_copy(group, group, w_in_sem.at[p // GROUP]).wait()

    def pair_group(p, part, seq):
        pair_add(p, part, seq)
        q = chunk_of(p)

        @pl.when((q >= c0) & (q < a0))
        def _():
            c_part(q - c0, part).start()

        @pl.when((home == 1) & (q < c0))
        def _():
            x_group(q, part, 0, NA + q // 2 if part else q).start()

        @pl.when((home == 0) & (q >= a0))
        def _():
            x_group(q - a0, part, a0, q - a0).start()

    def pair_sum(p):
        pair_add(p, WHOLE, p + EARLY)
        q = chunk_of(p)

        @pl.when((q >= c0) & (q < a0))
        def _():
            c_copy(q - c0).start()

        @pl.when((home == 0) & (q >= a0))
        def _():
            x_copy_of(q - a0, FIRST, a0).start()

    def up_early(part, seq):
        def step(p, _):
            if part:
                @pl.when(p % GROUP == 0)
                def _():
                    wait_w_in(p)
            up(p, part, p + seq)

            @pl.when(p >= 2)
            def _():
                pair_group(p - 2, part, p - 2 + seq)

            if part == FIRST:
                w_out_copy(p).start()
            return 0

        lax.fori_loop(0, EARLY, step, 0)

    def up_step(p, _):
        @pl.when(p % GROUP == 0)
        def _():
            wait_w_in(p)
        up(p, WHOLE, p + EARLY)
        w_out_copy(p).start()

        @pl.when(p >= EARLY + 2)
        def _():
            pair_sum(p - 2)

        @pl.when(p < EARLY + 2)
        def _():
            pair_group(p - 2, FIRST, p - 2 + EARLY)

        @pl.when((p == 17) & (home == 1))
        def _():
            pass_c(0)
        return 0

    make_z(1)
    up_early(1, 0)
    pair_group(EARLY - 2, 1, EARLY - 2)
    pair_group(EARLY - 1, 1, EARLY - 1)
    make_z(0)
    up_early(FIRST, EARLY)
    lax.fori_loop(EARLY, N, up_step, 0)
    pair_sum(N - 2)
    pair_sum(N - 1)

    @pl.when(home == 0)
    def _():
        x_copy_of(NF, 2, a0).start()
        x_copy_of(NF + 2, 2, a0).start()
        for j in range(NF + 4, NA):
            x_copy_of(j, 1, a0).start()

    with jax.named_scope('w_out_wait'):
        pltpu.make_async_copy(w_out_v, w_out_v, w_out_sem).wait()

    def y_copy(j, part):
        sem = y_rsem.at[b_index(j, part)] if part > 0 else y_rsem.at[j]
        return remote(part_of(hall, j, part), part_of(hall, NA + j, part), y_ssem, sem, y_next)

    def b_sem(j, part):
        return b_rsem.at[NB + j // 2] if part > 0 else b_rsem.at[j]

    def relay_copy(j, part):
        return remote(part_of(hall, NA + j, part), part_of(hall, 2 * NA + j, part), b_ssem, b_sem(j, part), x_next)

    def back_copy(j, part):
        return remote(part_of(hall, 2 * NA + j, part), part_of(hall, 2 * NA + j, part), b_ssem, b_sem(j, part), y_next)

    def put_h(j, part, left, right):
        rows = rows_of(part)
        for c in range(max(part, 1)):
            total = left(c)[rows, :] + right(c)[rows, :]
            hall[j + c, rows, :] = jax.nn.gelu(total, approximate=True).astype(BF16)

    def make_h(j, part, first):
        with jax.named_scope('x_wait'):
            x_copy_of(j, part, 0).wait_recv()
        put_h(j, part, lambda c: own.at[first + j + c], lambda c: x_recv.at[j + c])
        y_copy(j, part).start()

    def make_h_c(j, part):
        with jax.named_scope('c_wait'):
            if part == FIRST:
                c_copy(j).wait_recv()
            c_relay(j, part).wait_recv()
        put_h(c0 + j, part, lambda c: c_recv.at[0, j + c], lambda c: c_recv.at[1, j + c])
        yc_copy(j, part).start()

    def yc_copy(j, part):
        sem = y_rsem.at[NA + 2 + j // 3] if part > 0 else y_rsem.at[c0 + j]
        return remote(part_of(hall, c0 + j, part), part_of(hall, NA + c0 + j, part), y_ssem, sem, y_next)

    def down(slot, i, part):
        rows = rows_of(part)
        parts = [jnp.dot(hall[slot + c, rows, :], w_out_v[i + c], preferred_element_type=F32)
                 for c in range(max(part, 1))]
        acc[rows, :] += sum(parts[1:], parts[0])

    e_recv, f_send, f_recv = (ea_recv, eb_recv), (fa_send, fb_send), (fa_recv, fb_recv)

    def token_rows(group, r):
        n, base = ((TA, 0), (tb, rows_a))[group]
        return pl.ds(pl.multiple_of(base + n * r, 8), n)

    def e_copy(group, s):
        r = 2 * (s * x + (1 - s) * (1 - x)) + 1 - k
        return remote(acc.at[token_rows(group, r)], e_recv[group].at[s], e_ssem, e_rsem.at[2 * group + s], sibling)

    def f_copy(group):
        return remote(f_send[group], f_recv[group], f_ssem, f_rsem.at[group], x_next)

    def end_start(group):
        e_copy(group, 0).start()
        e_copy(group, 1).start()

    def end_send(group):
        with jax.named_scope('e0_wait'):
            e_copy(group, 0).wait_recv()
        f_send[group][...] = acc[token_rows(group, 2 * (1 - x) + k), :] + e_recv[group][0]
        f_copy(group).start()

    def end_sum(group):
        with jax.named_scope('e1_wait'):
            e_copy(group, 1).wait_recv()
        with jax.named_scope('f_wait'):
            f_copy(group).wait_recv()
        total = acc[token_rows(group, row), :] + e_recv[group][1] + f_recv[group][...]
        t0, n = ((0, TA), (TA, tb))[group]
        out_v[t0:t0 + n, :] = ((xa_v, xb_v)[group][...].astype(F32) + total).astype(BF16)

    def loop(lo, hi, step):
        def body(i, _):
            step(i)
            return 0
        lax.fori_loop(lo, hi, body, 0)

    @pl.when(home == 1)
    def _():
        def relay(i, part):
            with jax.named_scope('relay_wait'):
                y_copy(i, part).wait_recv()
            relay_copy(i, part).start()

        def b_step(i, part):
            with jax.named_scope('b_wait'):
                back_copy(i, part).wait_recv()
            down(2 * NA + i, i, part)

        def c_step(i, part):
            with jax.named_scope('ch_wait'):
                yc_copy(i, part).wait_recv()
            down(NA + c0 + i, c0 + i, part)

        def a_step(j, part):
            make_h(j, part, a0)
            down(j, a0 + j, part)

        pass_c(1)

        def step(j):
            @pl.when(j == 2)
            def _():
                pass_c(2)
            a_step(j, WHOLE)

        loop(0, NF, step)

        def step(j):
            for t, i in ((4, 3), (6, 4)):
                @pl.when(j == t)
                def _():
                    pass_c(i)

            @pl.when(j == 7)
            def _():
                relay(0, FIRST)
                relay(1, FIRST)
            a_step(j, FIRST)

        loop(NF, 8, step)
        relay(2, FIRST)
        relay(3, FIRST)
        c_relay(0, 3).start()
        c_relay(3, 2).start()

        def step(t):
            a_step(8 + t, FIRST)

            @pl.when(t == 0)
            def _():
                relay(0, 2)
                relay(2, 2)

            @pl.when(t == 1)
            def _():
                c_step(1, FIRST)
            c_step(2 * t, FIRST)

        loop(0, 2, step)
        a_step(10, FIRST)
        loop(3, 5, lambda i: c_step(i, FIRST))
        a_step(NF, 2)
        loop(0, 2, lambda i: b_step(i, FIRST))
        a_step(NF + 2, 2)
        b_step(2, FIRST)
        make_h(NF + 4, 1, a0)
        b_step(NB - 1, FIRST)
        end_start(0)
        make_h(NF + 5, 1, a0)
        down(NF + 4, a0 + NF + 4, 1)
        make_h(NF + 6, 1, a0)
        end_send(0)
        loop(NF + 5, NA, lambda j: down(j, a0 + j, 1))
        c_step(0, 3)
        c_step(3, 2)
        loop(0, 2, lambda m: b_step(2 * m, 2))

    @pl.when(home == 0)
    def _():
        def a_step(j, part):
            with jax.named_scope('a_wait'):
                y_copy(j, part).wait_recv()
            down(NA + j, a0 + j, part)

        def b_step(i, part):
            with jax.named_scope('b_wait'):
                relay_copy(i, part).wait_recv()
            back_copy(i, part).start()
            down(2 * NA + i, i, part)

        def c_step(i, part):
            make_h_c(i, part)
            down(c0 + i, c0 + i, part)

        loop(0, NB, lambda j: make_h(j, FIRST, 0))
        loop(0, NB // 2, lambda m: make_h(2 * m, 2, 0))
        c_step(0, FIRST)

        def step(t):
            c_step(1 + t, FIRST)
            a_step(t, WHOLE)

        loop(0, NF, step)

        def step(t):
            b_step(t, FIRST)
            a_step(NF + t, FIRST)

        loop(0, 4, step)
        a_step(8, FIRST)
        c_step(0, 3)
        loop(9, NA, lambda j: a_step(j, FIRST))
        end_start(0)
        c_step(3, 2)
        b_step(0, 2)
        end_send(0)
        b_step(2, 2)
        loop(0, 2, lambda m: a_step(NF + 2 * m, 2))
        loop(NF + 4, NA, lambda j: a_step(j, 1))

    end_start(1)
    end_send(1)

    def sent(ref, sem):
        remote(ref, ref, sem, sem, y_next).wait_send()

    with jax.named_scope('drain'):
        sent(stat_g.at[pl.ds(0, 7)], stat_ssem)
        sent(d_send, d_ssem)
        sent(hall.at[pl.ds(0, NB)], b_ssem)
        sent(c_recv.at[0], c_ssem)
        sent(ea_recv, e_ssem)
        sent(eb_recv, e_ssem)

        @pl.when(home == 0)
        def _():
            sent(x_ga, z_ssem)
            sent(x_gb, z_ssem)
            sent(own.at[pl.ds(0, NA)], x_ssem)
            sent(hall.at[pl.ds(0, NB + NC)], y_ssem)

        @pl.when(home == 1)
        def _():
            gain_cp.wait_send()
            sent(x_ga, z_ssem)
            sent(x_gb.at[pl.ds(0, 3)], z_ssem)
            sent(own.at[pl.ds(0, NB)], x_ssem)
            sent(c_recv.at[1], c_ssem)
            sent(hall.at[pl.ds(0, NA)], y_ssem)

    end_sum(0)
    end_sum(1)
    sent(fa_send, f_ssem)
    sent(fb_send, f_ssem)


def solution(mesh):
    def body(x_blk, gain_blk, w_in_blk, w_out_blk):
        tok, half = x_blk.shape
        feat = w_in_blk.shape[0]
        tokens = 4 * tok
        dma = pltpu.SemaphoreType.DMA
        return pl.pallas_call(
            kernel,
            out_shape=pltpu.VMEM((tok, half), BF16),
            in_specs=[pl.BlockSpec(memory_space=pl.ANY)] * 4,
            out_specs=pl.BlockSpec(memory_space=pltpu.VMEM),
            scratch_shapes=[
                pltpu.VMEM((TA, half), BF16),
                pltpu.VMEM((tok - TA, half), BF16),
                pltpu.VMEM((2, half), F32),
                pltpu.VMEM((8, 8, 128), F32),
                pltpu.VMEM((4, TA, feat), BF16),
                pltpu.VMEM((4, tok - TA, feat), BF16),
                pltpu.VMEM((TA, feat), BF16),
                pltpu.VMEM((tokens, feat), BF16),
                pltpu.VMEM((N, feat, 2 * C), BF16),
                pltpu.VMEM((N, C, half), BF16),
                pltpu.VMEM((N, tokens, C), F32),
                pltpu.VMEM((N, tokens, C), F32),
                pltpu.VMEM((N, tokens, C), F32),
                pltpu.VMEM((NA, tokens, C), F32),
                pltpu.VMEM((2, NC, tokens, C), F32),
                pltpu.VMEM((2 * NA + NB, tokens, C), BF16),
                pltpu.VMEM((tokens, half), F32),
                pltpu.VMEM((2, TA, half), F32),
                pltpu.VMEM((2, tok - TA, half), F32),
                pltpu.VMEM((TA, half), F32),
                pltpu.VMEM((TA, half), F32),
                pltpu.VMEM((tok - TA, half), F32),
                pltpu.VMEM((tok - TA, half), F32),
                dma((10,)),
                dma((N // GROUP,)),
                dma((9,)),
                dma((RING,)),
                dma((NA + 7,)),
                dma((NA + 7,)),
                dma((NB + NB // 2,)),
                dma((2 * NC + 2,)),
                dma((4,)),
                dma((2,)),
            ],
            compiler_params=pltpu.CompilerParams(
                collective_id=0, has_side_effects=True, vmem_limit_bytes=66_500_000
            ),
        )(x_blk, gain_blk, w_in_blk, w_out_blk)

    return jax.shard_map(
        body,
        mesh=mesh,
        in_specs=(P(("dp", "row"), "col"), P("col"), P("row", "col"), P("row", "col")),
        out_specs=P(("dp", "row"), "col"),
        check_vma=False,
    )
```

```python
import jax
import jax.numpy as jnp
from jax import lax
from jax.experimental import pallas as pl
from jax.experimental.pallas import tpu as pltpu
from jax.sharding import PartitionSpec as P

NORM_EPS = 1e-5
MESH = pl.DeviceIdType.MESH
WHOLE, FIRST = -1, 0
F32 = jnp.float32
BF16 = jnp.bfloat16

C = 256
NB = 4
NC = 5
NA = 11
N = NA + NB + NC
NF = 4
EARLY = 4
GROUP = 5
LAG = 3
RING = 12
TA = 16


def kernel(x_hbm, gain_hbm, w_in_hbm, w_out_hbm, out_v,
           xa_v, xb_v, gain_v, stat_g, x_ga, x_gb, x_relay, z_v, w_in_v, w_out_v, d_send, d_recv, own, x_recv, c_recv, hall,
           acc, ea_recv, eb_recv, fa_send, fa_recv, fb_send, fb_recv,
           misc_sem, w_in_sem, send_sem, d_rsem, x_rsem, y_rsem, b_rsem, c_rsem, e_rsem, f_rsem):
    w_out_sem, stat_rsem, za_rsem, zb_rsem = [misc_sem.at[i] for i in range(4, 8)]
    stat_ssem, z_ssem, d_ssem, x_ssem, y_ssem, b_ssem, c_ssem, e_ssem, f_ssem = [send_sem.at[i] for i in range(9)]
    y = lax.axis_index("col")
    row = lax.axis_index("row")
    x = row // 2
    k = row % 2
    dp = lax.axis_index("dp")
    home = 1 - (x + y) % 2
    tok, half = out_v.shape
    feat = half // 2
    block = N * C
    rows_a = 4 * TA
    tb = tok - TA
    rows_b = 4 * tb
    sibling = (dp, y, 2 * x + 1 - k)
    x_next = (dp, y, 2 * (1 - x) + k)
    y_next = (dp, 1 - y, row)

    def remote(src, dst, ssem, rsem, dev):
        return pltpu.make_async_remote_copy(src_ref=src, dst_ref=dst, send_sem=ssem, recv_sem=rsem,
                                            device_id=dev, device_id_type=MESH)

    c0, a0 = NB, NB + NC

    def chunk_of(p):
        u = p - 2 * NB - 1
        pair = jnp.where(p % 2 == 1, c0 + p // 2, p // 2 + (1 - home) * a0)
        mixed = jnp.where(u % 2 == 1, u // 2, a0 + NB + u // 2)
        late = jnp.where((home == 1) | (u >= 2 * NB), a0 + u, mixed)
        return jnp.where(p < 2 * NB, pair, jnp.where(u < 0, a0 - 1, late))

    def w_in_copies(p):
        c = C * chunk_of(p)
        cs = pl.multiple_of((1 - k) * block + c, C)
        co = pl.multiple_of(k * block + c, C)
        return (pltpu.make_async_copy(w_in_hbm.at[:, pl.ds(cs, C)], w_in_v.at[p, :, pl.ds(0, C)], w_in_sem.at[p // GROUP]),
                pltpu.make_async_copy(w_in_hbm.at[:, pl.ds(co, C)], w_in_v.at[p, :, pl.ds(C, C)], w_in_sem.at[p // GROUP]))

    def w_out_copy(i):
        r = pl.multiple_of(i * C, C)
        return pltpu.make_async_copy(w_out_hbm.at[pl.ds(r, C), :], w_out_v.at[i], w_out_sem)

    xa_copy = pltpu.make_async_copy(x_hbm.at[pl.ds(0, TA)], xa_v, misc_sem.at[0])
    xb_copy = pltpu.make_async_copy(x_hbm.at[pl.ds(TA, tb)], xb_v, misc_sem.at[8])
    g_copy = pltpu.make_async_copy(gain_hbm, gain_v.at[0], misc_sem.at[1])
    xa_copy.start()
    xb_copy.start()
    g_copy.start()

    barrier = pltpu.get_barrier_semaphore()
    for dy in range(2):
        for dr in range(4):
            if dy or dr:
                pl.semaphore_signal(barrier, inc=1, device_id=(dp, (y + dy) % 2, (row + dr) % 4), device_id_type=MESH)

    def start_w_in(p, _):
        for cp in w_in_copies(p):
            cp.start()
        return 0

    lax.fori_loop(0, N, start_w_in, 0)

    xa_copy.wait()
    xb_copy.wait()
    g_copy.wait()

    def row_sums(ref):
        v = ref[...].astype(F32)
        lane = lax.broadcasted_iota(jnp.int32, (v.shape[0], 128), 1)
        return jnp.where(lane == 0, jnp.sum(v, axis=1, keepdims=True), jnp.sum(v * v, axis=1, keepdims=True))

    me = 4 * y + row
    stat_g[me, :, :tok] = jnp.transpose(jnp.concatenate([row_sums(xa_v), row_sums(xb_v)], axis=0))[:8]
    with jax.named_scope('barrier'):
        pl.semaphore_wait(barrier, 7)

    def tok_copy(group, dy, dk):
        tk = (k + dk) % 2
        cols = pl.ds(pl.multiple_of(feat * tk, 128), feat)
        src, dst, sem = ((xa_v, x_ga, za_rsem), (xb_v, x_gb, zb_rsem))[group]
        return remote(src.at[:, cols], dst.at[row], z_ssem, sem, (dp, (y + dy) % 2, 2 * y + tk))

    def stat_copy(d):
        ty = (y + d // 4) % 2
        tr = (row + d % 4) % 4
        return remote(stat_g.at[me], stat_g.at[me], stat_ssem, stat_rsem, (dp, ty, tr))

    gain_cp = remote(gain_v.at[0], gain_v.at[1], misc_sem.at[2], misc_sem.at[3], y_next)
    half_cols = pl.ds(pl.multiple_of(feat * (1 - k), 128), feat)
    to_relay = remote(xa_v.at[:, half_cols], x_relay, z_ssem, misc_sem.at[9], y_next)
    from_relay = remote(x_relay, x_ga.at[row], z_ssem, za_rsem, (dp, y, 2 * (1 - x) + 1 - k))

    for d in range(1, 8):
        stat_copy(d).start()

    @pl.when(home == 0)
    def _():
        to_relay.start()
        tok_copy(1, 1, 0).start()
        tok_copy(1, 1, 1).start()
        tok_copy(1, 0, 0).start()
        tok_copy(1, 0, 1).start()
        tok_copy(0, 1, 0).start()
        tok_copy(0, 0, 0).start()
        tok_copy(0, 0, 1).start()

    @pl.when(home == 1)
    def _():
        gain_cp.start()
        for group in (1, 0):
            tok_copy(group, 0, 1).start()
            tok_copy(group, 1, 0).start()
            tok_copy(group, 1, 1).start()
        x_ga[row] = jnp.where(k == 0, xa_v[:, :feat], xa_v[:, feat:])
        x_gb[row] = jnp.where(k == 0, xb_v[:, :feat], xb_v[:, feat:])
        gain_v[1] = gain_v[0]
        with jax.named_scope('x_relay_wait'):
            to_relay.wait_recv()
        from_relay.start()

    @pl.when(home == 0)
    def _():
        with jax.named_scope('gain_wait'):
            gain_cp.wait_recv()
    gain = jnp.where(k == 0, gain_v[1, :feat], gain_v[1, feat:]).reshape(1, feat)
    acc[...] = jnp.zeros_like(acc)
    with jax.named_scope('stat_wait'):
        remote(stat_g.at[pl.ds(0, 7)], stat_g.at[pl.ds(0, 7)], stat_ssem, stat_rsem, y_next).wait_recv()

    def make_z(group):
        ref, sem = ((x_ga, za_rsem), (x_gb, zb_rsem))[group]

        @pl.when(home == 0)
        def _():
            with jax.named_scope('z_wait'):
                remote(ref, ref, z_ssem, sem, y_next).wait_recv()

        @pl.when(home == 1)
        def _():
            with jax.named_scope('z_wait'):
                remote(ref.at[pl.ds(0, 3)], ref.at[pl.ds(0, 3)], z_ssem, sem, y_next).wait_recv()

        t0, n, base = ((0, TA, 0), (TA, tb, rows_a))[group]
        for src in range(4):
            st = jnp.transpose(stat_g[src] + stat_g[4 + src])[t0:t0 + n] * (1.0 / (2 * half))
            mean = st[:, 0:1]
            var = st[:, 1:2] - mean * mean
            z = (ref[src].astype(F32) - mean) * lax.rsqrt(var + NORM_EPS) * gain
            z_v[pl.ds(base + n * src, n), :] = z.astype(BF16)

    row_group = (pl.ds(0, rows_a), pl.ds(rows_a, rows_b))

    def part_of(ref, j, part):
        if part == WHOLE:
            return ref.at[j]
        if part == FIRST:
            return ref.at[j, row_group[0]]
        return ref.at[pl.ds(j, part), row_group[1]]

    def rows_of(part):
        return pl.ds(0, rows_a + rows_b) if part == WHOLE else row_group[int(part > 0)]

    def d_copy(p, part, seq):
        return remote(part_of(d_send, p, part), part_of(d_recv, p, part), d_ssem, d_rsem.at[seq % RING], sibling)

    def b_index(j, part):
        return NA + j // 2 if part == 2 else j + 7

    def x_group(j, part, first, sem):
        return remote(part_of(own, first + j, part), part_of(x_recv, j, part), x_ssem, x_rsem.at[sem], x_next)

    def x_copy_of(j, part, first):
        sem = x_rsem.at[b_index(j, part)] if part > 0 else x_rsem.at[j]
        return remote(part_of(own, first + j, part), part_of(x_recv, j, part), x_ssem, sem, x_next)

    def c_copy(j):
        return c_part(j, WHOLE)

    def c_part(j, part):
        return remote(part_of(own, c0 + j, part), part_of(c_recv.at[0], j, part), c_ssem, c_rsem.at[j], y_next)

    def c_relay(j, part):
        sem = c_rsem.at[2 * NC + j // 3] if part > 0 else c_rsem.at[NC + j]
        return remote(part_of(c_recv.at[0], j, part), part_of(c_recv.at[1], j, part), c_ssem, sem, x_next)

    def pass_c(j):
        with jax.named_scope('c_wait'):
            c_copy(j).wait_recv()
        c_relay(j, FIRST).start()

    def up(p, part, seq):
        rows = rows_of(part)
        sums = jnp.dot(z_v[rows, :], w_in_v[p], preferred_element_type=F32)
        d_send[p, rows, :] = sums[:, :C]
        own[chunk_of(p), rows, :] = sums[:, C:]
        d_copy(p, part, seq).start()

    def pair_add(p, part, seq):
        with jax.named_scope('pair_wait'):
            d_copy(p, part, seq).wait_recv()
        q, rows = chunk_of(p), rows_of(part)
        own[q, rows, :] = own[q, rows, :] + d_recv[p, rows, :]

    def wait_w_in(p):
        with jax.named_scope('w_in_wait'):
            group = w_in_v.at[pl.ds(p, GROUP)]
            pltpu.make_async_copy(group, group, w_in_sem.at[p // GROUP]).wait()

    def pair_group(p, part, seq):
        pair_add(p, part, seq)
        q = chunk_of(p)

        @pl.when((q >= c0) & (q < a0))
        def _():
            c_part(q - c0, part).start()

        @pl.when((home == 1) & (q < c0))
        def _():
            x_group(q, part, 0, NA + q // 2 if part else q).start()

        @pl.when((home == 0) & (q >= a0))
        def _():
            x_group(q - a0, part, a0, q - a0).start()

    def pair_sum(p):
        pair_add(p, WHOLE, p + EARLY)
        q = chunk_of(p)

        @pl.when((q >= c0) & (q < a0))
        def _():
            c_copy(q - c0).start()

        @pl.when((home == 1) & (q < c0))
        def _():
            x_copy_of(q, FIRST, 0).start()

            @pl.when(q % 2 == 1)
            def _():
                x_copy_of(q - 1, 2, 0).start()

        @pl.when((home == 0) & (q >= a0 + NF))
        def _():
            x_copy_of(q - a0, FIRST, a0).start()

        @pl.when((home == 0) & (q >= a0) & (q < a0 + NF))
        def _():
            x_copy_of(q - a0, WHOLE, a0).start()

    def up_loop(lo, hi, part, seq, then):
        def step(p, _):
            if part != FIRST:
                @pl.when(p % GROUP == 0)
                def _():
                    wait_w_in(p)
            up(p, part, p + seq)
            if part != 1:
                w_out_copy(p).start()
            then(p)
            return 0

        lax.fori_loop(lo, hi, step, 0)

    def late(p):
        pair_sum(p - LAG)

        @pl.when((p == 17) & (home == 1))
        def _():
            pass_c(0)

    make_z(1)
    up_loop(0, EARLY, 1, 0, lambda p: None)
    pair_group(0, 1, 0)
    make_z(0)
    up_loop(0, LAG, FIRST, EARLY, lambda p: pair_group(p + 1, 1, p + 1))
    up_loop(LAG, EARLY, FIRST, EARLY, lambda p: pair_group(p - LAG, FIRST, p - LAG + EARLY))
    up_loop(EARLY, EARLY + LAG, WHOLE, EARLY, lambda p: pair_group(p - LAG, FIRST, p - LAG + EARLY))
    up_loop(EARLY + LAG, N, WHOLE, EARLY, late)
    for p in range(N - LAG, N):
        pair_sum(p)

    @pl.when(home == 0)
    def _():
        x_copy_of(NF, 2, a0).start()
        x_copy_of(NF + 2, 2, a0).start()
        for j in range(NF + 4, NA):
            x_copy_of(j, 1, a0).start()

    with jax.named_scope('w_out_wait'):
        pltpu.make_async_copy(w_out_v, w_out_v, w_out_sem).wait()

    def y_copy(j, part):
        sem = y_rsem.at[b_index(j, part)] if part > 0 else y_rsem.at[j]
        return remote(part_of(hall, j, part), part_of(hall, NA + j, part), y_ssem, sem, y_next)

    def b_sem(j, part):
        return b_rsem.at[NB + j // 2] if part > 0 else b_rsem.at[j]

    def relay_copy(j, part):
        return remote(part_of(hall, NA + j, part), part_of(hall, 2 * NA + j, part), b_ssem, b_sem(j, part), x_next)

    def back_copy(j, part):
        return remote(part_of(hall, 2 * NA + j, part), part_of(hall, 2 * NA + j, part), b_ssem, b_sem(j, part), y_next)

    def put_h(j, part, left, right):
        rows = rows_of(part)
        for c in range(max(part, 1)):
            total = left(c)[rows, :] + right(c)[rows, :]
            hall[j + c, rows, :] = jax.nn.gelu(total, approximate=True).astype(BF16)

    def make_h(j, part, first):
        with jax.named_scope('x_wait'):
            x_copy_of(j, part, 0).wait_recv()
        put_h(j, part, lambda c: own.at[first + j + c], lambda c: x_recv.at[j + c])
        y_copy(j, part).start()

    def make_h_c(j, part):
        with jax.named_scope('c_wait'):
            if part == FIRST:
                c_copy(j).wait_recv()
            c_relay(j, part).wait_recv()
        put_h(c0 + j, part, lambda c: c_recv.at[0, j + c], lambda c: c_recv.at[1, j + c])
        yc_copy(j, part).start()

    def yc_copy(j, part):
        sem = y_rsem.at[NA + 2 + j // 3] if part > 0 else y_rsem.at[c0 + j]
        return remote(part_of(hall, c0 + j, part), part_of(hall, NA + c0 + j, part), y_ssem, sem, y_next)

    def down(slot, i, part):
        rows = rows_of(part)
        parts = [jnp.dot(hall[slot + c, rows, :], w_out_v[i + c], preferred_element_type=F32)
                 for c in range(max(part, 1))]
        acc[rows, :] += sum(parts[1:], parts[0])

    e_recv, f_send, f_recv = (ea_recv, eb_recv), (fa_send, fb_send), (fa_recv, fb_recv)

    def token_rows(group, r):
        n, base = ((TA, 0), (tb, rows_a))[group]
        return pl.ds(pl.multiple_of(base + n * r, 8), n)

    def e_copy(group, s):
        r = 2 * (s * x + (1 - s) * (1 - x)) + 1 - k
        return remote(acc.at[token_rows(group, r)], e_recv[group].at[s], e_ssem, e_rsem.at[2 * group + s], sibling)

    def f_copy(group):
        return remote(f_send[group], f_recv[group], f_ssem, f_rsem.at[group], x_next)

    def end_start(group):
        e_copy(group, 0).start()
        e_copy(group, 1).start()

    def end_send(group):
        with jax.named_scope('e0_wait'):
            e_copy(group, 0).wait_recv()
        f_send[group][...] = acc[token_rows(group, 2 * (1 - x) + k), :] + e_recv[group][0]
        f_copy(group).start()

    def end_send_from(core):
        @pl.when(k == core)
        def _():
            end_send(0)

    def end_sum(group):
        with jax.named_scope('e1_wait'):
            e_copy(group, 1).wait_recv()
        with jax.named_scope('f_wait'):
            f_copy(group).wait_recv()
        total = acc[token_rows(group, row), :] + e_recv[group][1] + f_recv[group][...]
        t0, n = ((0, TA), (TA, tb))[group]
        out_v[t0:t0 + n, :] = ((xa_v, xb_v)[group][...].astype(F32) + total).astype(BF16)

    def loop(lo, hi, step):
        def body(i, _):
            step(i)
            return 0
        lax.fori_loop(lo, hi, body, 0)

    @pl.when(home == 1)
    def _():
        def relay(i, part):
            with jax.named_scope('relay_wait'):
                y_copy(i, part).wait_recv()
            relay_copy(i, part).start()

        def b_step(i, part):
            with jax.named_scope('b_wait'):
                back_copy(i, part).wait_recv()
            down(2 * NA + i, i, part)

        def c_step(i, part):
            with jax.named_scope('ch_wait'):
                yc_copy(i, part).wait_recv()
            down(NA + c0 + i, c0 + i, part)

        def a_step(j, part):
            make_h(j, part, a0)
            down(j, a0 + j, part)

        pass_c(1)

        def step(j):
            @pl.when(j == 2)
            def _():
                pass_c(2)
            a_step(j, WHOLE)

        loop(0, NF, step)

        def step(j):
            for t, i in ((4, 3), (6, 4)):
                @pl.when(j == t)
                def _():
                    pass_c(i)

            @pl.when(j == 7)
            def _():
                relay(0, FIRST)
                relay(1, FIRST)
            a_step(j, FIRST)

        loop(NF, 8, step)
        relay(2, FIRST)
        relay(3, FIRST)
        c_relay(0, 3).start()
        c_relay(3, 2).start()

        def step(t):
            a_step(8 + t, FIRST)

            @pl.when(t == 0)
            def _():
                relay(0, 2)
                relay(2, 2)

            @pl.when(t == 1)
            def _():
                c_step(1, FIRST)
            c_step(2 * t, FIRST)

        loop(0, 2, step)
        a_step(10, FIRST)
        loop(3, 5, lambda i: c_step(i, FIRST))
        a_step(NF, 2)
        loop(0, 2, lambda i: b_step(i, FIRST))
        a_step(NF + 2, 2)
        b_step(2, FIRST)
        make_h(NF + 4, 1, a0)
        b_step(NB - 1, FIRST)
        end_start(0)
        make_h(NF + 5, 1, a0)
        down(NF + 4, a0 + NF + 4, 1)
        make_h(NF + 6, 1, a0)
        end_send_from(0)
        loop(NF + 5, NA, lambda j: down(j, a0 + j, 1))
        end_send_from(1)
        c_step(0, 3)
        c_step(3, 2)
        loop(0, 2, lambda m: b_step(2 * m, 2))

    @pl.when(home == 0)
    def _():
        def a_step(j, part):
            with jax.named_scope('a_wait'):
                y_copy(j, part).wait_recv()
            down(NA + j, a0 + j, part)

        def b_step(i, part):
            with jax.named_scope('b_wait'):
                relay_copy(i, part).wait_recv()
            back_copy(i, part).start()
            down(2 * NA + i, i, part)

        def c_step(i, part):
            make_h_c(i, part)
            down(c0 + i, c0 + i, part)

        loop(0, NB, lambda j: make_h(j, FIRST, 0))
        loop(0, NB // 2, lambda m: make_h(2 * m, 2, 0))
        c_step(0, FIRST)

        def step(t):
            c_step(1 + t, FIRST)
            a_step(t, WHOLE)

        loop(0, NF, step)

        def step(t):
            b_step(t, FIRST)
            a_step(NF + t, FIRST)

        loop(0, 4, step)
        a_step(8, FIRST)
        c_step(0, 3)
        loop(9, NA, lambda j: a_step(j, FIRST))
        end_start(0)
        c_step(3, 2)
        end_send_from(0)
        loop(0, 2, lambda m: b_step(2 * m, 2))
        a_step(NF, 2)
        end_send_from(1)
        a_step(NF + 2, 2)
        loop(NF + 4, NA, lambda j: a_step(j, 1))

    end_start(1)
    end_send(1)

    def sent(ref, sem):
        remote(ref, ref, sem, sem, y_next).wait_send()

    with jax.named_scope('drain'):
        sent(stat_g.at[pl.ds(0, 7)], stat_ssem)
        sent(d_send, d_ssem)
        sent(hall.at[pl.ds(0, NB)], b_ssem)
        sent(c_recv.at[0], c_ssem)
        sent(ea_recv, e_ssem)
        sent(eb_recv, e_ssem)

        @pl.when(home == 0)
        def _():
            sent(x_ga, z_ssem)
            sent(x_gb, z_ssem)
            sent(own.at[pl.ds(0, NA)], x_ssem)
            sent(hall.at[pl.ds(0, NB + NC)], y_ssem)

        @pl.when(home == 1)
        def _():
            gain_cp.wait_send()
            sent(x_ga, z_ssem)
            sent(x_gb.at[pl.ds(0, 3)], z_ssem)
            sent(own.at[pl.ds(0, NB)], x_ssem)
            sent(c_recv.at[1], c_ssem)
            sent(hall.at[pl.ds(0, NA)], y_ssem)

    end_sum(0)
    end_sum(1)
    sent(fa_send, f_ssem)
    sent(fb_send, f_ssem)


def solution(mesh):
    def body(x_blk, gain_blk, w_in_blk, w_out_blk):
        tok, half = x_blk.shape
        feat = w_in_blk.shape[0]
        tokens = 4 * tok
        dma = pltpu.SemaphoreType.DMA
        return pl.pallas_call(
            kernel,
            out_shape=pltpu.VMEM((tok, half), BF16),
            in_specs=[pl.BlockSpec(memory_space=pl.ANY)] * 4,
            out_specs=pl.BlockSpec(memory_space=pltpu.VMEM),
            scratch_shapes=[
                pltpu.VMEM((TA, half), BF16),
                pltpu.VMEM((tok - TA, half), BF16),
                pltpu.VMEM((2, half), F32),
                pltpu.VMEM((8, 8, 128), F32),
                pltpu.VMEM((4, TA, feat), BF16),
                pltpu.VMEM((4, tok - TA, feat), BF16),
                pltpu.VMEM((TA, feat), BF16),
                pltpu.VMEM((tokens, feat), BF16),
                pltpu.VMEM((N, feat, 2 * C), BF16),
                pltpu.VMEM((N, C, half), BF16),
                pltpu.VMEM((N, tokens, C), F32),
                pltpu.VMEM((N, tokens, C), F32),
                pltpu.VMEM((N, tokens, C), F32),
                pltpu.VMEM((NA, tokens, C), F32),
                pltpu.VMEM((2, NC, tokens, C), F32),
                pltpu.VMEM((2 * NA + NB, tokens, C), BF16),
                pltpu.VMEM((tokens, half), F32),
                pltpu.VMEM((2, TA, half), F32),
                pltpu.VMEM((2, tok - TA, half), F32),
                pltpu.VMEM((TA, half), F32),
                pltpu.VMEM((TA, half), F32),
                pltpu.VMEM((tok - TA, half), F32),
                pltpu.VMEM((tok - TA, half), F32),
                dma((10,)),
                dma((N // GROUP,)),
                dma((9,)),
                dma((RING,)),
                dma((NA + 7,)),
                dma((NA + 7,)),
                dma((NB + NB // 2,)),
                dma((2 * NC + 2,)),
                dma((4,)),
                dma((2,)),
            ],
            compiler_params=pltpu.CompilerParams(
                collective_id=0, has_side_effects=True, vmem_limit_bytes=66_500_000
            ),
        )(x_blk, gain_blk, w_in_blk, w_out_blk)

    return jax.shard_map(
        body,
        mesh=mesh,
        in_specs=(P(("dp", "row"), "col"), P("col"), P("row", "col"), P("row", "col")),
        out_specs=P(("dp", "row"), "col"),
        check_vma=False,
    )
```

```python
import jax
import jax.numpy as jnp
from jax import lax
from jax.experimental import pallas as pl
from jax.experimental.pallas import tpu as pltpu
from jax.sharding import PartitionSpec as P

NORM_EPS = 1e-5
MESH = pl.DeviceIdType.MESH
WHOLE, FIRST = -1, 0
F32 = jnp.float32
BF16 = jnp.bfloat16

C = 256
NB = 4
NC = 5
NA = 11
N = NA + NB + NC
NF = 4
EARLY = 4
GROUP = 10
LAG = 3
RING = 8
TA = 16


def kernel(x_hbm, gain_hbm, w_in_hbm, w_out_hbm, out_v,
           xa_v, xb_v, gain_v, stat_g, x_ga, x_gb, x_relay, z_v, w_in_v, w_out_v, d_send, d_recv, own, x_recv, c_recv, hall,
           acc, ea_recv, eb_recv, fa_send, fa_recv, fb_send, fb_recv,
           misc_sem, w_in_sem, send_sem, d_rsem, x_rsem, y_rsem, b_rsem, c_rsem, e_rsem, f_rsem):
    w_out_sem, stat_rsem, za_rsem, zb_rsem = [misc_sem.at[i] for i in range(4, 8)]
    stat_ssem = z_ssem = d_ssem = x_ssem = y_ssem = b_ssem = c_ssem = e_ssem = send_sem.at[0]
    f_ssem = send_sem.at[1]
    y = lax.axis_index("col")
    row = lax.axis_index("row")
    x = row // 2
    k = row % 2
    dp = lax.axis_index("dp")
    home = 1 - (x + y) % 2
    tok, half = out_v.shape
    feat = half // 2
    block = N * C
    rows_a = 4 * TA
    tb = tok - TA
    rows_b = 4 * tb
    sibling = (dp, y, 2 * x + 1 - k)
    x_next = (dp, y, 2 * (1 - x) + k)
    y_next = (dp, 1 - y, row)

    def remote(src, dst, ssem, rsem, dev):
        return pltpu.make_async_remote_copy(src_ref=src, dst_ref=dst, send_sem=ssem, recv_sem=rsem,
                                            device_id=dev, device_id_type=MESH)

    c0, a0 = NB, NB + NC

    def chunk_of(p):
        u = p - 2 * NB - 1
        pair = jnp.where(p % 2 == 1, c0 + p // 2, p // 2 + (1 - home) * a0)
        mixed = jnp.where(u % 2 == 1, u // 2, a0 + NB + u // 2)
        late = jnp.where((home == 1) | (u >= 2 * NB), a0 + u, mixed)
        return jnp.where(p < 2 * NB, pair, jnp.where(u < 0, a0 - 1, late))

    def w_in_copies(p):
        c = C * chunk_of(p)
        cs = pl.multiple_of((1 - k) * block + c, C)
        co = pl.multiple_of(k * block + c, C)
        return (pltpu.make_async_copy(w_in_hbm.at[:, pl.ds(cs, C)], w_in_v.at[p, :, pl.ds(0, C)], w_in_sem.at[p // GROUP]),
                pltpu.make_async_copy(w_in_hbm.at[:, pl.ds(co, C)], w_in_v.at[p, :, pl.ds(C, C)], w_in_sem.at[p // GROUP]))

    def w_out_copy(i):
        r = pl.multiple_of(i * C, C)
        return pltpu.make_async_copy(w_out_hbm.at[pl.ds(r, C), :], w_out_v.at[i], w_out_sem)

    xa_copy = pltpu.make_async_copy(x_hbm.at[pl.ds(0, TA)], xa_v, misc_sem.at[0])
    xb_copy = pltpu.make_async_copy(x_hbm.at[pl.ds(TA, tb)], xb_v, misc_sem.at[8])
    g_copy = pltpu.make_async_copy(gain_hbm, gain_v.at[0], misc_sem.at[1])
    xa_copy.start()
    xb_copy.start()
    g_copy.start()

    barrier = pltpu.get_barrier_semaphore()
    for dy in range(2):
        for dr in range(4):
            if dy or dr:
                pl.semaphore_signal(barrier, inc=1, device_id=(dp, (y + dy) % 2, (row + dr) % 4), device_id_type=MESH)

    def start_w_in(p, _):
        for cp in w_in_copies(p):
            cp.start()
        return 0

    lax.fori_loop(0, N, start_w_in, 0)

    xa_copy.wait()
    xb_copy.wait()
    g_copy.wait()

    def row_sums(ref):
        v = ref[...].astype(F32)
        lane = lax.broadcasted_iota(jnp.int32, (v.shape[0], 128), 1)
        return jnp.where(lane == 0, jnp.sum(v, axis=1, keepdims=True), jnp.sum(v * v, axis=1, keepdims=True))

    me = 4 * y + row
    stat_g[me, :, :tok] = jnp.transpose(jnp.concatenate([row_sums(xa_v), row_sums(xb_v)], axis=0))[:8]
    with jax.named_scope('barrier'):
        pl.semaphore_wait(barrier, 7)

    def tok_copy(group, dy, dk):
        tk = (k + dk) % 2
        cols = pl.ds(pl.multiple_of(feat * tk, 128), feat)
        src, dst, sem = ((xa_v, x_ga, za_rsem), (xb_v, x_gb, zb_rsem))[group]
        return remote(src.at[:, cols], dst.at[row], z_ssem, sem, (dp, (y + dy) % 2, 2 * y + tk))

    def stat_copy(d):
        ty = (y + d // 4) % 2
        tr = (row + d % 4) % 4
        return remote(stat_g.at[me], stat_g.at[me], stat_ssem, stat_rsem, (dp, ty, tr))

    gain_cp = remote(gain_v.at[0], gain_v.at[1], z_ssem, misc_sem.at[3], y_next)
    half_cols = pl.ds(pl.multiple_of(feat * (1 - k), 128), feat)
    to_relay = remote(xa_v.at[:, half_cols], x_relay, z_ssem, misc_sem.at[2], y_next)
    from_relay = remote(x_relay, x_ga.at[row], z_ssem, za_rsem, (dp, y, 2 * (1 - x) + 1 - k))

    for d in range(1, 8):
        stat_copy(d).start()

    @pl.when(home == 0)
    def _():
        to_relay.start()
        tok_copy(1, 1, 0).start()
        tok_copy(1, 1, 1).start()
        tok_copy(1, 0, 0).start()
        tok_copy(1, 0, 1).start()
        tok_copy(0, 1, 0).start()
        tok_copy(0, 0, 0).start()
        tok_copy(0, 0, 1).start()

    @pl.when(home == 1)
    def _():
        gain_cp.start()
        for group in (1, 0):
            tok_copy(group, 0, 1).start()
            tok_copy(group, 1, 0).start()
            tok_copy(group, 1, 1).start()
        x_ga[row] = jnp.where(k == 0, xa_v[:, :feat], xa_v[:, feat:])
        x_gb[row] = jnp.where(k == 0, xb_v[:, :feat], xb_v[:, feat:])
        gain_v[1] = gain_v[0]
        with jax.named_scope('x_relay_wait'):
            to_relay.wait_recv()
        from_relay.start()

    @pl.when(home == 0)
    def _():
        with jax.named_scope('gain_wait'):
            gain_cp.wait_recv()
    gain = jnp.where(k == 0, gain_v[1, :feat], gain_v[1, feat:]).reshape(1, feat)
    acc[...] = jnp.zeros_like(acc)
    with jax.named_scope('stat_wait'):
        remote(stat_g.at[pl.ds(0, 7)], stat_g.at[pl.ds(0, 7)], stat_ssem, stat_rsem, y_next).wait_recv()

    def make_z(group):
        ref, sem = ((x_ga, za_rsem), (x_gb, zb_rsem))[group]

        @pl.when(home == 0)
        def _():
            with jax.named_scope('z_wait'):
                remote(ref, ref, z_ssem, sem, y_next).wait_recv()

        @pl.when(home == 1)
        def _():
            with jax.named_scope('z_wait'):
                remote(ref.at[pl.ds(0, 3)], ref.at[pl.ds(0, 3)], z_ssem, sem, y_next).wait_recv()

        t0, n, base = ((0, TA, 0), (TA, tb, rows_a))[group]
        for src in range(4):
            st = jnp.transpose(stat_g[src] + stat_g[4 + src])[t0:t0 + n] * (1.0 / (2 * half))
            mean = st[:, 0:1]
            var = st[:, 1:2] - mean * mean
            z = (ref[src].astype(F32) - mean) * lax.rsqrt(var + NORM_EPS) * gain
            z_v[pl.ds(base + n * src, n), :] = z.astype(BF16)

    row_group = (pl.ds(0, rows_a), pl.ds(rows_a, rows_b))

    def part_of(ref, j, part):
        if part == WHOLE:
            return ref.at[j]
        if part == FIRST:
            return ref.at[j, row_group[0]]
        return ref.at[pl.ds(j, part), row_group[1]]

    def rows_of(part):
        return pl.ds(0, rows_a + rows_b) if part == WHOLE else row_group[int(part > 0)]

    def d_copy(p, part, seq):
        return remote(part_of(d_send, p, part), part_of(d_recv, p, part), d_ssem, d_rsem.at[seq % RING], sibling)

    def b_index(j, part):
        return 9 + j // 2 if part == 2 else j + 5

    def x_group(j, part, first, sem):
        return remote(part_of(own, first + j, part), part_of(x_recv, j, part), x_ssem, x_rsem.at[sem], x_next)

    def x_copy_of(j, part, first):
        sem = x_rsem.at[b_index(j, part)] if part > 0 else x_rsem.at[j]
        return remote(part_of(own, first + j, part), part_of(x_recv, j, part), x_ssem, sem, x_next)

    def c_copy(j):
        return c_part(j, WHOLE)

    def c_part(j, part):
        return remote(part_of(own, c0 + j, part), part_of(c_recv.at[0], j, part), c_ssem, c_rsem.at[j], y_next)

    def c_relay(j, part):
        sem = c_rsem.at[2 * NC + j // 3] if part > 0 else c_rsem.at[NC + j]
        return remote(part_of(c_recv.at[0], j, part), part_of(c_recv.at[1], j, part), c_ssem, sem, x_next)

    def pass_c(j):
        with jax.named_scope('c_wait'):
            c_copy(j).wait_recv()
        c_relay(j, FIRST).start()

    def up(p, part, seq):
        rows = rows_of(part)
        sums = jnp.dot(z_v[rows, :], w_in_v[p], preferred_element_type=F32)
        d_send[p, rows, :] = sums[:, :C]
        own[chunk_of(p), rows, :] = sums[:, C:]
        d_copy(p, part, seq).start()

    def pair_add(p, part, seq):
        with jax.named_scope('pair_wait'):
            d_copy(p, part, seq).wait_recv()
        q, rows = chunk_of(p), rows_of(part)
        own[q, rows, :] = own[q, rows, :] + d_recv[p, rows, :]

    def wait_w_in(p):
        with jax.named_scope('w_in_wait'):
            group = w_in_v.at[pl.ds(p, GROUP)]
            pltpu.make_async_copy(group, group, w_in_sem.at[p // GROUP]).wait()

    def pair_group(p, part, seq):
        pair_add(p, part, seq)
        q = chunk_of(p)

        @pl.when((q >= c0) & (q < a0))
        def _():
            c_part(q - c0, part).start()

        @pl.when((home == 1) & (q < c0))
        def _():
            x_group(q, part, 0, 9 + q // 2 if part else q).start()

        @pl.when((home == 0) & (q >= a0))
        def _():
            x_group(q - a0, part, a0, q - a0).start()

    def pair_sum(p):
        pair_add(p, WHOLE, p + EARLY)
        q = chunk_of(p)

        @pl.when((q >= c0) & (q < a0))
        def _():
            c_copy(q - c0).start()

        @pl.when((home == 1) & (q < c0))
        def _():
            x_copy_of(q, FIRST, 0).start()

            @pl.when(q % 2 == 1)
            def _():
                x_copy_of(q - 1, 2, 0).start()

        @pl.when((home == 0) & (q >= a0 + NF))
        def _():
            x_copy_of(q - a0, FIRST, a0).start()

        @pl.when((home == 0) & (q >= a0) & (q < a0 + NF))
        def _():
            x_copy_of(q - a0, WHOLE, a0).start()

    def up_loop(lo, hi, part, seq, then):
        def step(p, _):
            if part != FIRST:
                @pl.when(p % GROUP == 0)
                def _():
                    wait_w_in(p)
            up(p, part, p + seq)
            if part != 1:
                w_out_copy(p).start()
            then(p)
            return 0

        lax.fori_loop(lo, hi, step, 0)

    def late(p):
        pair_sum(p - LAG)

        @pl.when((p == 17) & (home == 1))
        def _():
            pass_c(0)

    make_z(1)
    up_loop(0, EARLY, 1, 0, lambda p: None)
    pair_group(0, 1, 0)
    make_z(0)
    up_loop(0, LAG, FIRST, EARLY, lambda p: pair_group(p + 1, 1, p + 1))
    up_loop(LAG, EARLY, FIRST, EARLY, lambda p: pair_group(p - LAG, FIRST, p - LAG + EARLY))
    up_loop(EARLY, EARLY + LAG, WHOLE, EARLY, lambda p: pair_group(p - LAG, FIRST, p - LAG + EARLY))
    up_loop(EARLY + LAG, N, WHOLE, EARLY, late)
    for p in range(N - LAG, N):
        pair_sum(p)

    @pl.when(home == 0)
    def _():
        x_copy_of(NF, 2, a0).start()
        x_copy_of(NF + 2, 2, a0).start()
        for j in range(NF + 4, NA):
            x_copy_of(j, 1, a0).start()

    with jax.named_scope('w_out_wait'):
        pltpu.make_async_copy(w_out_v, w_out_v, w_out_sem).wait()

    def y_copy(j, part):
        sem = y_rsem.at[b_index(j, part)] if part > 0 else y_rsem.at[j]
        return remote(part_of(hall, j, part), part_of(hall, NA + j, part), y_ssem, sem, y_next)

    def b_sem(j, part):
        return b_rsem.at[NB + j // 2] if part > 0 else b_rsem.at[j]

    def relay_copy(j, part):
        return remote(part_of(hall, NA + j, part), part_of(hall, 2 * NA + j, part), b_ssem, b_sem(j, part), x_next)

    def back_copy(j, part):
        return remote(part_of(hall, 2 * NA + j, part), part_of(hall, 2 * NA + j, part), b_ssem, b_sem(j, part), y_next)

    def put_h(j, part, left, right):
        rows = rows_of(part)
        for c in range(max(part, 1)):
            total = left(c)[rows, :] + right(c)[rows, :]
            hall[j + c, rows, :] = jax.nn.gelu(total, approximate=True).astype(BF16)

    def make_h(j, part, first):
        with jax.named_scope('x_wait'):
            x_copy_of(j, part, 0).wait_recv()
        put_h(j, part, lambda c: own.at[first + j + c], lambda c: x_recv.at[j + c])
        y_copy(j, part).start()

    def make_h_c(j, part):
        with jax.named_scope('c_wait'):
            if part == FIRST:
                c_copy(j).wait_recv()
            c_relay(j, part).wait_recv()
        put_h(c0 + j, part, lambda c: c_recv.at[0, j + c], lambda c: c_recv.at[1, j + c])
        yc_copy(j, part).start()

    def yc_copy(j, part):
        sem = y_rsem.at[NA + j // 3] if part > 0 else y_rsem.at[c0 + j]
        return remote(part_of(hall, c0 + j, part), part_of(hall, NA + c0 + j, part), y_ssem, sem, y_next)

    def down(slot, i, part):
        rows = rows_of(part)
        parts = [jnp.dot(hall[slot + c, rows, :], w_out_v[i + c], preferred_element_type=F32)
                 for c in range(max(part, 1))]
        acc[rows, :] += sum(parts[1:], parts[0])

    e_recv, f_send, f_recv = (ea_recv, eb_recv), (fa_send, fb_send), (fa_recv, fb_recv)

    def token_rows(group, r):
        n, base = ((TA, 0), (tb, rows_a))[group]
        return pl.ds(pl.multiple_of(base + n * r, 8), n)

    def e_copy(group, s):
        r = 2 * (s * x + (1 - s) * (1 - x)) + 1 - k
        return remote(acc.at[token_rows(group, r)], e_recv[group].at[s], e_ssem, e_rsem.at[2 * group + s], sibling)

    def f_copy(group):
        return remote(f_send[group], f_recv[group], f_ssem, f_rsem.at[group], x_next)

    def end_start(group):
        e_copy(group, 0).start()
        e_copy(group, 1).start()

    def end_send(group):
        with jax.named_scope('e0_wait'):
            e_copy(group, 0).wait_recv()
        f_send[group][...] = acc[token_rows(group, 2 * (1 - x) + k), :] + e_recv[group][0]
        f_copy(group).start()

    def end_send_from(core):
        @pl.when(k == core)
        def _():
            end_send(0)

    def end_sum(group):
        with jax.named_scope('e1_wait'):
            e_copy(group, 1).wait_recv()
        with jax.named_scope('f_wait'):
            f_copy(group).wait_recv()
        total = acc[token_rows(group, row), :] + e_recv[group][1] + f_recv[group][...]
        t0, n = ((0, TA), (TA, tb))[group]
        out_v[t0:t0 + n, :] = ((xa_v, xb_v)[group][...].astype(F32) + total).astype(BF16)

    def loop(lo, hi, step):
        def body(i, _):
            step(i)
            return 0
        lax.fori_loop(lo, hi, body, 0)

    @pl.when(home == 1)
    def _():
        def relay(i, part):
            with jax.named_scope('relay_wait'):
                y_copy(i, part).wait_recv()
            relay_copy(i, part).start()

        def b_step(i, part):
            with jax.named_scope('b_wait'):
                back_copy(i, part).wait_recv()
            down(2 * NA + i, i, part)

        def c_step(i, part):
            with jax.named_scope('ch_wait'):
                yc_copy(i, part).wait_recv()
            down(NA + c0 + i, c0 + i, part)

        def a_step(j, part):
            make_h(j, part, a0)
            down(j, a0 + j, part)

        pass_c(1)

        def step(j):
            @pl.when(j == 2)
            def _():
                pass_c(2)
            a_step(j, WHOLE)

        loop(0, NF, step)

        def step(j):
            for t, i in ((4, 3), (6, 4)):
                @pl.when(j == t)
                def _():
                    pass_c(i)

            @pl.when(j == 7)
            def _():
                relay(0, FIRST)
                relay(1, FIRST)
            a_step(j, FIRST)

        loop(NF, 8, step)
        relay(2, FIRST)
        relay(3, FIRST)
        c_relay(0, 3).start()
        c_relay(3, 2).start()

        def step(t):
            a_step(8 + t, FIRST)

            @pl.when(t == 0)
            def _():
                relay(0, 2)
                relay(2, 2)

            @pl.when(t == 1)
            def _():
                c_step(1, FIRST)
            c_step(2 * t, FIRST)

        loop(0, 2, step)
        a_step(10, FIRST)
        loop(3, 5, lambda i: c_step(i, FIRST))
        a_step(NF, 2)
        loop(0, 2, lambda i: b_step(i, FIRST))
        a_step(NF + 2, 2)
        b_step(2, FIRST)
        make_h(NF + 4, 1, a0)
        b_step(NB - 1, FIRST)
        end_start(0)
        make_h(NF + 5, 1, a0)
        down(NF + 4, a0 + NF + 4, 1)
        make_h(NF + 6, 1, a0)
        end_send_from(0)
        loop(NF + 5, NA, lambda j: down(j, a0 + j, 1))
        end_send_from(1)
        c_step(0, 3)
        c_step(3, 2)
        loop(0, 2, lambda m: b_step(2 * m, 2))

    @pl.when(home == 0)
    def _():
        def a_step(j, part):
            with jax.named_scope('a_wait'):
                y_copy(j, part).wait_recv()
            down(NA + j, a0 + j, part)

        def b_pass(i, part):
            with jax.named_scope('b_wait'):
                relay_copy(i, part).wait_recv()
            back_copy(i, part).start()

        def b_step(i, part):
            b_pass(i, part)
            down(2 * NA + i, i, part)

        def c_step(i, part):
            make_h_c(i, part)
            down(c0 + i, c0 + i, part)

        loop(0, NB, lambda j: make_h(j, FIRST, 0))
        loop(0, NB // 2, lambda m: make_h(2 * m, 2, 0))
        c_step(0, FIRST)

        def step(t):
            c_step(1 + t, FIRST)
            a_step(t, WHOLE)

        loop(0, NF, step)

        def step(t):
            b_step(t, FIRST)
            a_step(NF + t, FIRST)

        loop(0, 4, step)
        loop(8, 10, lambda j: a_step(j, FIRST))
        c_step(0, 3)
        a_step(10, FIRST)
        end_start(0)
        end_send_from(0)
        c_step(3, 2)
        b_pass(0, 2)
        b_pass(2, 2)
        down(2 * NA, 0, 4)
        a_step(NF, 2)
        end_send_from(1)
        a_step(NF + 2, 2)
        loop(NF + 4, NA, lambda j: a_step(j, 1))

    end_start(1)
    end_send(1)

    def sent(ref, sem):
        remote(ref, ref, sem, sem, y_next).wait_send()

    with jax.named_scope('drain'):
        sent(stat_g.at[pl.ds(0, 7)], stat_ssem)
        sent(d_send, d_ssem)
        sent(hall.at[pl.ds(0, NB)], b_ssem)
        sent(c_recv.at[0], c_ssem)
        sent(ea_recv, e_ssem)
        sent(eb_recv, e_ssem)

        @pl.when(home == 0)
        def _():
            sent(x_ga, z_ssem)
            sent(x_gb, z_ssem)
            sent(own.at[pl.ds(0, NA)], x_ssem)
            sent(hall.at[pl.ds(0, NB + NC)], y_ssem)

        @pl.when(home == 1)
        def _():
            gain_cp.wait_send()
            sent(x_ga, z_ssem)
            sent(x_gb.at[pl.ds(0, 3)], z_ssem)
            sent(own.at[pl.ds(0, NB)], x_ssem)
            sent(c_recv.at[1], c_ssem)
            sent(hall.at[pl.ds(0, NA)], y_ssem)

    end_sum(0)
    end_sum(1)
    sent(fa_send, f_ssem)
    sent(fb_send, f_ssem)


def solution(mesh):
    def body(x_blk, gain_blk, w_in_blk, w_out_blk):
        tok, half = x_blk.shape
        feat = w_in_blk.shape[0]
        tokens = 4 * tok
        dma = pltpu.SemaphoreType.DMA
        return pl.pallas_call(
            kernel,
            out_shape=pltpu.VMEM((tok, half), BF16),
            in_specs=[pl.BlockSpec(memory_space=pl.ANY)] * 4,
            out_specs=pl.BlockSpec(memory_space=pltpu.VMEM),
            scratch_shapes=[
                pltpu.VMEM((TA, half), BF16),
                pltpu.VMEM((tok - TA, half), BF16),
                pltpu.VMEM((2, half), F32),
                pltpu.VMEM((8, 8, 128), F32),
                pltpu.VMEM((4, TA, feat), BF16),
                pltpu.VMEM((4, tok - TA, feat), BF16),
                pltpu.VMEM((TA, feat), BF16),
                pltpu.VMEM((tokens, feat), BF16),
                pltpu.VMEM((N, feat, 2 * C), BF16),
                pltpu.VMEM((N, C, half), BF16),
                pltpu.VMEM((N, tokens, C), F32),
                pltpu.VMEM((N, tokens, C), F32),
                pltpu.VMEM((N, tokens, C), F32),
                pltpu.VMEM((NA, tokens, C), F32),
                pltpu.VMEM((2, NC, tokens, C), F32),
                pltpu.VMEM((2 * NA + NB, tokens, C), BF16),
                pltpu.VMEM((tokens, half), F32),
                pltpu.VMEM((2, TA, half), F32),
                pltpu.VMEM((2, tok - TA, half), F32),
                pltpu.VMEM((TA, half), F32),
                pltpu.VMEM((TA, half), F32),
                pltpu.VMEM((tok - TA, half), F32),
                pltpu.VMEM((tok - TA, half), F32),
                dma((9,)),
                dma((N // GROUP,)),
                dma((2,)),
                dma((RING,)),
                dma((NA + 5,)),
                dma((NA + 5,)),
                dma((NB + NB // 2,)),
                dma((2 * NC + 2,)),
                dma((4,)),
                dma((2,)),
            ],
            compiler_params=pltpu.CompilerParams(
                collective_id=0, has_side_effects=True, vmem_limit_bytes=66_500_000
            ),
        )(x_blk, gain_blk, w_in_blk, w_out_blk)

    return jax.shard_map(
        body,
        mesh=mesh,
        in_specs=(P(("dp", "row"), "col"), P("col"), P("row", "col"), P("row", "col")),
        out_specs=P(("dp", "row"), "col"),
        check_vma=False,
    )
```

```python
import jax
import jax.numpy as jnp
from jax import lax
from jax.experimental import pallas as pl
from jax.experimental.pallas import tpu as pltpu
from jax.sharding import PartitionSpec as P

NORM_EPS = 1e-5
MESH = pl.DeviceIdType.MESH
WHOLE, FIRST = -1, 0
F32 = jnp.float32
BF16 = jnp.bfloat16

C = 256
NB = 4
NC = 5
NA = 11
N = NA + NB + NC
NF = 4
EARLY = 6
GROUP = 10
LAG = 3
RING = 10
TA = 16


def kernel(x_hbm, gain_hbm, w_in_hbm, w_out_hbm, out_v,
           xa_v, xb_v, gain_v, stat_g, x_ga, x_gb, x_relay, z_v, w_in_v, w_out_v, d_send, d_recv, own, x_recv, c_recv, hall,
           acc, ea_recv, eb_recv, fa_send, fa_recv, fb_send, fb_recv,
           misc_sem, w_in_sem, send_sem, d_rsem, x_rsem, y_rsem, b_rsem, c_rsem, e_rsem, f_rsem):
    w_out_sem, stat_rsem, za_rsem, zb_rsem = [misc_sem.at[i] for i in range(4, 8)]
    stat_ssem = z_ssem = d_ssem = x_ssem = y_ssem = b_ssem = c_ssem = e_ssem = send_sem.at[0]
    f_ssem = send_sem.at[1]
    y = lax.axis_index("col")
    row = lax.axis_index("row")
    x = row // 2
    k = row % 2
    dp = lax.axis_index("dp")
    home = 1 - (x + y) % 2
    tok, half = out_v.shape
    feat = half // 2
    block = N * C
    rows_a = 4 * TA
    tb = tok - TA
    rows_b = 4 * tb
    sibling = (dp, y, 2 * x + 1 - k)
    x_next = (dp, y, 2 * (1 - x) + k)
    y_next = (dp, 1 - y, row)

    def remote(src, dst, ssem, rsem, dev):
        return pltpu.make_async_remote_copy(src_ref=src, dst_ref=dst, send_sem=ssem, recv_sem=rsem,
                                            device_id=dev, device_id_type=MESH)

    c0, a0 = NB, NB + NC

    def chunk_of(p):
        u = p - 2 * NB - 1
        pair = jnp.where(p % 2 == 1, c0 + p // 2, p // 2 + (1 - home) * a0)
        mixed = jnp.where(u % 2 == 1, u // 2, a0 + NB + u // 2)
        late = jnp.where((home == 1) | (u >= 2 * NB), a0 + u, mixed)
        return jnp.where(p < 2 * NB, pair, jnp.where(u < 0, a0 - 1, late))

    def w_in_copies(p):
        c = C * chunk_of(p)
        cs = pl.multiple_of((1 - k) * block + c, C)
        co = pl.multiple_of(k * block + c, C)
        return (pltpu.make_async_copy(w_in_hbm.at[:, pl.ds(cs, C)], w_in_v.at[p, :, pl.ds(0, C)], w_in_sem.at[p // GROUP]),
                pltpu.make_async_copy(w_in_hbm.at[:, pl.ds(co, C)], w_in_v.at[p, :, pl.ds(C, C)], w_in_sem.at[p // GROUP]))

    def w_out_copy(i):
        r = pl.multiple_of(i * C, C)
        return pltpu.make_async_copy(w_out_hbm.at[pl.ds(r, C), :], w_out_v.at[i], w_out_sem)

    xa_copy = pltpu.make_async_copy(x_hbm.at[pl.ds(0, TA)], xa_v, misc_sem.at[0])
    xb_copy = pltpu.make_async_copy(x_hbm.at[pl.ds(TA, tb)], xb_v, misc_sem.at[8])
    g_copy = pltpu.make_async_copy(gain_hbm, gain_v.at[0], misc_sem.at[1])
    xa_copy.start()
    xb_copy.start()
    g_copy.start()

    barrier = pltpu.get_barrier_semaphore()
    for dy in range(2):
        for dr in range(4):
            if dy or dr:
                pl.semaphore_signal(barrier, inc=1, device_id=(dp, (y + dy) % 2, (row + dr) % 4), device_id_type=MESH)

    def start_w_in(p, _):
        for cp in w_in_copies(p):
            cp.start()
        return 0

    lax.fori_loop(0, N, start_w_in, 0)

    xa_copy.wait()
    xb_copy.wait()
    g_copy.wait()

    def row_sums(ref):
        v = ref[...].astype(F32)
        lane = lax.broadcasted_iota(jnp.int32, (v.shape[0], 128), 1)
        return jnp.where(lane == 0, jnp.sum(v, axis=1, keepdims=True), jnp.sum(v * v, axis=1, keepdims=True))

    me = 4 * y + row
    stat_g[me, :, :tok] = jnp.transpose(jnp.concatenate([row_sums(xa_v), row_sums(xb_v)], axis=0))[:2]
    with jax.named_scope('barrier'):
        pl.semaphore_wait(barrier, 7)

    def tok_copy(group, dy, dk):
        tk = (k + dk) % 2
        cols = pl.ds(pl.multiple_of(feat * tk, 128), feat)
        src, dst, sem = ((xa_v, x_ga, za_rsem), (xb_v, x_gb, zb_rsem))[group]
        return remote(src.at[:, cols], dst.at[row], z_ssem, sem, (dp, (y + dy) % 2, 2 * y + tk))

    def stat_copy(d):
        ty = (y + d // 4) % 2
        tr = (row + d % 4) % 4
        return remote(stat_g.at[me], stat_g.at[me], stat_ssem, stat_rsem, (dp, ty, tr))

    gain_cp = remote(gain_v.at[0], gain_v.at[1], z_ssem, misc_sem.at[3], y_next)
    half_cols = pl.ds(pl.multiple_of(feat * (1 - k), 128), feat)
    to_relay = remote(xa_v.at[:, half_cols], x_relay, z_ssem, misc_sem.at[2], y_next)
    from_relay = remote(x_relay, x_ga.at[row], z_ssem, za_rsem, (dp, y, 2 * (1 - x) + 1 - k))

    for d in range(1, 8):
        stat_copy(d).start()

    @pl.when(home == 0)
    def _():
        to_relay.start()
        tok_copy(1, 1, 0).start()
        tok_copy(1, 1, 1).start()
        tok_copy(1, 0, 0).start()
        tok_copy(1, 0, 1).start()
        tok_copy(0, 1, 0).start()
        tok_copy(0, 0, 0).start()
        tok_copy(0, 0, 1).start()

    @pl.when(home == 1)
    def _():
        gain_cp.start()
        for group in (1, 0):
            tok_copy(group, 0, 1).start()
            tok_copy(group, 1, 0).start()
            tok_copy(group, 1, 1).start()
        x_ga[row] = jnp.where(k == 0, xa_v[:, :feat], xa_v[:, feat:])
        x_gb[row] = jnp.where(k == 0, xb_v[:, :feat], xb_v[:, feat:])
        gain_v[1] = gain_v[0]
        with jax.named_scope('x_relay_wait'):
            to_relay.wait_recv()
        from_relay.start()

    @pl.when(home == 0)
    def _():
        with jax.named_scope('gain_wait'):
            gain_cp.wait_recv()
    gain = jnp.where(k == 0, gain_v[1, :feat], gain_v[1, feat:]).reshape(1, feat)
    acc[...] = jnp.zeros_like(acc)
    with jax.named_scope('stat_wait'):
        remote(stat_g.at[pl.ds(0, 7)], stat_g.at[pl.ds(0, 7)], stat_ssem, stat_rsem, y_next).wait_recv()

    def make_z(group):
        ref, sem = ((x_ga, za_rsem), (x_gb, zb_rsem))[group]

        @pl.when(home == 0)
        def _():
            with jax.named_scope('z_wait'):
                remote(ref, ref, z_ssem, sem, y_next).wait_recv()

        @pl.when(home == 1)
        def _():
            with jax.named_scope('z_wait'):
                remote(ref.at[pl.ds(0, 3)], ref.at[pl.ds(0, 3)], z_ssem, sem, y_next).wait_recv()

        t0, n, base = ((0, TA, 0), (TA, tb, rows_a))[group]
        for src in range(4):
            both = stat_g[src] + stat_g[4 + src]
            st = jnp.transpose(jnp.concatenate([both] * 4, axis=0))[t0:t0 + n] * (1.0 / (2 * half))
            mean = st[:, 0:1]
            var = st[:, 1:2] - mean * mean
            z = (ref[src].astype(F32) - mean) * lax.rsqrt(var + NORM_EPS) * gain
            z_v[pl.ds(base + n * src, n), :] = z.astype(BF16)

    row_group = (pl.ds(0, rows_a), pl.ds(rows_a, rows_b))

    def part_of(ref, j, part):
        if part == WHOLE:
            return ref.at[j]
        if part == FIRST:
            return ref.at[j, row_group[0]]
        return ref.at[pl.ds(j, part), row_group[1]]

    def rows_of(part):
        return pl.ds(0, rows_a + rows_b) if part == WHOLE else row_group[int(part > 0)]

    def d_copy(p, part, seq):
        return remote(part_of(d_send, p, part), part_of(d_recv, p, part), d_ssem, d_rsem.at[seq % RING], sibling)

    def b_index(j, part):
        return 9 + j // 2 if part == 2 else j + 5

    def x_group(j, part, first, sem):
        return remote(part_of(own, first + j, part), part_of(x_recv, j, part), x_ssem, x_rsem.at[sem], x_next)

    def x_copy_of(j, part, first):
        sem = x_rsem.at[b_index(j, part)] if part > 0 else x_rsem.at[j]
        return remote(part_of(own, first + j, part), part_of(x_recv, j, part), x_ssem, sem, x_next)

    def c_copy(j):
        return c_part(j, WHOLE)

    def c_part(j, part):
        return remote(part_of(own, c0 + j, part), part_of(c_recv.at[0], j, part), c_ssem, c_rsem.at[j], y_next)

    def c_relay(j, part):
        sem = c_rsem.at[2 * NC + j // 3] if part > 0 else c_rsem.at[NC + j]
        return remote(part_of(c_recv.at[0], j, part), part_of(c_recv.at[1], j, part), c_ssem, sem, x_next)

    def pass_c(j):
        with jax.named_scope('c_wait'):
            c_copy(j).wait_recv()
        c_relay(j, FIRST).start()

    def up(p, part, seq):
        rows = rows_of(part)
        sums = jnp.dot(z_v[rows, :], w_in_v[p], preferred_element_type=F32)
        d_send[p, rows, :] = sums[:, :C]
        own[chunk_of(p), rows, :] = sums[:, C:]
        d_copy(p, part, seq).start()

    def pair_add(p, part, seq):
        with jax.named_scope('pair_wait'):
            d_copy(p, part, seq).wait_recv()
        q, rows = chunk_of(p), rows_of(part)
        own[q, rows, :] = own[q, rows, :] + d_recv[p, rows, :]

    def wait_w_in(p):
        with jax.named_scope('w_in_wait'):
            group = w_in_v.at[pl.ds(p, GROUP)]
            pltpu.make_async_copy(group, group, w_in_sem.at[p // GROUP]).wait()

    def pair_group(p, part, seq):
        pair_add(p, part, seq)
        q = chunk_of(p)

        @pl.when((q >= c0) & (q < a0))
        def _():
            c_part(q - c0, part).start()

        @pl.when((home == 1) & (q < c0))
        def _():
            x_group(q, part, 0, 9 + q // 2 if part else q).start()

        @pl.when((home == 0) & (q >= a0))
        def _():
            x_group(q - a0, part, a0, q - a0).start()

    def pair_sum(p):
        pair_add(p, WHOLE, p + EARLY)
        q = chunk_of(p)

        @pl.when((q >= c0) & (q < a0))
        def _():
            c_copy(q - c0).start()

        @pl.when((home == 1) & (q < c0))
        def _():
            x_copy_of(q, FIRST, 0).start()

            x_group(q, 1, 0, 9 + q // 2).start()

        @pl.when((home == 0) & (q >= a0 + NF))
        def _():
            x_copy_of(q - a0, FIRST, a0).start()

        @pl.when((home == 0) & (q >= a0) & (q < a0 + NF))
        def _():
            x_copy_of(q - a0, WHOLE, a0).start()

    def up_loop(lo, hi, part, seq, then):
        def step(p, _):
            if part != FIRST:
                @pl.when(p % GROUP == 0)
                def _():
                    wait_w_in(p)
            up(p, part, p + seq)
            if part != 1:
                w_out_copy(p).start()
            then(p)
            return 0

        lax.fori_loop(lo, hi, step, 0)

    def late(p):
        pair_sum(p - LAG)

        @pl.when((p == 17) & (home == 1))
        def _():
            pass_c(0)

    def flush(p):
        for i in range(2):
            pair_group(2 * p + 2 + i, 1, 2 * p + 2 + i)

    make_z(1)
    up_loop(0, 4, 1, 0, lambda p: None)
    up_loop(4, EARLY, 1, 0, lambda p: pair_group(p - 4, 1, p - 4))
    make_z(0)
    up_loop(0, 2, FIRST, EARLY, flush)
    up_loop(2, LAG, FIRST, EARLY, lambda p: None)
    up_loop(LAG, EARLY, FIRST, EARLY, lambda p: pair_group(p - LAG, FIRST, p - LAG + EARLY))
    up_loop(EARLY, EARLY + LAG, WHOLE, EARLY, lambda p: pair_group(p - LAG, FIRST, p - LAG + EARLY))
    up_loop(EARLY + LAG, N, WHOLE, EARLY, late)
    for p in range(N - LAG, N):
        pair_sum(p)

    @pl.when(home == 0)
    def _():
        x_copy_of(NF, 2, a0).start()
        x_copy_of(NF + 2, 2, a0).start()
        for j in range(NF + 4, NA):
            x_copy_of(j, 1, a0).start()

    with jax.named_scope('w_out_wait'):
        pltpu.make_async_copy(w_out_v, w_out_v, w_out_sem).wait()

    def y_copy(j, part):
        sem = y_rsem.at[b_index(j, part)] if part > 0 else y_rsem.at[j]
        return remote(part_of(hall, j, part), part_of(hall, NA + j, part), y_ssem, sem, y_next)

    def b_sem(j, part):
        return b_rsem.at[NB + j // 2] if part > 0 else b_rsem.at[j]

    def relay_copy(j, part):
        return remote(part_of(hall, NA + j, part), part_of(hall, 2 * NA + j, part), b_ssem, b_sem(j, part), x_next)

    def back_copy(j, part):
        return remote(part_of(hall, 2 * NA + j, part), part_of(hall, 2 * NA + j, part), b_ssem, b_sem(j, part), y_next)

    def put_h(j, part, left, right):
        rows = rows_of(part)
        for c in range(max(part, 1)):
            total = left(c)[rows, :] + right(c)[rows, :]
            hall[j + c, rows, :] = jax.nn.gelu(total, approximate=True).astype(BF16)

    def make_h(j, part, first):
        with jax.named_scope('x_wait'):
            x_copy_of(j, part, 0).wait_recv()
        put_h(j, part, lambda c: own.at[first + j + c], lambda c: x_recv.at[j + c])
        y_copy(j, part).start()

    def make_h_c(j, part):
        with jax.named_scope('c_wait'):
            if part == FIRST:
                c_copy(j).wait_recv()
            c_relay(j, part).wait_recv()
        put_h(c0 + j, part, lambda c: c_recv.at[0, j + c], lambda c: c_recv.at[1, j + c])
        yc_copy(j, part).start()

    def yc_copy(j, part):
        sem = y_rsem.at[NA + j // 3] if part > 0 else y_rsem.at[c0 + j]
        return remote(part_of(hall, c0 + j, part), part_of(hall, NA + c0 + j, part), y_ssem, sem, y_next)

    def down(slot, i, part):
        rows = rows_of(part)
        parts = [jnp.dot(hall[slot + c, rows, :], w_out_v[i + c], preferred_element_type=F32)
                 for c in range(max(part, 1))]
        acc[rows, :] += sum(parts[1:], parts[0])

    e_recv, f_send, f_recv = (ea_recv, eb_recv), (fa_send, fb_send), (fa_recv, fb_recv)

    def token_rows(group, r):
        n, base = ((TA, 0), (tb, rows_a))[group]
        return pl.ds(pl.multiple_of(base + n * r, 8), n)

    def e_copy(group, s):
        r = 2 * (s * x + (1 - s) * (1 - x)) + 1 - k
        return remote(acc.at[token_rows(group, r)], e_recv[group].at[s], e_ssem, e_rsem.at[2 * group + s], sibling)

    def f_copy(group):
        return remote(f_send[group], f_recv[group], f_ssem, f_rsem.at[group], x_next)

    def end_start(group):
        e_copy(group, 0).start()
        e_copy(group, 1).start()

    def end_send(group):
        with jax.named_scope('e0_wait'):
            e_copy(group, 0).wait_recv()
        f_send[group][...] = acc[token_rows(group, 2 * (1 - x) + k), :] + e_recv[group][0]
        f_copy(group).start()

    def end_send_from(core):
        @pl.when(k == core)
        def _():
            end_send(0)

    def end_sum(group):
        with jax.named_scope('e1_wait'):
            e_copy(group, 1).wait_recv()
        with jax.named_scope('f_wait'):
            f_copy(group).wait_recv()
        total = acc[token_rows(group, row), :] + e_recv[group][1] + f_recv[group][...]
        t0, n = ((0, TA), (TA, tb))[group]
        out_v[t0:t0 + n, :] = ((xa_v, xb_v)[group][...].astype(F32) + total).astype(BF16)

    def loop(lo, hi, step):
        def body(i, _):
            step(i)
            return 0
        lax.fori_loop(lo, hi, body, 0)

    @pl.when(home == 1)
    def _():
        def relay(i, part):
            with jax.named_scope('relay_wait'):
                y_copy(i, part).wait_recv()
            relay_copy(i, part).start()

        def b_step(i, part):
            with jax.named_scope('b_wait'):
                back_copy(i, part).wait_recv()
            down(2 * NA + i, i, part)

        def c_step(i, part):
            with jax.named_scope('ch_wait'):
                yc_copy(i, part).wait_recv()
            down(NA + c0 + i, c0 + i, part)

        def a_step(j, part):
            make_h(j, part, a0)
            down(j, a0 + j, part)

        pass_c(1)

        def step(j):
            @pl.when(j == 2)
            def _():
                pass_c(2)
            a_step(j, WHOLE)

        loop(0, NF, step)

        def step(j):
            for t, i in ((4, 3), (6, 4)):
                @pl.when(j == t)
                def _():
                    pass_c(i)

            @pl.when(j == 7)
            def _():
                relay(0, FIRST)
                relay(1, FIRST)
            a_step(j, FIRST)

        loop(NF, 8, step)
        relay(2, FIRST)
        relay(3, FIRST)
        c_relay(0, 3).start()
        c_relay(3, 2).start()

        def step(t):
            a_step(8 + t, FIRST)

            @pl.when(t == 0)
            def _():
                relay(0, 2)
                relay(2, 2)

            @pl.when(t == 1)
            def _():
                c_step(1, FIRST)
            c_step(2 * t, FIRST)

        loop(0, 2, step)
        a_step(10, FIRST)
        loop(3, 5, lambda i: c_step(i, FIRST))
        a_step(NF, 2)
        loop(0, 2, lambda i: b_step(i, FIRST))
        a_step(NF + 2, 2)
        b_step(2, FIRST)
        make_h(NF + 4, 1, a0)
        b_step(NB - 1, FIRST)
        end_start(0)
        make_h(NF + 5, 1, a0)
        down(NF + 4, a0 + NF + 4, 1)
        make_h(NF + 6, 1, a0)
        end_send_from(0)
        loop(NF + 5, NA, lambda j: down(j, a0 + j, 1))
        end_send_from(1)
        c_step(0, 3)
        c_step(3, 2)
        loop(0, 2, lambda m: b_step(2 * m, 2))

    @pl.when(home == 0)
    def _():
        def a_step(j, part):
            with jax.named_scope('a_wait'):
                y_copy(j, part).wait_recv()
            down(NA + j, a0 + j, part)

        def b_pass(i, part):
            with jax.named_scope('b_wait'):
                relay_copy(i, part).wait_recv()
            back_copy(i, part).start()

        def b_step(i, part):
            b_pass(i, part)
            down(2 * NA + i, i, part)

        def c_step(i, part):
            make_h_c(i, part)
            down(c0 + i, c0 + i, part)

        loop(0, NB, lambda j: make_h(j, FIRST, 0))
        loop(0, NB // 2, lambda m: make_h(2 * m, 2, 0))
        c_step(0, FIRST)

        def step(t):
            c_step(1 + t, FIRST)
            a_step(t, WHOLE)

        loop(0, NF, step)

        def step(t):
            b_step(t, FIRST)
            a_step(NF + t, FIRST)

        loop(0, 4, step)
        loop(8, 10, lambda j: a_step(j, FIRST))
        c_step(0, 3)
        a_step(10, FIRST)
        end_start(0)
        end_send_from(0)
        c_step(3, 2)
        b_pass(0, 2)
        b_pass(2, 2)
        down(2 * NA, 0, 4)
        a_step(NF, 2)
        end_send_from(1)
        a_step(NF + 2, 2)
        loop(NF + 4, NA, lambda j: a_step(j, 1))

    end_start(1)
    end_send(1)

    def sent(ref, sem):
        remote(ref, ref, sem, sem, y_next).wait_send()

    with jax.named_scope('drain'):
        sent(stat_g.at[pl.ds(0, 7)], stat_ssem)
        sent(d_send, d_ssem)
        sent(hall.at[pl.ds(0, NB)], b_ssem)
        sent(c_recv.at[0], c_ssem)
        sent(ea_recv, e_ssem)
        sent(eb_recv, e_ssem)

        @pl.when(home == 0)
        def _():
            sent(x_ga, z_ssem)
            sent(x_gb, z_ssem)
            sent(own.at[pl.ds(0, NA)], x_ssem)
            sent(hall.at[pl.ds(0, NB + NC)], y_ssem)

        @pl.when(home == 1)
        def _():
            gain_cp.wait_send()
            sent(x_ga, z_ssem)
            sent(x_gb.at[pl.ds(0, 3)], z_ssem)
            sent(own.at[pl.ds(0, NB)], x_ssem)
            sent(c_recv.at[1], c_ssem)
            sent(hall.at[pl.ds(0, NA)], y_ssem)

    end_sum(0)
    end_sum(1)
    sent(fa_send, f_ssem)
    sent(fb_send, f_ssem)


def solution(mesh):
    def body(x_blk, gain_blk, w_in_blk, w_out_blk):
        tok, half = x_blk.shape
        feat = w_in_blk.shape[0]
        tokens = 4 * tok
        dma = pltpu.SemaphoreType.DMA
        return pl.pallas_call(
            kernel,
            out_shape=pltpu.VMEM((tok, half), BF16),
            in_specs=[pl.BlockSpec(memory_space=pl.ANY)] * 4,
            out_specs=pl.BlockSpec(memory_space=pltpu.VMEM),
            scratch_shapes=[
                pltpu.VMEM((TA, half), BF16),
                pltpu.VMEM((tok - TA, half), BF16),
                pltpu.VMEM((2, half), F32),
                pltpu.VMEM((8, 2, 128), F32),
                pltpu.VMEM((4, TA, feat), BF16),
                pltpu.VMEM((4, tok - TA, feat), BF16),
                pltpu.VMEM((TA, feat), BF16),
                pltpu.VMEM((tokens, feat), BF16),
                pltpu.VMEM((N, feat, 2 * C), BF16),
                pltpu.VMEM((N, C, half), BF16),
                pltpu.VMEM((N, tokens, C), F32),
                pltpu.VMEM((N, tokens, C), F32),
                pltpu.VMEM((N, tokens, C), F32),
                pltpu.VMEM((NA, tokens, C), F32),
                pltpu.VMEM((2, NC, tokens, C), F32),
                pltpu.VMEM((2 * NA + NB, tokens, C), BF16),
                pltpu.VMEM((tokens, half), F32),
                pltpu.VMEM((2, TA, half), F32),
                pltpu.VMEM((2, tok - TA, half), F32),
                pltpu.VMEM((TA, half), F32),
                pltpu.VMEM((TA, half), F32),
                pltpu.VMEM((tok - TA, half), F32),
                pltpu.VMEM((tok - TA, half), F32),
                dma((9,)),
                dma((N // GROUP,)),
                dma((2,)),
                dma((RING,)),
                dma((NA + 5,)),
                dma((NA + 5,)),
                dma((NB + NB // 2,)),
                dma((2 * NC + 2,)),
                dma((4,)),
                dma((2,)),
            ],
            compiler_params=pltpu.CompilerParams(
                collective_id=0, has_side_effects=True, vmem_limit_bytes=66_500_000
            ),
        )(x_blk, gain_blk, w_in_blk, w_out_blk)

    return jax.shard_map(
        body,
        mesh=mesh,
        in_specs=(P(("dp", "row"), "col"), P("col"), P("row", "col"), P("row", "col")),
        out_specs=P(("dp", "row"), "col"),
        check_vma=False,
    )
```

```python
import jax
import jax.numpy as jnp
from jax import lax
from jax.experimental import pallas as pl
from jax.experimental.pallas import tpu as pltpu
from jax.sharding import PartitionSpec as P

NORM_EPS = 1e-5
MESH = pl.DeviceIdType.MESH
WHOLE, FIRST = -1, 0
F32 = jnp.float32
BF16 = jnp.bfloat16

C = 256
NB = 4
NC = 5
NA = 11
N = NA + NB + NC
NF = 4
EARLY = 6
GROUP = 10
LAG = 3
RING = 10
TA = 16


def kernel(x_hbm, gain_hbm, w_in_hbm, w_out_hbm, out_v,
           xa_v, xb_v, gain_v, stat_g, x_ga, x_gb, x_relay, z_v, w_in_v, w_out_v, d_send, d_recv, own, x_recv, c_recv, hall,
           acc, ea_recv, eb_recv, fa_send, fa_recv, fb_send, fb_recv,
           misc_sem, w_in_sem, send_sem, d_rsem, x_rsem, y_rsem, b_rsem, c_rsem, e_rsem, f_rsem):
    w_out_sem, stat_rsem, za_rsem, zb_rsem = [misc_sem.at[i] for i in range(4, 8)]
    stat_ssem = z_ssem = d_ssem = x_ssem = y_ssem = b_ssem = c_ssem = e_ssem = send_sem.at[0]
    f_ssem = send_sem.at[1]
    y = lax.axis_index("col")
    row = lax.axis_index("row")
    x = row // 2
    k = row % 2
    dp = lax.axis_index("dp")
    home = 1 - (x + y) % 2
    tok, half = out_v.shape
    feat = half // 2
    block = N * C
    rows_a = 4 * TA
    tb = tok - TA
    rows_b = 4 * tb
    sibling = (dp, y, 2 * x + 1 - k)
    x_next = (dp, y, 2 * (1 - x) + k)
    y_next = (dp, 1 - y, row)

    def remote(src, dst, ssem, rsem, dev):
        return pltpu.make_async_remote_copy(src_ref=src, dst_ref=dst, send_sem=ssem, recv_sem=rsem,
                                            device_id=dev, device_id_type=MESH)

    c0, a0 = NB, NB + NC

    def chunk_of(p):
        u = p - 2 * NB - 1
        pair = jnp.where(p % 2 == 1, c0 + p // 2, p // 2 + (1 - home) * a0)
        mixed = jnp.where(u % 2 == 1, u // 2, a0 + NB + u // 2)
        late = jnp.where((home == 1) | (u >= 2 * NB), a0 + u, mixed)
        return jnp.where(p < 2 * NB, pair, jnp.where(u < 0, a0 - 1, late))

    def w_in_copies(p):
        c = C * chunk_of(p)
        cs = pl.multiple_of((1 - k) * block + c, C)
        co = pl.multiple_of(k * block + c, C)
        return (pltpu.make_async_copy(w_in_hbm.at[:, pl.ds(cs, C)], w_in_v.at[p, :, pl.ds(0, C)], w_in_sem.at[p // GROUP]),
                pltpu.make_async_copy(w_in_hbm.at[:, pl.ds(co, C)], w_in_v.at[p, :, pl.ds(C, C)], w_in_sem.at[p // GROUP]))

    def w_out_copy(i):
        r = pl.multiple_of(i * C, C)
        return pltpu.make_async_copy(w_out_hbm.at[pl.ds(r, C), :], w_out_v.at[i], w_out_sem)

    xa_copy = pltpu.make_async_copy(x_hbm.at[pl.ds(0, TA)], xa_v, misc_sem.at[0])
    xb_copy = pltpu.make_async_copy(x_hbm.at[pl.ds(TA, tb)], xb_v, misc_sem.at[8])
    g_copy = pltpu.make_async_copy(gain_hbm, gain_v.at[0], misc_sem.at[1])
    xa_copy.start()
    xb_copy.start()
    g_copy.start()

    barrier = pltpu.get_barrier_semaphore()
    for dy in range(2):
        for dr in range(4):
            if dy or dr:
                pl.semaphore_signal(barrier, inc=1, device_id=(dp, (y + dy) % 2, (row + dr) % 4), device_id_type=MESH)

    def start_w_in(p, _):
        for cp in w_in_copies(p):
            cp.start()
        return 0

    lax.fori_loop(0, N, start_w_in, 0)

    xa_copy.wait()
    xb_copy.wait()
    g_copy.wait()

    def row_sums(ref):
        v = ref[...].astype(F32)
        lane = lax.broadcasted_iota(jnp.int32, (v.shape[0], 128), 1)
        return jnp.where(lane == 0, jnp.sum(v, axis=1, keepdims=True), jnp.sum(v * v, axis=1, keepdims=True))

    me = 4 * y + row
    stat_g[me, :, :tok] = jnp.transpose(jnp.concatenate([row_sums(xa_v), row_sums(xb_v)], axis=0))[:2]
    with jax.named_scope('barrier'):
        pl.semaphore_wait(barrier, 7)

    def tok_copy(group, dy, dk):
        tk = (k + dk) % 2
        cols = pl.ds(pl.multiple_of(feat * tk, 128), feat)
        src, dst, sem = ((xa_v, x_ga, za_rsem), (xb_v, x_gb, zb_rsem))[group]
        return remote(src.at[:, cols], dst.at[row], z_ssem, sem, (dp, (y + dy) % 2, 2 * y + tk))

    def stat_copy(d):
        ty = (y + d // 4) % 2
        tr = (row + d % 4) % 4
        return remote(stat_g.at[me], stat_g.at[me], stat_ssem, stat_rsem, (dp, ty, tr))

    gain_cp = remote(gain_v.at[0], gain_v.at[1], z_ssem, misc_sem.at[3], y_next)
    half_cols = pl.ds(pl.multiple_of(feat * (1 - k), 128), feat)
    to_relay = remote(xa_v.at[:, half_cols], x_relay, z_ssem, misc_sem.at[2], y_next)
    from_relay = remote(x_relay, x_ga.at[row], z_ssem, za_rsem, (dp, y, 2 * (1 - x) + 1 - k))

    for d in range(1, 8):
        stat_copy(d).start()

    @pl.when(home == 0)
    def _():
        to_relay.start()
        tok_copy(1, 1, 0).start()
        tok_copy(1, 1, 1).start()
        tok_copy(1, 0, 0).start()
        tok_copy(1, 0, 1).start()
        tok_copy(0, 1, 0).start()
        tok_copy(0, 0, 0).start()
        tok_copy(0, 0, 1).start()

    @pl.when(home == 1)
    def _():
        gain_cp.start()
        for group in (1, 0):
            tok_copy(group, 0, 1).start()
            tok_copy(group, 1, 0).start()
            tok_copy(group, 1, 1).start()
        x_ga[row] = jnp.where(k == 0, xa_v[:, :feat], xa_v[:, feat:])
        x_gb[row] = jnp.where(k == 0, xb_v[:, :feat], xb_v[:, feat:])
        gain_v[1] = gain_v[0]
        with jax.named_scope('x_relay_wait'):
            to_relay.wait_recv()
        from_relay.start()

    @pl.when(home == 0)
    def _():
        with jax.named_scope('gain_wait'):
            gain_cp.wait_recv()
    gain = jnp.where(k == 0, gain_v[1, :feat], gain_v[1, feat:]).reshape(1, feat)
    acc[...] = jnp.zeros_like(acc)
    with jax.named_scope('stat_wait'):
        remote(stat_g.at[pl.ds(0, 7)], stat_g.at[pl.ds(0, 7)], stat_ssem, stat_rsem, y_next).wait_recv()

    def make_z(group):
        ref, sem = ((x_ga, za_rsem), (x_gb, zb_rsem))[group]

        @pl.when(home == 0)
        def _():
            with jax.named_scope('z_wait'):
                remote(ref, ref, z_ssem, sem, y_next).wait_recv()

        @pl.when(home == 1)
        def _():
            with jax.named_scope('z_wait'):
                remote(ref.at[pl.ds(0, 3)], ref.at[pl.ds(0, 3)], z_ssem, sem, y_next).wait_recv()

        t0, n, base = ((0, TA, 0), (TA, tb, rows_a))[group]
        for src in range(4):
            both = stat_g[src] + stat_g[4 + src]
            st = jnp.transpose(jnp.concatenate([both] * 4, axis=0))[t0:t0 + n] * (1.0 / (2 * half))
            mean = st[:, 0:1]
            var = st[:, 1:2] - mean * mean
            z = (ref[src].astype(F32) - mean) * lax.rsqrt(var + NORM_EPS) * gain
            z_v[pl.ds(base + n * src, n), :] = z.astype(BF16)

    row_group = (pl.ds(0, rows_a), pl.ds(rows_a, rows_b))

    def part_of(ref, j, part):
        if part == WHOLE:
            return ref.at[j]
        if part == FIRST:
            return ref.at[j, row_group[0]]
        return ref.at[pl.ds(j, part), row_group[1]]

    def rows_of(part):
        return pl.ds(0, rows_a + rows_b) if part == WHOLE else row_group[int(part > 0)]

    def d_copy(p, part, seq):
        return remote(part_of(d_send, p, part), part_of(d_recv, p, part), d_ssem, d_rsem.at[seq % RING], sibling)

    def b_index(j, part):
        return 9 + j // 2 if part == 2 else j + 5

    def x_group(j, part, first, sem):
        return remote(part_of(own, first + j, part), part_of(x_recv, j, part), x_ssem, x_rsem.at[sem], x_next)

    def x_copy_of(j, part, first):
        sem = x_rsem.at[b_index(j, part)] if part > 0 else x_rsem.at[j]
        return remote(part_of(own, first + j, part), part_of(x_recv, j, part), x_ssem, sem, x_next)

    def c_copy(j):
        return c_part(j, WHOLE)

    def c_part(j, part):
        return remote(part_of(own, c0 + j, part), part_of(c_recv.at[0], j, part), c_ssem, c_rsem.at[j], y_next)

    def c_relay(j, part):
        sem = c_rsem.at[2 * NC + j // 3] if part > 0 else c_rsem.at[NC + j]
        return remote(part_of(c_recv.at[0], j, part), part_of(c_recv.at[1], j, part), c_ssem, sem, x_next)

    last = NA - 1

    def both_home():
        return remote(part_of(own, a0 + last, 1), part_of(c_recv.at[0], NC, 1), c_ssem, c_rsem.at[2 * NC + 2], y_next)

    def both_far():
        return remote(part_of(own, a0 + last, 1), part_of(c_recv.at[1], NC, 1), c_ssem, c_rsem.at[2 * NC + 3],
                      (dp, 1 - y, 2 * (1 - x) + k))

    def pass_c(j):
        with jax.named_scope('c_wait'):
            c_copy(j).wait_recv()
        c_relay(j, FIRST).start()

    def up(p, part, seq):
        rows = rows_of(part)
        sums = jnp.dot(z_v[rows, :], w_in_v[p], preferred_element_type=F32)
        d_send[p, rows, :] = sums[:, :C]
        own[chunk_of(p), rows, :] = sums[:, C:]
        d_copy(p, part, seq).start()

    def pair_add(p, part, seq):
        with jax.named_scope('pair_wait'):
            d_copy(p, part, seq).wait_recv()
        q, rows = chunk_of(p), rows_of(part)
        own[q, rows, :] = own[q, rows, :] + d_recv[p, rows, :]

    def wait_w_in(p):
        with jax.named_scope('w_in_wait'):
            group = w_in_v.at[pl.ds(p, GROUP)]
            pltpu.make_async_copy(group, group, w_in_sem.at[p // GROUP]).wait()

    def pair_group(p, part, seq):
        pair_add(p, part, seq)
        q = chunk_of(p)

        @pl.when((q >= c0) & (q < a0))
        def _():
            c_part(q - c0, part).start()

        @pl.when((home == 1) & (q < c0))
        def _():
            x_group(q, part, 0, 9 + q // 2 if part else q).start()

        @pl.when((home == 0) & (q >= a0))
        def _():
            x_group(q - a0, part, a0, q - a0).start()

    def pair_sum(p):
        pair_add(p, WHOLE, p + EARLY)
        q = chunk_of(p)

        @pl.when((q >= c0) & (q < a0))
        def _():
            c_copy(q - c0).start()

        @pl.when((home == 1) & (q < c0))
        def _():
            x_copy_of(q, FIRST, 0).start()

            x_group(q, 1, 0, 9 + q // 2).start()

        @pl.when((home == 0) & (q >= a0 + NF))
        def _():
            x_copy_of(q - a0, FIRST, a0).start()

        @pl.when((home == 0) & (q >= a0) & (q < a0 + NF))
        def _():
            x_copy_of(q - a0, WHOLE, a0).start()

    def up_loop(lo, hi, part, seq, then):
        def step(p, _):
            if part != FIRST:
                @pl.when(p % GROUP == 0)
                def _():
                    wait_w_in(p)
            up(p, part, p + seq)
            if part != 1:
                w_out_copy(p).start()
            then(p)
            return 0

        lax.fori_loop(lo, hi, step, 0)

    def late(p):
        pair_sum(p - LAG)

        @pl.when((p == 17) & (home == 1))
        def _():
            pass_c(0)

    def flush(p):
        for i in range(2):
            pair_group(2 * p + 2 + i, 1, 2 * p + 2 + i)

    make_z(1)
    up_loop(0, 4, 1, 0, lambda p: None)
    up_loop(4, EARLY, 1, 0, lambda p: pair_group(p - 4, 1, p - 4))
    make_z(0)
    up_loop(0, 2, FIRST, EARLY, flush)
    up_loop(2, LAG, FIRST, EARLY, lambda p: None)
    up_loop(LAG, EARLY, FIRST, EARLY, lambda p: pair_group(p - LAG, FIRST, p - LAG + EARLY))
    up_loop(EARLY, EARLY + LAG, WHOLE, EARLY, lambda p: pair_group(p - LAG, FIRST, p - LAG + EARLY))
    up_loop(EARLY + LAG, N, WHOLE, EARLY, late)
    for p in range(N - LAG, N):
        pair_sum(p)

    @pl.when(home == 0)
    def _():
        x_copy_of(NF, 2, a0).start()
        x_copy_of(NF + 2, 2, a0).start()
        x_copy_of(NF + 4, 2, a0).start()
        both_far().start()
        x_copy_of(last, 1, a0).start()

    with jax.named_scope('w_out_wait'):
        pltpu.make_async_copy(w_out_v, w_out_v, w_out_sem).wait()

    def y_copy(j, part):
        sem = y_rsem.at[b_index(j, part)] if part > 0 else y_rsem.at[j]
        return remote(part_of(hall, j, part), part_of(hall, NA + j, part), y_ssem, sem, y_next)

    def b_sem(j, part):
        return b_rsem.at[NB + j // 2] if part > 0 else b_rsem.at[j]

    def relay_copy(j, part):
        return remote(part_of(hall, NA + j, part), part_of(hall, 2 * NA + j, part), b_ssem, b_sem(j, part), x_next)

    def back_copy(j, part):
        return remote(part_of(hall, 2 * NA + j, part), part_of(hall, 2 * NA + j, part), b_ssem, b_sem(j, part), y_next)

    def put_h(j, part, left, right):
        rows = rows_of(part)
        for c in range(max(part, 1)):
            total = left(c)[rows, :] + right(c)[rows, :]
            hall[j + c, rows, :] = jax.nn.gelu(total, approximate=True).astype(BF16)

    def make_h(j, part, first, send=True):
        with jax.named_scope('x_wait'):
            x_copy_of(j, part, 0).wait_recv()
        put_h(j, part, lambda c: own.at[first + j + c], lambda c: x_recv.at[j + c])
        if send:
            y_copy(j, part).start()

    def make_h_c(j, part):
        with jax.named_scope('c_wait'):
            if part == FIRST:
                c_copy(j).wait_recv()
            c_relay(j, part).wait_recv()
        put_h(c0 + j, part, lambda c: c_recv.at[0, j + c], lambda c: c_recv.at[1, j + c])
        yc_copy(j, part).start()

    def yc_copy(j, part):
        sem = y_rsem.at[NA + j // 3] if part > 0 else y_rsem.at[c0 + j]
        return remote(part_of(hall, c0 + j, part), part_of(hall, NA + c0 + j, part), y_ssem, sem, y_next)

    def down(slot, i, part):
        rows = rows_of(part)
        parts = [jnp.dot(hall[slot + c, rows, :], w_out_v[i + c], preferred_element_type=F32)
                 for c in range(max(part, 1))]
        acc[rows, :] += sum(parts[1:], parts[0])

    e_recv, f_send, f_recv = (ea_recv, eb_recv), (fa_send, fb_send), (fa_recv, fb_recv)

    def token_rows(group, r):
        n, base = ((TA, 0), (tb, rows_a))[group]
        return pl.ds(pl.multiple_of(base + n * r, 8), n)

    def e_copy(group, s):
        r = 2 * (s * x + (1 - s) * (1 - x)) + 1 - k
        return remote(acc.at[token_rows(group, r)], e_recv[group].at[s], e_ssem, e_rsem.at[2 * group + s], sibling)

    def f_copy(group):
        return remote(f_send[group], f_recv[group], f_ssem, f_rsem.at[group], x_next)

    def end_start(group):
        e_copy(group, 0).start()
        e_copy(group, 1).start()

    def end_send(group):
        with jax.named_scope('e0_wait'):
            e_copy(group, 0).wait_recv()
        f_send[group][...] = acc[token_rows(group, 2 * (1 - x) + k), :] + e_recv[group][0]
        f_copy(group).start()

    def end_send_from(core):
        @pl.when(k == core)
        def _():
            end_send(0)

    def end_sum(group):
        with jax.named_scope('e1_wait'):
            e_copy(group, 1).wait_recv()
        with jax.named_scope('f_wait'):
            f_copy(group).wait_recv()
        total = acc[token_rows(group, row), :] + e_recv[group][1] + f_recv[group][...]
        t0, n = ((0, TA), (TA, tb))[group]
        out_v[t0:t0 + n, :] = ((xa_v, xb_v)[group][...].astype(F32) + total).astype(BF16)

    def loop(lo, hi, step):
        def body(i, _):
            step(i)
            return 0
        lax.fori_loop(lo, hi, body, 0)

    @pl.when(home == 1)
    def _():
        def relay(i, part):
            with jax.named_scope('relay_wait'):
                y_copy(i, part).wait_recv()
            relay_copy(i, part).start()

        def b_step(i, part):
            with jax.named_scope('b_wait'):
                back_copy(i, part).wait_recv()
            down(2 * NA + i, i, part)

        def c_step(i, part):
            with jax.named_scope('ch_wait'):
                yc_copy(i, part).wait_recv()
            down(NA + c0 + i, c0 + i, part)

        def a_step(j, part):
            make_h(j, part, a0)
            down(j, a0 + j, part)

        pass_c(1)
        both_home().start()

        def step(j):
            @pl.when(j == 2)
            def _():
                pass_c(2)
            a_step(j, WHOLE)

        loop(0, NF, step)

        def step(j):
            for t, i in ((4, 3), (6, 4)):
                @pl.when(j == t)
                def _():
                    pass_c(i)

            @pl.when(j == 7)
            def _():
                relay(0, FIRST)
                relay(1, FIRST)
            a_step(j, FIRST)

        loop(NF, 8, step)
        relay(2, FIRST)
        relay(3, FIRST)
        c_relay(0, 3).start()
        c_relay(3, 2).start()

        def step(t):
            a_step(8 + t, FIRST)

            @pl.when(t == 0)
            def _():
                relay(0, 2)
                relay(2, 2)

            @pl.when(t == 1)
            def _():
                c_step(1, FIRST)
            c_step(2 * t, FIRST)

        loop(0, 2, step)
        a_step(10, FIRST)
        loop(3, 5, lambda i: c_step(i, FIRST))
        a_step(NF, 2)
        loop(0, 2, lambda i: b_step(i, FIRST))
        a_step(NF + 2, 2)
        b_step(2, FIRST)
        b_step(NB - 1, FIRST)
        end_start(0)
        make_h(NF + 4, 2, a0)
        end_send_from(0)
        down(NF + 4, a0 + NF + 4, 2)
        c_step(0, 3)
        end_send_from(1)
        make_h(last, 1, a0, send=False)
        down(last, a0 + last, 1)
        c_step(3, 2)
        loop(0, 2, lambda m: b_step(2 * m, 2))

    @pl.when(home == 0)
    def _():
        def a_step(j, part):
            with jax.named_scope('a_wait'):
                y_copy(j, part).wait_recv()
            down(NA + j, a0 + j, part)

        def b_pass(i, part):
            with jax.named_scope('b_wait'):
                relay_copy(i, part).wait_recv()
            back_copy(i, part).start()

        def b_step(i, part):
            b_pass(i, part)
            down(2 * NA + i, i, part)

        def c_step(i, part):
            make_h_c(i, part)
            down(c0 + i, c0 + i, part)

        loop(0, NB, lambda j: make_h(j, FIRST, 0))
        loop(0, NB // 2, lambda m: make_h(2 * m, 2, 0))
        c_step(0, FIRST)

        def step(t):
            c_step(1 + t, FIRST)
            a_step(t, WHOLE)

        loop(0, NF, step)

        def step(t):
            b_step(t, FIRST)
            a_step(NF + t, FIRST)

        loop(0, 4, step)
        loop(8, 10, lambda j: a_step(j, FIRST))
        c_step(0, 3)
        a_step(10, FIRST)
        end_start(0)
        end_send_from(0)
        c_step(3, 2)
        b_pass(0, 2)
        b_pass(2, 2)
        down(2 * NA, 0, 4)
        a_step(NF, 2)
        end_send_from(1)
        with jax.named_scope('both_wait'):
            both_home().wait_recv()
            both_far().wait_recv()
        put_h(c0 + NC, 1, lambda c: c_recv.at[0, NC + c], lambda c: c_recv.at[1, NC + c])
        down(c0 + NC, a0 + last, 1)
        a_step(NF + 2, 2)
        a_step(NF + 4, 2)

    end_start(1)
    end_send(1)

    def sent(ref, sem):
        remote(ref, ref, sem, sem, y_next).wait_send()

    with jax.named_scope('drain'):
        sent(stat_g.at[pl.ds(0, 7)], stat_ssem)
        sent(d_send, d_ssem)
        sent(hall.at[pl.ds(0, NB)], b_ssem)
        sent(c_recv.at[0, pl.ds(0, NC)], c_ssem)
        sent(part_of(own, 0, 1), c_ssem)
        sent(ea_recv, e_ssem)
        sent(eb_recv, e_ssem)

        @pl.when(home == 0)
        def _():
            sent(x_ga, z_ssem)
            sent(x_gb, z_ssem)
            sent(own.at[pl.ds(0, NA)], x_ssem)
            sent(hall.at[pl.ds(0, NB + NC)], y_ssem)

        @pl.when(home == 1)
        def _():
            gain_cp.wait_send()
            sent(x_ga, z_ssem)
            sent(x_gb.at[pl.ds(0, 3)], z_ssem)
            sent(own.at[pl.ds(0, NB)], x_ssem)
            sent(c_recv.at[1, pl.ds(0, NC)], c_ssem)
            sent(hall.at[pl.ds(0, last)], y_ssem)
            sent(part_of(hall, 0, FIRST), y_ssem)

    end_sum(0)
    end_sum(1)
    sent(fa_send, f_ssem)
    sent(fb_send, f_ssem)


def solution(mesh):
    def body(x_blk, gain_blk, w_in_blk, w_out_blk):
        tok, half = x_blk.shape
        feat = w_in_blk.shape[0]
        tokens = 4 * tok
        dma = pltpu.SemaphoreType.DMA
        return pl.pallas_call(
            kernel,
            out_shape=pltpu.VMEM((tok, half), BF16),
            in_specs=[pl.BlockSpec(memory_space=pl.ANY)] * 4,
            out_specs=pl.BlockSpec(memory_space=pltpu.VMEM),
            scratch_shapes=[
                pltpu.VMEM((TA, half), BF16),
                pltpu.VMEM((tok - TA, half), BF16),
                pltpu.VMEM((2, half), F32),
                pltpu.VMEM((8, 2, 128), F32),
                pltpu.VMEM((4, TA, feat), BF16),
                pltpu.VMEM((4, tok - TA, feat), BF16),
                pltpu.VMEM((TA, feat), BF16),
                pltpu.VMEM((tokens, feat), BF16),
                pltpu.VMEM((N, feat, 2 * C), BF16),
                pltpu.VMEM((N, C, half), BF16),
                pltpu.VMEM((N, tokens, C), F32),
                pltpu.VMEM((N, tokens, C), F32),
                pltpu.VMEM((N, tokens, C), F32),
                pltpu.VMEM((NA, tokens, C), F32),
                pltpu.VMEM((2, NC + 1, tokens, C), F32),
                pltpu.VMEM((2 * NA + NB, tokens, C), BF16),
                pltpu.VMEM((tokens, half), F32),
                pltpu.VMEM((2, TA, half), F32),
                pltpu.VMEM((2, tok - TA, half), F32),
                pltpu.VMEM((TA, half), F32),
                pltpu.VMEM((TA, half), F32),
                pltpu.VMEM((tok - TA, half), F32),
                pltpu.VMEM((tok - TA, half), F32),
                dma((9,)),
                dma((N // GROUP,)),
                dma((2,)),
                dma((RING,)),
                dma((NA + 5,)),
                dma((NA + 5,)),
                dma((NB + NB // 2,)),
                dma((2 * NC + 4,)),
                dma((4,)),
                dma((2,)),
            ],
            compiler_params=pltpu.CompilerParams(
                collective_id=0, has_side_effects=True, vmem_limit_bytes=66_500_000
            ),
        )(x_blk, gain_blk, w_in_blk, w_out_blk)

    return jax.shard_map(
        body,
        mesh=mesh,
        in_specs=(P(("dp", "row"), "col"), P("col"), P("row", "col"), P("row", "col")),
        out_specs=P(("dp", "row"), "col"),
        check_vma=False,
    )
```

```python
import jax
import jax.numpy as jnp
from jax import lax
from jax.experimental import pallas as pl
from jax.experimental.pallas import tpu as pltpu
from jax.sharding import PartitionSpec as P

NORM_EPS = 1e-5
MESH = pl.DeviceIdType.MESH
WHOLE, FIRST = -1, 0
F32 = jnp.float32
BF16 = jnp.bfloat16

C = 256
NB = 4
NC = 5
NA = 11
N = NA + NB + NC
NF = 4
EARLY = 6
GROUP = 10
LAG = 3
RING = 10
TA = 16


def kernel(x_hbm, gain_hbm, w_in_hbm, w_out_hbm, out_v,
           xa_v, xb_v, gain_v, stat_g, x_ga, x_gb, x_relay, z_v, w_in_v, w_out_v, d_send, d_recv, own, x_recv, c_recv, hall,
           acc, ea_recv, eb_recv, fa_send, fa_recv, fb_send, fb_recv,
           misc_sem, w_in_sem, send_sem, d_rsem, x_rsem, y_rsem, b_rsem, c_rsem, e_rsem, f_rsem):
    w_out_sem, stat_rsem, za_rsem, zb_rsem = [misc_sem.at[i] for i in range(4, 8)]
    stat_ssem = z_ssem = d_ssem = x_ssem = y_ssem = b_ssem = c_ssem = e_ssem = send_sem.at[0]
    f_ssem = send_sem.at[1]
    y = lax.axis_index("col")
    row = lax.axis_index("row")
    x = row // 2
    k = row % 2
    dp = lax.axis_index("dp")
    home = 1 - (x + y) % 2
    tok, half = out_v.shape
    feat = half // 2
    block = N * C
    rows_a = 4 * TA
    tb = tok - TA
    rows_b = 4 * tb
    sibling = (dp, y, 2 * x + 1 - k)
    x_next = (dp, y, 2 * (1 - x) + k)
    y_next = (dp, 1 - y, row)

    def remote(src, dst, ssem, rsem, dev):
        return pltpu.make_async_remote_copy(src_ref=src, dst_ref=dst, send_sem=ssem, recv_sem=rsem,
                                            device_id=dev, device_id_type=MESH)

    c0, a0 = NB, NB + NC

    def chunk_of(p):
        u = p - 2 * NB - 1
        pair = jnp.where(p % 2 == 1, c0 + p // 2, p // 2 + (1 - home) * a0)
        mixed = jnp.where(u % 2 == 1, u // 2, a0 + NB + u // 2)
        late = jnp.where((home == 1) | (u >= 2 * NB), a0 + u, mixed)
        return jnp.where(p < 2 * NB, pair, jnp.where(u < 0, a0 - 1, late))

    def w_in_copies(p):
        c = C * chunk_of(p)
        cs = pl.multiple_of((1 - k) * block + c, C)
        co = pl.multiple_of(k * block + c, C)
        return (pltpu.make_async_copy(w_in_hbm.at[:, pl.ds(cs, C)], w_in_v.at[p, :, pl.ds(0, C)], w_in_sem.at[p // GROUP]),
                pltpu.make_async_copy(w_in_hbm.at[:, pl.ds(co, C)], w_in_v.at[p, :, pl.ds(C, C)], w_in_sem.at[p // GROUP]))

    def w_out_copy(i):
        r = pl.multiple_of(i * C, C)
        return pltpu.make_async_copy(w_out_hbm.at[pl.ds(r, C), :], w_out_v.at[i], w_out_sem)

    xa_copy = pltpu.make_async_copy(x_hbm.at[pl.ds(0, TA)], xa_v, misc_sem.at[0])
    xb_copy = pltpu.make_async_copy(x_hbm.at[pl.ds(TA, tb)], xb_v, misc_sem.at[8])
    g_copy = pltpu.make_async_copy(gain_hbm, gain_v.at[0], misc_sem.at[1])
    xa_copy.start()
    xb_copy.start()
    g_copy.start()

    barrier = pltpu.get_barrier_semaphore()
    for dy in range(2):
        for dr in range(4):
            if dy or dr:
                pl.semaphore_signal(barrier, inc=1, device_id=(dp, (y + dy) % 2, (row + dr) % 4), device_id_type=MESH)

    def start_w_in(p, _):
        for cp in w_in_copies(p):
            cp.start()
        return 0

    lax.fori_loop(0, N, start_w_in, 0)

    xa_copy.wait()
    xb_copy.wait()
    g_copy.wait()

    def row_sums(ref):
        v = ref[...].astype(F32)
        lane = lax.broadcasted_iota(jnp.int32, (v.shape[0], 128), 1)
        return jnp.where(lane == 0, jnp.sum(v, axis=1, keepdims=True), jnp.sum(v * v, axis=1, keepdims=True))

    me = 4 * y + row
    stat_g[me, :, :tok] = jnp.transpose(jnp.concatenate([row_sums(xa_v), row_sums(xb_v)], axis=0))[:2]
    with jax.named_scope('barrier'):
        pl.semaphore_wait(barrier, 7)

    def tok_copy(group, dy, dk):
        tk = (k + dk) % 2
        cols = pl.ds(pl.multiple_of(feat * tk, 128), feat)
        src, dst, sem = ((xa_v, x_ga, za_rsem), (xb_v, x_gb, zb_rsem))[group]
        return remote(src.at[:, cols], dst.at[row], z_ssem, sem, (dp, (y + dy) % 2, 2 * y + tk))

    def stat_copy(d):
        ty = (y + d // 4) % 2
        tr = (row + d % 4) % 4
        return remote(stat_g.at[me], stat_g.at[me], stat_ssem, stat_rsem, (dp, ty, tr))

    gain_cp = remote(gain_v.at[0], gain_v.at[1], z_ssem, misc_sem.at[3], y_next)
    half_cols = pl.ds(pl.multiple_of(feat * (1 - k), 128), feat)
    to_relay = remote(xa_v.at[:, half_cols], x_relay, z_ssem, misc_sem.at[2], y_next)
    from_relay = remote(x_relay, x_ga.at[row], z_ssem, za_rsem, (dp, y, 2 * (1 - x) + 1 - k))

    for d in range(1, 8):
        stat_copy(d).start()

    @pl.when(home == 0)
    def _():
        to_relay.start()
        tok_copy(1, 1, 0).start()
        tok_copy(1, 1, 1).start()
        tok_copy(1, 0, 0).start()
        tok_copy(1, 0, 1).start()
        tok_copy(0, 1, 0).start()
        tok_copy(0, 0, 0).start()
        tok_copy(0, 0, 1).start()

    @pl.when(home == 1)
    def _():
        gain_cp.start()
        for group in (1, 0):
            tok_copy(group, 0, 1).start()
            tok_copy(group, 1, 0).start()
            tok_copy(group, 1, 1).start()
        x_ga[row] = jnp.where(k == 0, xa_v[:, :feat], xa_v[:, feat:])
        x_gb[row] = jnp.where(k == 0, xb_v[:, :feat], xb_v[:, feat:])
        gain_v[1] = gain_v[0]
        with jax.named_scope('x_relay_wait'):
            to_relay.wait_recv()
        from_relay.start()

    @pl.when(home == 0)
    def _():
        with jax.named_scope('gain_wait'):
            gain_cp.wait_recv()
    gain = jnp.where(k == 0, gain_v[1, :feat], gain_v[1, feat:]).reshape(1, feat)
    acc[...] = jnp.zeros_like(acc)
    with jax.named_scope('stat_wait'):
        remote(stat_g.at[pl.ds(0, 7)], stat_g.at[pl.ds(0, 7)], stat_ssem, stat_rsem, y_next).wait_recv()

    def make_z(group):
        ref, sem = ((x_ga, za_rsem), (x_gb, zb_rsem))[group]

        @pl.when(home == 0)
        def _():
            with jax.named_scope('z_wait'):
                remote(ref, ref, z_ssem, sem, y_next).wait_recv()

        @pl.when(home == 1)
        def _():
            with jax.named_scope('z_wait'):
                remote(ref.at[pl.ds(0, 3)], ref.at[pl.ds(0, 3)], z_ssem, sem, y_next).wait_recv()

        t0, n, base = ((0, TA, 0), (TA, tb, rows_a))[group]
        for src in range(4):
            both = stat_g[src] + stat_g[4 + src]
            st = jnp.transpose(jnp.concatenate([both] * 4, axis=0))[t0:t0 + n] * (1.0 / (2 * half))
            mean = st[:, 0:1]
            var = st[:, 1:2] - mean * mean
            z = (ref[src].astype(F32) - mean) * lax.rsqrt(var + NORM_EPS) * gain
            z_v[pl.ds(base + n * src, n), :] = z.astype(BF16)

    row_group = (pl.ds(0, rows_a), pl.ds(rows_a, rows_b))

    def part_of(ref, j, part):
        if part == WHOLE:
            return ref.at[j]
        if part == FIRST:
            return ref.at[j, row_group[0]]
        return ref.at[pl.ds(j, part), row_group[1]]

    def rows_of(part):
        return pl.ds(0, rows_a + rows_b) if part == WHOLE else row_group[int(part > 0)]

    def d_copy(p, part, seq):
        return remote(part_of(d_send, p, part), part_of(d_recv, p, part), d_ssem, d_rsem.at[seq % RING], sibling)

    def b_index(j, part):
        return 9 + j // 2 if part == 2 else j + 4

    def x_group(j, part, first, sem):
        return remote(part_of(own, first + j, part), part_of(x_recv, j, part), x_ssem, x_rsem.at[sem], x_next)

    def x_copy_of(j, part, first):
        sem = x_rsem.at[b_index(j, part)] if part > 0 else x_rsem.at[j]
        return remote(part_of(own, first + j, part), part_of(x_recv, j, part), x_ssem, sem, x_next)

    def c_copy(j):
        return c_part(j, WHOLE)

    def c_part(j, part):
        return remote(part_of(own, c0 + j, part), part_of(c_recv.at[0], j, part), c_ssem, c_rsem.at[home * NC + (1 - home) * j], y_next)

    def c_relay(j, part):
        sem = c_rsem.at[NC + 1 + j // 3] if part > 0 else c_rsem.at[j]
        return remote(part_of(c_recv.at[0], j, part), part_of(c_recv.at[1], j, part), c_ssem, sem, x_next)

    last = NA - 1

    def both_home():
        return remote(part_of(own, a0 + last, 1), part_of(c_recv.at[0], NC, 1), c_ssem, c_rsem.at[NC + 3], y_next)

    def both_far():
        return remote(part_of(own, a0 + last, 1), part_of(c_recv.at[1], NC, 1), c_ssem, c_rsem.at[NC + 4],
                      (dp, 1 - y, 2 * (1 - x) + k))

    def pass_c(j):
        with jax.named_scope('c_wait'):
            remote(c_recv.at[0, j], c_recv.at[0, j], c_ssem, c_rsem.at[j], y_next).wait_recv()
        c_relay(j, FIRST).start()

    def up(p, part, seq):
        rows = rows_of(part)
        sums = jnp.dot(z_v[rows, :], w_in_v[p], preferred_element_type=F32)
        d_send[p, rows, :] = sums[:, :C]
        own[chunk_of(p), rows, :] = sums[:, C:]
        d_copy(p, part, seq).start()

    def pair_add(p, part, seq):
        with jax.named_scope('pair_wait'):
            d_copy(p, part, seq).wait_recv()
        q, rows = chunk_of(p), rows_of(part)
        own[q, rows, :] = own[q, rows, :] + d_recv[p, rows, :]

    def wait_w_in(p):
        with jax.named_scope('w_in_wait'):
            group = w_in_v.at[pl.ds(p, GROUP)]
            pltpu.make_async_copy(group, group, w_in_sem.at[p // GROUP]).wait()

    def pair_group(p, part, seq):
        pair_add(p, part, seq)
        q = chunk_of(p)

        @pl.when((q >= c0) & (q < a0))
        def _():
            c_part(q - c0, part).start()

        @pl.when((home == 1) & (q < c0))
        def _():
            x_group(q, part, 0, 9 + q // 2 if part else q).start()

        @pl.when((home == 0) & (q >= a0))
        def _():
            x_group(q - a0, part, a0, q - a0).start()

    def pair_sum(p):
        pair_add(p, WHOLE, p + EARLY)
        q = chunk_of(p)

        @pl.when((q >= c0) & (q < a0))
        def _():
            c_copy(q - c0).start()

        @pl.when((home == 1) & (q < c0))
        def _():
            x_copy_of(q, FIRST, 0).start()

            x_group(q, 1, 0, 9 + q // 2).start()

        @pl.when((home == 0) & (q >= a0 + NF))
        def _():
            x_copy_of(q - a0, FIRST, a0).start()

        @pl.when((home == 0) & (q >= a0) & (q < a0 + NF))
        def _():
            x_copy_of(q - a0, WHOLE, a0).start()

    def up_loop(lo, hi, part, seq, then):
        def step(p, _):
            if part != FIRST:
                @pl.when(p % GROUP == 0)
                def _():
                    wait_w_in(p)
            up(p, part, p + seq)
            if part != 1:
                w_out_copy(p).start()
            then(p)
            return 0

        lax.fori_loop(lo, hi, step, 0)

    def late(p):
        pair_sum(p - LAG)

        @pl.when((p == 17) & (home == 1))
        def _():
            pass_c(0)

    def flush(p):
        for i in range(2):
            pair_group(2 * p + 2 + i, 1, 2 * p + 2 + i)

    make_z(1)
    up_loop(0, 4, 1, 0, lambda p: None)
    up_loop(4, EARLY, 1, 0, lambda p: pair_group(p - 4, 1, p - 4))
    make_z(0)
    up_loop(0, 2, FIRST, EARLY, flush)
    up_loop(2, LAG, FIRST, EARLY, lambda p: None)
    up_loop(LAG, EARLY, FIRST, EARLY, lambda p: pair_group(p - LAG, FIRST, p - LAG + EARLY))
    up_loop(EARLY, EARLY + LAG, WHOLE, EARLY, lambda p: pair_group(p - LAG, FIRST, p - LAG + EARLY))
    up_loop(EARLY + LAG, N, WHOLE, EARLY, late)
    for p in range(N - LAG, N):
        pair_sum(p)

    @pl.when(home == 0)
    def _():
        x_copy_of(NF, 2, a0).start()
        x_copy_of(NF + 2, 2, a0).start()
        x_copy_of(NF + 4, 2, a0).start()
        both_far().start()
        x_copy_of(last, 1, a0).start()

    with jax.named_scope('w_out_wait'):
        pltpu.make_async_copy(w_out_v, w_out_v, w_out_sem).wait()

    def y_copy(j, part):
        sem = y_rsem.at[b_index(j, part)] if part > 0 else y_rsem.at[j]
        return remote(part_of(hall, j, part), part_of(hall, NA + j, part), y_ssem, sem, y_next)

    def b_sem(j, part):
        return b_rsem.at[NB + j // 2] if part > 0 else b_rsem.at[j]

    def relay_copy(j, part):
        return remote(part_of(hall, NA + j, part), part_of(hall, 2 * NA + j, part), b_ssem, b_sem(j, part), x_next)

    def back_copy(j, part):
        return remote(part_of(hall, 2 * NA + j, part), part_of(hall, 2 * NA + j, part), b_ssem, b_sem(j, part), y_next)

    def put_h(j, part, left, right):
        rows = rows_of(part)
        for c in range(max(part, 1)):
            total = left(c)[rows, :] + right(c)[rows, :]
            hall[j + c, rows, :] = jax.nn.gelu(total, approximate=True).astype(BF16)

    def make_h(j, part, first, send=True):
        with jax.named_scope('x_wait'):
            x_copy_of(j, part, 0).wait_recv()
        put_h(j, part, lambda c: own.at[first + j + c], lambda c: x_recv.at[j + c])
        if send:
            y_copy(j, part).start()

    def make_h_c(j, part, first=False):
        with jax.named_scope('c_wait'):
            if first:
                own_part = c_recv.at[0, pl.ds(0, NC)]
                remote(own_part, own_part, c_ssem, c_rsem.at[NC], y_next).wait_recv()
            c_relay(j, part).wait_recv()
        put_h(c0 + j, part, lambda c: c_recv.at[0, j + c], lambda c: c_recv.at[1, j + c])
        yc_copy(j, part).start()

    def yc_copy(j, part):
        sem = y_rsem.at[NA + j // 3] if part > 0 else y_rsem.at[c0 + j]
        return remote(part_of(hall, c0 + j, part), part_of(hall, NA + c0 + j, part), y_ssem, sem, y_next)

    def down(slot, i, part):
        rows = rows_of(part)
        parts = [jnp.dot(hall[slot + c, rows, :], w_out_v[i + c], preferred_element_type=F32)
                 for c in range(max(part, 1))]
        acc[rows, :] += sum(parts[1:], parts[0])

    e_recv, f_send, f_recv = (ea_recv, eb_recv), (fa_send, fb_send), (fa_recv, fb_recv)

    def token_rows(group, r):
        n, base = ((TA, 0), (tb, rows_a))[group]
        return pl.ds(pl.multiple_of(base + n * r, 8), n)

    def e_copy(group, s):
        r = 2 * (s * x + (1 - s) * (1 - x)) + 1 - k
        return remote(acc.at[token_rows(group, r)], e_recv[group].at[s], e_ssem, e_rsem.at[group], sibling)

    def f_copy(group):
        return remote(f_send[group], f_recv[group], f_ssem, f_rsem.at[group], x_next)

    def end_start(group):
        e_copy(group, 0).start()
        e_copy(group, 1).start()

    def end_send(group):
        with jax.named_scope('e0_wait'):
            remote(e_recv[group], e_recv[group], e_ssem, e_rsem.at[group], sibling).wait_recv()
        f_send[group][...] = acc[token_rows(group, 2 * (1 - x) + k), :] + e_recv[group][0]
        f_copy(group).start()

    def end_send_from(core):
        @pl.when(k == core)
        def _():
            end_send(0)

    def end_sum(group):
        with jax.named_scope('f_wait'):
            f_copy(group).wait_recv()
        total = acc[token_rows(group, row), :] + e_recv[group][1] + f_recv[group][...]
        t0, n = ((0, TA), (TA, tb))[group]
        out_v[t0:t0 + n, :] = ((xa_v, xb_v)[group][...].astype(F32) + total).astype(BF16)

    def loop(lo, hi, step):
        def body(i, _):
            step(i)
            return 0
        lax.fori_loop(lo, hi, body, 0)

    @pl.when(home == 1)
    def _():
        def relay(i, part):
            with jax.named_scope('relay_wait'):
                y_copy(i, part).wait_recv()
            relay_copy(i, part).start()

        def b_step(i, part):
            with jax.named_scope('b_wait'):
                back_copy(i, part).wait_recv()
            down(2 * NA + i, i, part)

        def c_step(i, part):
            with jax.named_scope('ch_wait'):
                yc_copy(i, part).wait_recv()
            down(NA + c0 + i, c0 + i, part)

        def a_step(j, part):
            make_h(j, part, a0)
            down(j, a0 + j, part)

        pass_c(1)
        both_home().start()

        def step(j):
            @pl.when(j == 2)
            def _():
                pass_c(2)
            a_step(j, WHOLE)

        loop(0, NF, step)

        def step(j):
            for t, i in ((4, 3), (6, 4)):
                @pl.when(j == t)
                def _():
                    pass_c(i)

            @pl.when(j == 7)
            def _():
                relay(0, FIRST)
                relay(1, FIRST)
            a_step(j, FIRST)

        loop(NF, 8, step)
        relay(2, FIRST)
        relay(3, FIRST)
        c_relay(0, 3).start()
        c_relay(3, 2).start()

        def step(t):
            a_step(8 + t, FIRST)

            @pl.when(t == 0)
            def _():
                relay(0, 2)
                relay(2, 2)

            @pl.when(t == 1)
            def _():
                c_step(1, FIRST)
            c_step(2 * t, FIRST)

        loop(0, 2, step)
        a_step(10, FIRST)
        loop(3, 5, lambda i: c_step(i, FIRST))
        a_step(NF, 2)
        loop(0, 2, lambda i: b_step(i, FIRST))
        a_step(NF + 2, 2)
        b_step(2, FIRST)
        b_step(NB - 1, FIRST)
        end_start(0)
        make_h(NF + 4, 2, a0)
        end_send_from(0)
        down(NF + 4, a0 + NF + 4, 2)
        c_step(0, 3)
        end_send_from(1)
        make_h(last, 1, a0, send=False)
        down(last, a0 + last, 1)
        c_step(3, 2)
        loop(0, 2, lambda m: b_step(2 * m, 2))

    @pl.when(home == 0)
    def _():
        def a_step(j, part):
            with jax.named_scope('a_wait'):
                y_copy(j, part).wait_recv()
            down(NA + j, a0 + j, part)

        def b_pass(i, part):
            with jax.named_scope('b_wait'):
                relay_copy(i, part).wait_recv()
            back_copy(i, part).start()

        def b_step(i, part):
            b_pass(i, part)
            down(2 * NA + i, i, part)

        def c_step(i, part, first=False):
            make_h_c(i, part, first)
            down(c0 + i, c0 + i, part)

        loop(0, NB, lambda j: make_h(j, FIRST, 0))
        loop(0, NB // 2, lambda m: make_h(2 * m, 2, 0))
        c_step(0, FIRST, first=True)

        def step(t):
            c_step(1 + t, FIRST)
            a_step(t, WHOLE)

        loop(0, NF, step)

        def step(t):
            b_step(t, FIRST)
            a_step(NF + t, FIRST)

        loop(0, 4, step)
        loop(8, 10, lambda j: a_step(j, FIRST))
        c_step(0, 3)
        a_step(10, FIRST)
        end_start(0)
        end_send_from(0)
        c_step(3, 2)
        b_pass(0, 2)
        b_pass(2, 2)
        down(2 * NA, 0, 4)
        a_step(NF, 2)
        end_send_from(1)
        with jax.named_scope('both_wait'):
            both_home().wait_recv()
            both_far().wait_recv()
        put_h(c0 + NC, 1, lambda c: c_recv.at[0, NC + c], lambda c: c_recv.at[1, NC + c])
        down(c0 + NC, a0 + last, 1)
        a_step(NF + 2, 2)
        a_step(NF + 4, 2)

    end_start(1)
    end_send(1)

    def sent(ref, sem):
        remote(ref, ref, sem, sem, y_next).wait_send()

    with jax.named_scope('drain'):
        sent(stat_g.at[pl.ds(0, 7)], stat_ssem)
        sent(d_send, d_ssem)
        sent(hall.at[pl.ds(0, NB)], b_ssem)
        sent(c_recv.at[0, pl.ds(0, NC)], c_ssem)
        sent(part_of(own, 0, 1), c_ssem)
        sent(ea_recv, e_ssem)
        sent(eb_recv, e_ssem)

        @pl.when(home == 0)
        def _():
            sent(x_ga, z_ssem)
            sent(x_gb, z_ssem)
            sent(own.at[pl.ds(0, NA)], x_ssem)
            sent(hall.at[pl.ds(0, NB + NC)], y_ssem)

        @pl.when(home == 1)
        def _():
            gain_cp.wait_send()
            sent(x_ga, z_ssem)
            sent(x_gb.at[pl.ds(0, 3)], z_ssem)
            sent(own.at[pl.ds(0, NB)], x_ssem)
            sent(c_recv.at[1, pl.ds(0, NC)], c_ssem)
            sent(hall.at[pl.ds(0, last)], y_ssem)
            sent(part_of(hall, 0, FIRST), y_ssem)

    end_sum(0)
    end_sum(1)
    sent(fa_send, f_ssem)
    sent(fb_send, f_ssem)


def solution(mesh):
    def body(x_blk, gain_blk, w_in_blk, w_out_blk):
        tok, half = x_blk.shape
        feat = w_in_blk.shape[0]
        tokens = 4 * tok
        dma = pltpu.SemaphoreType.DMA
        return pl.pallas_call(
            kernel,
            out_shape=pltpu.VMEM((tok, half), BF16),
            in_specs=[pl.BlockSpec(memory_space=pl.ANY)] * 4,
            out_specs=pl.BlockSpec(memory_space=pltpu.VMEM),
            scratch_shapes=[
                pltpu.VMEM((TA, half), BF16),
                pltpu.VMEM((tok - TA, half), BF16),
                pltpu.VMEM((2, half), F32),
                pltpu.VMEM((8, 2, 128), F32),
                pltpu.VMEM((4, TA, feat), BF16),
                pltpu.VMEM((4, tok - TA, feat), BF16),
                pltpu.VMEM((TA, feat), BF16),
                pltpu.VMEM((tokens, feat), BF16),
                pltpu.VMEM((N, feat, 2 * C), BF16),
                pltpu.VMEM((N, C, half), BF16),
                pltpu.VMEM((N, tokens, C), F32),
                pltpu.VMEM((N, tokens, C), F32),
                pltpu.VMEM((N, tokens, C), F32),
                pltpu.VMEM((NA, tokens, C), F32),
                pltpu.VMEM((2, NC + 1, tokens, C), F32),
                pltpu.VMEM((2 * NA + NB, tokens, C), BF16),
                pltpu.VMEM((tokens, half), F32),
                pltpu.VMEM((2, TA, half), F32),
                pltpu.VMEM((2, tok - TA, half), F32),
                pltpu.VMEM((TA, half), F32),
                pltpu.VMEM((TA, half), F32),
                pltpu.VMEM((tok - TA, half), F32),
                pltpu.VMEM((tok - TA, half), F32),
                dma((9,)),
                dma((N // GROUP,)),
                dma((2,)),
                dma((RING,)),
                dma((NA + 4,)),
                dma((NA + 4,)),
                dma((NB + NB // 2,)),
                dma((NC + 5,)),
                dma((2,)),
                dma((2,)),
            ],
            compiler_params=pltpu.CompilerParams(
                collective_id=0, has_side_effects=True, vmem_limit_bytes=66_500_000
            ),
        )(x_blk, gain_blk, w_in_blk, w_out_blk)

    return jax.shard_map(
        body,
        mesh=mesh,
        in_specs=(P(("dp", "row"), "col"), P("col"), P("row", "col"), P("row", "col")),
        out_specs=P(("dp", "row"), "col"),
        check_vma=False,
    )
```

```python
import jax
import jax.numpy as jnp
from jax import lax
from jax.experimental import pallas as pl
from jax.experimental.pallas import tpu as pltpu
from jax.sharding import PartitionSpec as P

NORM_EPS = 1e-5
MESH = pl.DeviceIdType.MESH
WHOLE, FIRST = -1, 0
F32 = jnp.float32
BF16 = jnp.bfloat16

C = 256
NB = 4
NC = 5
NA = 11
N = NA + NB + NC
NF = 4
EARLY = 6
GROUP = 10
LAG = 3
RING = 10
TA = 16


def kernel(x_hbm, gain_hbm, w_in_hbm, w_out_hbm, out_v,
           xa_v, xb_v, gain_v, stat_g, x_ga, x_gb, x_relay, z_v, w_in_v, w_out_v, d_send, d_recv, own, x_recv, c_recv, hall,
           acc, ea_recv, eb_recv, fa_send, fa_recv, fb_send, fb_recv,
           misc_sem, w_in_sem, send_sem, d_rsem, x_rsem, y_rsem, b_rsem, c_rsem, e_rsem, f_rsem):
    w_out_sem, stat_rsem, za_rsem, zb_rsem = [misc_sem.at[i] for i in range(4, 8)]
    stat_ssem = z_ssem = d_ssem = x_ssem = y_ssem = b_ssem = c_ssem = e_ssem = send_sem.at[0]
    f_ssem = send_sem.at[1]
    y = lax.axis_index("col")
    row = lax.axis_index("row")
    x = row // 2
    k = row % 2
    dp = lax.axis_index("dp")
    home = 1 - (x + y) % 2
    tok, half = out_v.shape
    feat = half // 2
    block = N * C
    rows_a = 4 * TA
    tb = tok - TA
    rows_b = 4 * tb
    sibling = (dp, y, 2 * x + 1 - k)
    x_next = (dp, y, 2 * (1 - x) + k)
    y_next = (dp, 1 - y, row)

    def remote(src, dst, ssem, rsem, dev):
        return pltpu.make_async_remote_copy(src_ref=src, dst_ref=dst, send_sem=ssem, recv_sem=rsem,
                                            device_id=dev, device_id_type=MESH)

    c0, a0 = NB, NB + NC

    def chunk_of(p):
        u = p - 2 * NB - 1
        pair = jnp.where(p % 2 == 1, c0 + p // 2, p // 2 + (1 - home) * a0)
        mixed = jnp.where(u % 2 == 1, u // 2, a0 + NB + u // 2)
        late = jnp.where((home == 1) | (u >= 2 * NB), a0 + u, mixed)
        return jnp.where(p < 2 * NB, pair, jnp.where(u < 0, a0 - 1, late))

    def w_in_copies(p):
        c = C * chunk_of(p)
        cs = pl.multiple_of((1 - k) * block + c, C)
        co = pl.multiple_of(k * block + c, C)
        return (pltpu.make_async_copy(w_in_hbm.at[:, pl.ds(cs, C)], w_in_v.at[p, :, pl.ds(0, C)], w_in_sem.at[p // GROUP]),
                pltpu.make_async_copy(w_in_hbm.at[:, pl.ds(co, C)], w_in_v.at[p, :, pl.ds(C, C)], w_in_sem.at[p // GROUP]))

    def w_out_copy(i):
        r = pl.multiple_of(i * C, C)
        return pltpu.make_async_copy(w_out_hbm.at[pl.ds(r, C), :], w_out_v.at[i], w_out_sem)

    xa_copy = pltpu.make_async_copy(x_hbm.at[pl.ds(0, TA)], xa_v, misc_sem.at[0])
    xb_copy = pltpu.make_async_copy(x_hbm.at[pl.ds(TA, tb)], xb_v, misc_sem.at[8])
    g_copy = pltpu.make_async_copy(gain_hbm, gain_v.at[0], misc_sem.at[1])
    xa_copy.start()
    xb_copy.start()
    g_copy.start()

    barrier = pltpu.get_barrier_semaphore()
    for dy in range(2):
        for dr in range(4):
            if dy or dr:
                pl.semaphore_signal(barrier, inc=1, device_id=(dp, (y + dy) % 2, (row + dr) % 4), device_id_type=MESH)

    def start_w_in(p, _):
        for cp in w_in_copies(p):
            cp.start()
        return 0

    lax.fori_loop(0, N, start_w_in, 0)

    xa_copy.wait()
    xb_copy.wait()
    g_copy.wait()

    def row_sums(ref):
        v = ref[...].astype(F32)
        lane = lax.broadcasted_iota(jnp.int32, (v.shape[0], 128), 1)
        return jnp.where(lane == 0, jnp.sum(v, axis=1, keepdims=True), jnp.sum(v * v, axis=1, keepdims=True))

    me = 4 * y + row
    stat_g[me, :, :tok] = jnp.transpose(jnp.concatenate([row_sums(xa_v), row_sums(xb_v)], axis=0))[:2]
    with jax.named_scope('barrier'):
        pl.semaphore_wait(barrier, 7)

    def tok_copy(group, dy, dk):
        tk = (k + dk) % 2
        cols = pl.ds(pl.multiple_of(feat * tk, 128), feat)
        src, dst, sem = ((xa_v, x_ga, za_rsem), (xb_v, x_gb, zb_rsem))[group]
        return remote(src.at[:, cols], dst.at[row], z_ssem, sem, (dp, (y + dy) % 2, 2 * y + tk))

    def stat_copy(d):
        ty = (y + d // 4) % 2
        tr = (row + d % 4) % 4
        return remote(stat_g.at[me], stat_g.at[me], stat_ssem, stat_rsem, (dp, ty, tr))

    gain_cp = remote(gain_v.at[0], gain_v.at[1], z_ssem, misc_sem.at[3], y_next)
    half_cols = pl.ds(pl.multiple_of(feat * (1 - k), 128), feat)
    to_relay = remote(xa_v.at[:, half_cols], x_relay, z_ssem, misc_sem.at[2], y_next)
    from_relay = remote(x_relay, x_ga.at[row], z_ssem, za_rsem, (dp, y, 2 * (1 - x) + 1 - k))

    for d in range(1, 8):
        stat_copy(d).start()

    @pl.when(home == 0)
    def _():
        to_relay.start()
        tok_copy(1, 1, 0).start()
        tok_copy(1, 1, 1).start()
        tok_copy(1, 0, 0).start()
        tok_copy(1, 0, 1).start()
        tok_copy(0, 1, 0).start()
        tok_copy(0, 0, 0).start()
        tok_copy(0, 0, 1).start()

    @pl.when(home == 1)
    def _():
        gain_cp.start()
        for group in (1, 0):
            tok_copy(group, 0, 1).start()
            tok_copy(group, 1, 0).start()
            tok_copy(group, 1, 1).start()
        x_ga[row] = jnp.where(k == 0, xa_v[:, :feat], xa_v[:, feat:])
        x_gb[row] = jnp.where(k == 0, xb_v[:, :feat], xb_v[:, feat:])
        gain_v[1] = gain_v[0]
        with jax.named_scope('x_relay_wait'):
            to_relay.wait_recv()
        from_relay.start()

    @pl.when(home == 0)
    def _():
        with jax.named_scope('gain_wait'):
            gain_cp.wait_recv()
    gain = jnp.where(k == 0, gain_v[1, :feat], gain_v[1, feat:]).reshape(1, feat)
    acc[...] = jnp.zeros_like(acc)
    with jax.named_scope('stat_wait'):
        remote(stat_g.at[pl.ds(0, 7)], stat_g.at[pl.ds(0, 7)], stat_ssem, stat_rsem, y_next).wait_recv()

    def make_z(group):
        ref, sem = ((x_ga, za_rsem), (x_gb, zb_rsem))[group]

        @pl.when(home == 0)
        def _():
            with jax.named_scope('z_wait'):
                remote(ref, ref, z_ssem, sem, y_next).wait_recv()

        @pl.when(home == 1)
        def _():
            with jax.named_scope('z_wait'):
                remote(ref.at[pl.ds(0, 3)], ref.at[pl.ds(0, 3)], z_ssem, sem, y_next).wait_recv()

        t0, n, base = ((0, TA, 0), (TA, tb, rows_a))[group]
        for src in range(4):
            both = stat_g[src] + stat_g[4 + src]
            st = jnp.transpose(jnp.concatenate([both] * 4, axis=0))[t0:t0 + n] * (1.0 / (2 * half))
            mean = st[:, 0:1]
            var = st[:, 1:2] - mean * mean
            z = (ref[src].astype(F32) - mean) * lax.rsqrt(var + NORM_EPS) * gain
            z_v[pl.ds(base + n * src, n), :] = z.astype(BF16)

    row_group = (pl.ds(0, rows_a), pl.ds(rows_a, rows_b))

    def part_of(ref, j, part):
        if part == WHOLE:
            return ref.at[j]
        if part == FIRST:
            return ref.at[j, row_group[0]]
        return ref.at[pl.ds(j, part), row_group[1]]

    def rows_of(part):
        return pl.ds(0, rows_a + rows_b) if part == WHOLE else row_group[int(part > 0)]

    def d_copy(p, part, seq):
        return remote(part_of(d_send, p, part), part_of(d_recv, p, part), d_ssem, d_rsem.at[seq % RING], sibling)

    def b_index(j, part):
        return 9 + j // 2 if part == 2 else j + 5

    def x_group(j, part, first, sem):
        return remote(part_of(own, first + j, part), part_of(x_recv, j, part), x_ssem, x_rsem.at[sem], x_next)

    def x_copy_of(j, part, first):
        sem = x_rsem.at[b_index(j, part)] if part > 0 else x_rsem.at[j]
        return remote(part_of(own, first + j, part), part_of(x_recv, j, part), x_ssem, sem, x_next)

    def c_copy(j):
        return c_part(j, WHOLE)

    def c_part(j, part):
        return remote(part_of(own, c0 + j, part), part_of(c_recv.at[0], j, part), c_ssem, c_rsem.at[home * NC + (1 - home) * j], y_next)

    def c_relay(j, part):
        sem = c_rsem.at[NC + 1 + j // 3] if part > 0 else c_rsem.at[j]
        return remote(part_of(c_recv.at[0], j, part), part_of(c_recv.at[1], j, part), c_ssem, sem, x_next)

    last = NA - 1

    def both_home():
        return remote(part_of(own, a0 + last, 1), part_of(c_recv.at[0], NC, 1), c_ssem, c_rsem.at[NC + 3], y_next)

    def both_far():
        return remote(part_of(own, a0 + last, 1), part_of(c_recv.at[1], NC, 1), c_ssem, c_rsem.at[NC + 4],
                      (dp, 1 - y, 2 * (1 - x) + k))

    def pass_c(j):
        with jax.named_scope('c_wait'):
            remote(c_recv.at[0, j], c_recv.at[0, j], c_ssem, c_rsem.at[j], y_next).wait_recv()
        c_relay(j, FIRST).start()

    def up(p, part, seq):
        rows = rows_of(part)
        sums = jnp.dot(z_v[rows, :], w_in_v[p], preferred_element_type=F32)
        d_send[p, rows, :] = sums[:, :C]
        own[chunk_of(p), rows, :] = sums[:, C:]
        d_copy(p, part, seq).start()

    def pair_add(p, part, seq):
        with jax.named_scope('pair_wait'):
            d_copy(p, part, seq).wait_recv()
        q, rows = chunk_of(p), rows_of(part)
        own[q, rows, :] = own[q, rows, :] + d_recv[p, rows, :]

    def wait_w_in(p):
        with jax.named_scope('w_in_wait'):
            group = w_in_v.at[pl.ds(p, GROUP)]
            pltpu.make_async_copy(group, group, w_in_sem.at[p // GROUP]).wait()

    def pair_group(p, part, seq):
        pair_add(p, part, seq)
        q = chunk_of(p)

        @pl.when((q >= c0) & (q < a0))
        def _():
            c_part(q - c0, part).start()

        @pl.when((home == 1) & (q < c0))
        def _():
            x_group(q, part, 0, 9 + q // 2 if part else q).start()

        @pl.when((home == 0) & (q >= a0))
        def _():
            x_group(q - a0, part, a0, q - a0).start()

    def pair_sum(p):
        pair_add(p, WHOLE, p + EARLY)
        q = chunk_of(p)

        @pl.when((q >= c0) & (q < a0))
        def _():
            c_copy(q - c0).start()

        @pl.when((home == 1) & (q < c0))
        def _():
            x_copy_of(q, FIRST, 0).start()

            x_group(q, 1, 0, 9 + q // 2).start()

        @pl.when((home == 0) & (q >= a0 + NF))
        def _():
            x_copy_of(q - a0, FIRST, a0).start()

        @pl.when((home == 0) & (q >= a0) & (q < a0 + NF))
        def _():
            x_copy_of(q - a0, WHOLE, a0).start()

    def up_loop(lo, hi, part, seq, then):
        def step(p, _):
            if part != FIRST:
                @pl.when(p % GROUP == 0)
                def _():
                    wait_w_in(p)
            up(p, part, p + seq)
            if part != 1:
                w_out_copy(p).start()
            then(p)
            return 0

        lax.fori_loop(lo, hi, step, 0)

    def late(p):
        pair_sum(p - LAG)

        @pl.when((p == 17) & (home == 1))
        def _():
            pass_c(0)

    def flush(p):
        for i in range(2):
            pair_group(2 * p + 2 + i, 1, 2 * p + 2 + i)

    make_z(1)
    up_loop(0, 4, 1, 0, lambda p: None)
    up_loop(4, EARLY, 1, 0, lambda p: pair_group(p - 4, 1, p - 4))
    make_z(0)
    up_loop(0, 2, FIRST, EARLY, flush)
    up_loop(2, LAG, FIRST, EARLY, lambda p: None)
    up_loop(LAG, EARLY, FIRST, EARLY, lambda p: pair_group(p - LAG, FIRST, p - LAG + EARLY))
    up_loop(EARLY, EARLY + LAG, WHOLE, EARLY, lambda p: pair_group(p - LAG, FIRST, p - LAG + EARLY))
    up_loop(EARLY + LAG, N, WHOLE, EARLY, late)
    for p in range(N - LAG, N):
        pair_sum(p)

    @pl.when(home == 0)
    def _():
        x_copy_of(NF, 2, a0).start()
        x_copy_of(NF + 2, 2, a0).start()
        x_copy_of(NF + 4, 1, a0).start()
        x_copy_of(NF + 5, 1, a0).start()
        both_far().start()
        x_copy_of(last, 1, a0).start()

    with jax.named_scope('w_out_wait'):
        pltpu.make_async_copy(w_out_v, w_out_v, w_out_sem).wait()

    def y_copy(j, part):
        sem = y_rsem.at[b_index(j, part)] if part > 0 else y_rsem.at[j]
        return remote(part_of(hall, j, part), part_of(hall, NA + j, part), y_ssem, sem, y_next)

    def b_sem(j, part):
        return b_rsem.at[NB + j // 2] if part > 0 else b_rsem.at[j]

    def relay_copy(j, part):
        return remote(part_of(hall, NA + j, part), part_of(hall, 2 * NA + j, part), b_ssem, b_sem(j, part), x_next)

    def back_copy(j, part):
        return remote(part_of(hall, 2 * NA + j, part), part_of(hall, 2 * NA + j, part), b_ssem, b_sem(j, part), y_next)

    def put_h(j, part, left, right):
        rows = rows_of(part)
        for c in range(max(part, 1)):
            total = left(c)[rows, :] + right(c)[rows, :]
            hall[j + c, rows, :] = jax.nn.gelu(total, approximate=True).astype(BF16)

    def make_h(j, part, first, send=True):
        with jax.named_scope('x_wait'):
            x_copy_of(j, part, 0).wait_recv()
        put_h(j, part, lambda c: own.at[first + j + c], lambda c: x_recv.at[j + c])
        if send:
            y_copy(j, part).start()

    def make_h_c(j, part, first=False):
        with jax.named_scope('c_wait'):
            if first:
                own_part = c_recv.at[0, pl.ds(0, NC)]
                remote(own_part, own_part, c_ssem, c_rsem.at[NC], y_next).wait_recv()
            c_relay(j, part).wait_recv()
        put_h(c0 + j, part, lambda c: c_recv.at[0, j + c], lambda c: c_recv.at[1, j + c])
        yc_copy(j, part).start()

    def yc_copy(j, part):
        sem = y_rsem.at[NA + j // 3] if part > 0 else y_rsem.at[c0 + j]
        return remote(part_of(hall, c0 + j, part), part_of(hall, NA + c0 + j, part), y_ssem, sem, y_next)

    def down(slot, i, part):
        rows = rows_of(part)
        parts = [jnp.dot(hall[slot + c, rows, :], w_out_v[i + c], preferred_element_type=F32)
                 for c in range(max(part, 1))]
        acc[rows, :] += sum(parts[1:], parts[0])

    e_recv, f_send, f_recv = (ea_recv, eb_recv), (fa_send, fb_send), (fa_recv, fb_recv)

    def token_rows(group, r):
        n, base = ((TA, 0), (tb, rows_a))[group]
        return pl.ds(pl.multiple_of(base + n * r, 8), n)

    def e_copy(group, s):
        r = 2 * (s * x + (1 - s) * (1 - x)) + 1 - k
        return remote(acc.at[token_rows(group, r)], e_recv[group].at[s], e_ssem, e_rsem.at[group], sibling)

    def f_copy(group):
        return remote(f_send[group], f_recv[group], f_ssem, f_rsem.at[group], x_next)

    def end_start(group):
        e_copy(group, 0).start()
        e_copy(group, 1).start()

    def end_send(group):
        with jax.named_scope('e0_wait'):
            remote(e_recv[group], e_recv[group], e_ssem, e_rsem.at[group], sibling).wait_recv()
        f_send[group][...] = acc[token_rows(group, 2 * (1 - x) + k), :] + e_recv[group][0]
        f_copy(group).start()

    def end_send_from(core):
        @pl.when(k == core)
        def _():
            end_send(0)

    def end_sum(group):
        with jax.named_scope('f_wait'):
            f_copy(group).wait_recv()
        total = acc[token_rows(group, row), :] + e_recv[group][1] + f_recv[group][...]
        t0, n = ((0, TA), (TA, tb))[group]
        out_v[t0:t0 + n, :] = ((xa_v, xb_v)[group][...].astype(F32) + total).astype(BF16)

    def loop(lo, hi, step):
        def body(i, _):
            step(i)
            return 0
        lax.fori_loop(lo, hi, body, 0)

    @pl.when(home == 1)
    def _():
        def relay(i, part):
            with jax.named_scope('relay_wait'):
                y_copy(i, part).wait_recv()
            relay_copy(i, part).start()

        def b_step(i, part):
            with jax.named_scope('b_wait'):
                back_copy(i, part).wait_recv()
            down(2 * NA + i, i, part)

        def c_step(i, part):
            with jax.named_scope('ch_wait'):
                yc_copy(i, part).wait_recv()
            down(NA + c0 + i, c0 + i, part)

        def a_step(j, part):
            make_h(j, part, a0)
            down(j, a0 + j, part)

        pass_c(1)
        both_home().start()

        def step(j):
            @pl.when(j == 2)
            def _():
                pass_c(2)
            a_step(j, WHOLE)

        loop(0, NF, step)

        def step(j):
            for t, i in ((4, 3), (6, 4)):
                @pl.when(j == t)
                def _():
                    pass_c(i)

            @pl.when(j == 7)
            def _():
                relay(0, FIRST)
                relay(1, FIRST)
            a_step(j, FIRST)

        loop(NF, 8, step)
        relay(2, FIRST)
        relay(3, FIRST)
        c_relay(0, 3).start()
        c_relay(3, 2).start()

        def step(t):
            a_step(8 + t, FIRST)

            @pl.when(t == 0)
            def _():
                relay(0, 2)
                relay(2, 2)

            @pl.when(t == 1)
            def _():
                c_step(1, FIRST)
            c_step(2 * t, FIRST)

        loop(0, 2, step)
        a_step(10, FIRST)
        loop(3, 5, lambda i: c_step(i, FIRST))
        a_step(NF, 2)
        loop(0, 2, lambda i: b_step(i, FIRST))
        a_step(NF + 2, 2)
        b_step(2, FIRST)
        b_step(NB - 1, FIRST)
        end_start(0)
        make_h(NF + 4, 1, a0)
        make_h(NF + 5, 1, a0)
        end_send_from(0)
        down(NF + 4, a0 + NF + 4, 2)
        c_step(0, 3)
        end_send_from(1)
        make_h(last, 1, a0, send=False)
        down(last, a0 + last, 1)
        c_step(3, 2)
        loop(0, 2, lambda m: b_step(2 * m, 2))

    @pl.when(home == 0)
    def _():
        def a_step(j, part):
            with jax.named_scope('a_wait'):
                y_copy(j, part).wait_recv()
            down(NA + j, a0 + j, part)

        def b_pass(i, part):
            with jax.named_scope('b_wait'):
                relay_copy(i, part).wait_recv()
            back_copy(i, part).start()

        def b_step(i, part):
            b_pass(i, part)
            down(2 * NA + i, i, part)

        def c_step(i, part, first=False):
            make_h_c(i, part, first)
            down(c0 + i, c0 + i, part)

        loop(0, NB, lambda j: make_h(j, FIRST, 0))
        loop(0, NB // 2, lambda m: make_h(2 * m, 2, 0))
        c_step(0, FIRST, first=True)

        def step(t):
            c_step(1 + t, FIRST)
            a_step(t, WHOLE)

        loop(0, NF, step)

        def step(t):
            b_step(t, FIRST)
            a_step(NF + t, FIRST)

        loop(0, 4, step)
        loop(8, 10, lambda j: a_step(j, FIRST))
        c_step(0, 3)
        a_step(10, FIRST)
        end_start(0)
        end_send_from(0)
        c_step(3, 2)
        b_pass(0, 2)
        b_pass(2, 2)
        down(2 * NA, 0, 4)
        a_step(NF, 2)
        end_send_from(1)
        with jax.named_scope('both_wait'):
            both_home().wait_recv()
            both_far().wait_recv()
        put_h(c0 + NC, 1, lambda c: c_recv.at[0, NC + c], lambda c: c_recv.at[1, NC + c])
        down(c0 + NC, a0 + last, 1)
        a_step(NF + 2, 2)
        with jax.named_scope('a_wait'):
            y_copy(NF + 4, 1).wait_recv()
            y_copy(NF + 5, 1).wait_recv()
        down(NA + NF + 4, a0 + NF + 4, 2)

    end_start(1)
    end_send(1)

    def sent(ref, sem):
        remote(ref, ref, sem, sem, y_next).wait_send()

    with jax.named_scope('drain'):
        sent(stat_g.at[pl.ds(0, 7)], stat_ssem)
        sent(d_send, d_ssem)
        sent(hall.at[pl.ds(0, NB)], b_ssem)
        sent(c_recv.at[0, pl.ds(0, NC)], c_ssem)
        sent(part_of(own, 0, 1), c_ssem)
        sent(ea_recv, e_ssem)
        sent(eb_recv, e_ssem)

        @pl.when(home == 0)
        def _():
            sent(x_ga, z_ssem)
            sent(x_gb, z_ssem)
            sent(own.at[pl.ds(0, NA)], x_ssem)
            sent(hall.at[pl.ds(0, NB + NC)], y_ssem)

        @pl.when(home == 1)
        def _():
            gain_cp.wait_send()
            sent(x_ga, z_ssem)
            sent(x_gb.at[pl.ds(0, 3)], z_ssem)
            sent(own.at[pl.ds(0, NB)], x_ssem)
            sent(c_recv.at[1, pl.ds(0, NC)], c_ssem)
            sent(hall.at[pl.ds(0, last)], y_ssem)
            sent(part_of(hall, 0, FIRST), y_ssem)

    end_sum(0)
    end_sum(1)
    sent(fa_send, f_ssem)
    sent(fb_send, f_ssem)


def solution(mesh):
    def body(x_blk, gain_blk, w_in_blk, w_out_blk):
        tok, half = x_blk.shape
        feat = w_in_blk.shape[0]
        tokens = 4 * tok
        dma = pltpu.SemaphoreType.DMA
        return pl.pallas_call(
            kernel,
            out_shape=pltpu.VMEM((tok, half), BF16),
            in_specs=[pl.BlockSpec(memory_space=pl.ANY)] * 4,
            out_specs=pl.BlockSpec(memory_space=pltpu.VMEM),
            scratch_shapes=[
                pltpu.VMEM((TA, half), BF16),
                pltpu.VMEM((tok - TA, half), BF16),
                pltpu.VMEM((2, half), F32),
                pltpu.VMEM((8, 2, 128), F32),
                pltpu.VMEM((4, TA, feat), BF16),
                pltpu.VMEM((4, tok - TA, feat), BF16),
                pltpu.VMEM((TA, feat), BF16),
                pltpu.VMEM((tokens, feat), BF16),
                pltpu.VMEM((N, feat, 2 * C), BF16),
                pltpu.VMEM((N, C, half), BF16),
                pltpu.VMEM((N, tokens, C), F32),
                pltpu.VMEM((N, tokens, C), F32),
                pltpu.VMEM((N, tokens, C), F32),
                pltpu.VMEM((NA, tokens, C), F32),
                pltpu.VMEM((2, NC + 1, tokens, C), F32),
                pltpu.VMEM((2 * NA + NB, tokens, C), BF16),
                pltpu.VMEM((tokens, half), F32),
                pltpu.VMEM((2, TA, half), F32),
                pltpu.VMEM((2, tok - TA, half), F32),
                pltpu.VMEM((TA, half), F32),
                pltpu.VMEM((TA, half), F32),
                pltpu.VMEM((tok - TA, half), F32),
                pltpu.VMEM((tok - TA, half), F32),
                dma((9,)),
                dma((N // GROUP,)),
                dma((2,)),
                dma((RING,)),
                dma((NA + 5,)),
                dma((NA + 5,)),
                dma((NB + NB // 2,)),
                dma((NC + 5,)),
                dma((2,)),
                dma((2,)),
            ],
            compiler_params=pltpu.CompilerParams(
                collective_id=0, has_side_effects=True, vmem_limit_bytes=66_500_000
            ),
        )(x_blk, gain_blk, w_in_blk, w_out_blk)

    return jax.shard_map(
        body,
        mesh=mesh,
        in_specs=(P(("dp", "row"), "col"), P("col"), P("row", "col"), P("row", "col")),
        out_specs=P(("dp", "row"), "col"),
        check_vma=False,
    )
```

```python
import jax
import jax.numpy as jnp
from jax import lax
from jax.experimental import pallas as pl
from jax.experimental.pallas import tpu as pltpu
from jax.sharding import PartitionSpec as P

NORM_EPS = 1e-5
MESH = pl.DeviceIdType.MESH
WHOLE, FIRST = -1, 0
F32 = jnp.float32
BF16 = jnp.bfloat16

C = 256
NB = 4
NC = 5
NA = 11
N = NA + NB + NC
NF = 4
EARLY = 6
GROUP = 10
LAG = 3
RING = 10
TA = 16


def kernel(x_hbm, gain_hbm, w_in_hbm, w_out_hbm, out_v,
           xa_v, xb_v, gain_v, stat_g, x_ga, x_gb, x_relay, z_v, w_in_v, w_out_v, d_send, d_recv, own, x_recv, c_recv, hall,
           acc, ea_recv, eb_recv, fa_send, fa_recv, fb_send, fb_recv,
           misc_sem, w_in_sem, send_sem, d_rsem, x_rsem, y_rsem, b_rsem, c_rsem, e_rsem, f_rsem):
    w_out_sem, stat_rsem, za_rsem, zb_rsem = [misc_sem.at[i] for i in range(4, 8)]
    stat_ssem = z_ssem = d_ssem = x_ssem = y_ssem = b_ssem = c_ssem = e_ssem = send_sem.at[0]
    f_ssem = send_sem.at[1]
    y = lax.axis_index("col")
    row = lax.axis_index("row")
    x = row // 2
    k = row % 2
    dp = lax.axis_index("dp")
    home = 1 - (x + y) % 2
    tok, half = out_v.shape
    feat = half // 2
    block = N * C
    rows_a = 4 * TA
    tb = tok - TA
    rows_b = 4 * tb
    sibling = (dp, y, 2 * x + 1 - k)
    x_next = (dp, y, 2 * (1 - x) + k)
    y_next = (dp, 1 - y, row)

    def remote(src, dst, ssem, rsem, dev):
        return pltpu.make_async_remote_copy(src_ref=src, dst_ref=dst, send_sem=ssem, recv_sem=rsem,
                                            device_id=dev, device_id_type=MESH)

    c0, a0 = NB, NB + NC

    def chunk_of(p):
        u = p - 2 * NB - 1
        pair = jnp.where(p % 2 == 1, c0 + p // 2, p // 2 + (1 - home) * a0)
        mixed = jnp.where(u % 2 == 1, u // 2, a0 + NB + u // 2)
        late = jnp.where((home == 1) | (u >= 2 * NB), a0 + u, mixed)
        return jnp.where(p < 2 * NB, pair, jnp.where(u < 0, a0 - 1, late))

    def w_in_copies(p):
        c = C * chunk_of(p)
        cs = pl.multiple_of((1 - k) * block + c, C)
        co = pl.multiple_of(k * block + c, C)
        return (pltpu.make_async_copy(w_in_hbm.at[:, pl.ds(cs, C)], w_in_v.at[p, :, pl.ds(0, C)], w_in_sem.at[p // GROUP]),
                pltpu.make_async_copy(w_in_hbm.at[:, pl.ds(co, C)], w_in_v.at[p, :, pl.ds(C, C)], w_in_sem.at[p // GROUP]))

    def w_out_copy(i):
        r = pl.multiple_of(i * C, C)
        return pltpu.make_async_copy(w_out_hbm.at[pl.ds(r, C), :], w_out_v.at[i], w_out_sem)

    xa_copy = pltpu.make_async_copy(x_hbm.at[pl.ds(0, TA)], xa_v, misc_sem.at[0])
    xb_copy = pltpu.make_async_copy(x_hbm.at[pl.ds(TA, tb)], xb_v, misc_sem.at[8])
    g_copy = pltpu.make_async_copy(gain_hbm, gain_v.at[0], misc_sem.at[1])
    xa_copy.start()
    xb_copy.start()
    g_copy.start()

    barrier = pltpu.get_barrier_semaphore()
    for dy in range(2):
        for dr in range(4):
            if dy or dr:
                pl.semaphore_signal(barrier, inc=1, device_id=(dp, (y + dy) % 2, (row + dr) % 4), device_id_type=MESH)

    def start_w_in(p, _):
        for cp in w_in_copies(p):
            cp.start()
        return 0

    lax.fori_loop(0, N, start_w_in, 0)

    xa_copy.wait()
    xb_copy.wait()
    g_copy.wait()

    def row_sums(ref):
        v = ref[...].astype(F32)
        lane = lax.broadcasted_iota(jnp.int32, (v.shape[0], 128), 1)
        return jnp.where(lane == 0, jnp.sum(v, axis=1, keepdims=True), jnp.sum(v * v, axis=1, keepdims=True))

    me = 4 * y + row
    stat_g[me, :, :tok] = jnp.transpose(jnp.concatenate([row_sums(xa_v), row_sums(xb_v)], axis=0))[:2]
    with jax.named_scope('barrier'):
        pl.semaphore_wait(barrier, 7)

    def tok_copy(group, dy, dk):
        tk = (k + dk) % 2
        cols = pl.ds(pl.multiple_of(feat * tk, 128), feat)
        src, dst, sem = ((xa_v, x_ga, za_rsem), (xb_v, x_gb, zb_rsem))[group]
        return remote(src.at[:, cols], dst.at[row], z_ssem, sem, (dp, (y + dy) % 2, 2 * y + tk))

    def stat_copy(d):
        ty = (y + d // 4) % 2
        tr = (row + d % 4) % 4
        return remote(stat_g.at[me], stat_g.at[me], stat_ssem, stat_rsem, (dp, ty, tr))

    gain_cp = remote(gain_v.at[0], gain_v.at[1], z_ssem, misc_sem.at[3], y_next)
    half_cols = pl.ds(pl.multiple_of(feat * (1 - k), 128), feat)
    to_relay = remote(xa_v.at[:, half_cols], x_relay, z_ssem, misc_sem.at[2], y_next)
    from_relay = remote(x_relay, x_ga.at[row], z_ssem, za_rsem, (dp, y, 2 * (1 - x) + 1 - k))

    for d in range(1, 8):
        stat_copy(d).start()

    @pl.when(home == 0)
    def _():
        to_relay.start()
        tok_copy(1, 1, 0).start()
        tok_copy(1, 1, 1).start()
        tok_copy(1, 0, 0).start()
        tok_copy(1, 0, 1).start()
        tok_copy(0, 1, 0).start()
        tok_copy(0, 0, 0).start()
        tok_copy(0, 0, 1).start()

    @pl.when(home == 1)
    def _():
        gain_cp.start()
        for group in (1, 0):
            tok_copy(group, 0, 1).start()
            tok_copy(group, 1, 0).start()
            tok_copy(group, 1, 1).start()
        x_ga[row] = jnp.where(k == 0, xa_v[:, :feat], xa_v[:, feat:])
        x_gb[row] = jnp.where(k == 0, xb_v[:, :feat], xb_v[:, feat:])
        gain_v[1] = gain_v[0]
        with jax.named_scope('x_relay_wait'):
            to_relay.wait_recv()
        from_relay.start()

    @pl.when(home == 0)
    def _():
        with jax.named_scope('gain_wait'):
            gain_cp.wait_recv()
    gain = jnp.where(k == 0, gain_v[1, :feat], gain_v[1, feat:]).reshape(1, feat)
    acc[...] = jnp.zeros_like(acc)
    with jax.named_scope('stat_wait'):
        remote(stat_g.at[pl.ds(0, 7)], stat_g.at[pl.ds(0, 7)], stat_ssem, stat_rsem, y_next).wait_recv()

    def make_z(group):
        ref, sem = ((x_ga, za_rsem), (x_gb, zb_rsem))[group]

        @pl.when(home == 0)
        def _():
            with jax.named_scope('z_wait'):
                remote(ref, ref, z_ssem, sem, y_next).wait_recv()

        @pl.when(home == 1)
        def _():
            with jax.named_scope('z_wait'):
                remote(ref.at[pl.ds(0, 3)], ref.at[pl.ds(0, 3)], z_ssem, sem, y_next).wait_recv()

        t0, n, base = ((0, TA, 0), (TA, tb, rows_a))[group]
        for src in range(4):
            both = stat_g[src] + stat_g[4 + src]
            st = jnp.transpose(jnp.concatenate([both] * 4, axis=0))[t0:t0 + n] * (1.0 / (2 * half))
            mean = st[:, 0:1]
            var = st[:, 1:2] - mean * mean
            z = (ref[src].astype(F32) - mean) * lax.rsqrt(var + NORM_EPS) * gain
            z_v[pl.ds(base + n * src, n), :] = z.astype(BF16)

    row_group = (pl.ds(0, rows_a), pl.ds(rows_a, rows_b))

    def part_of(ref, j, part):
        if part == WHOLE:
            return ref.at[j]
        if part == FIRST:
            return ref.at[j, row_group[0]]
        return ref.at[pl.ds(j, part), row_group[1]]

    def rows_of(part):
        return pl.ds(0, rows_a + rows_b) if part == WHOLE else row_group[int(part > 0)]

    def d_copy(p, part, seq):
        return remote(part_of(d_send, p, part), part_of(d_recv, p, part), d_ssem, d_rsem.at[seq % RING], sibling)

    def b_index(j, part):
        return 9 + j // 2 if part == 2 else j + 6

    def x_group(j, part, first, sem):
        return remote(part_of(own, first + j, part), part_of(x_recv, j, part), x_ssem, x_rsem.at[sem], x_next)

    def x_copy_of(j, part, first):
        sem = x_rsem.at[b_index(j, part)] if part > 0 else x_rsem.at[j]
        return remote(part_of(own, first + j, part), part_of(x_recv, j, part), x_ssem, sem, x_next)

    def c_copy(j):
        return c_part(j, WHOLE)

    def c_part(j, part):
        return remote(part_of(own, c0 + j, part), part_of(c_recv.at[0], j, part), c_ssem, c_rsem.at[home * NC + (1 - home) * j], y_next)

    def c_relay(j, part):
        sem = c_rsem.at[NC + 1 + j // 3] if part > 0 else c_rsem.at[j]
        return remote(part_of(c_recv.at[0], j, part), part_of(c_recv.at[1], j, part), c_ssem, sem, x_next)

    last = NA - 1

    def both_home():
        return remote(part_of(own, a0 + last, 1), part_of(c_recv.at[0], NC, 1), c_ssem, c_rsem.at[NC + 3], y_next)

    def both_far():
        return remote(part_of(own, a0 + last, 1), part_of(c_recv.at[1], NC, 1), c_ssem, c_rsem.at[NC + 4],
                      (dp, 1 - y, 2 * (1 - x) + k))

    def pass_c(j):
        with jax.named_scope('c_wait'):
            remote(c_recv.at[0, j], c_recv.at[0, j], c_ssem, c_rsem.at[j], y_next).wait_recv()
        c_relay(j, FIRST).start()

    def up(p, part, seq):
        rows = rows_of(part)
        sums = jnp.dot(z_v[rows, :], w_in_v[p], preferred_element_type=F32)
        d_send[p, rows, :] = sums[:, :C]
        own[chunk_of(p), rows, :] = sums[:, C:]
        d_copy(p, part, seq).start()

    def pair_add(p, part, seq):
        with jax.named_scope('pair_wait'):
            d_copy(p, part, seq).wait_recv()
        q, rows = chunk_of(p), rows_of(part)
        own[q, rows, :] = own[q, rows, :] + d_recv[p, rows, :]

    def wait_w_in(p):
        with jax.named_scope('w_in_wait'):
            group = w_in_v.at[pl.ds(p, GROUP)]
            pltpu.make_async_copy(group, group, w_in_sem.at[p // GROUP]).wait()

    def pair_group(p, part, seq):
        pair_add(p, part, seq)
        q = chunk_of(p)

        @pl.when((q >= c0) & (q < a0))
        def _():
            c_part(q - c0, part).start()

        @pl.when((home == 1) & (q < c0))
        def _():
            x_group(q, part, 0, 9 + q // 2 if part else q).start()

        @pl.when((home == 0) & (q >= a0))
        def _():
            x_group(q - a0, part, a0, q - a0).start()

    def pair_sum(p):
        pair_add(p, WHOLE, p + EARLY)
        q = chunk_of(p)

        @pl.when((q >= c0) & (q < a0))
        def _():
            c_copy(q - c0).start()

        @pl.when((home == 1) & (q < c0))
        def _():
            x_copy_of(q, FIRST, 0).start()

            x_group(q, 1, 0, 9 + q // 2).start()

        @pl.when((home == 0) & (q >= a0 + NF))
        def _():
            x_copy_of(q - a0, FIRST, a0).start()

        @pl.when((home == 0) & (q >= a0) & (q < a0 + NF))
        def _():
            x_copy_of(q - a0, WHOLE, a0).start()

    def up_loop(lo, hi, part, seq, then):
        def step(p, _):
            if part != FIRST:
                @pl.when(p % GROUP == 0)
                def _():
                    wait_w_in(p)
            up(p, part, p + seq)
            if part != 1:
                w_out_copy(p).start()
            then(p)
            return 0

        lax.fori_loop(lo, hi, step, 0)

    def late(p):
        pair_sum(p - LAG)

        @pl.when((p == 17) & (home == 1))
        def _():
            pass_c(0)

    def flush(p):
        for i in range(2):
            pair_group(2 * p + 2 + i, 1, 2 * p + 2 + i)

    make_z(1)
    up_loop(0, 4, 1, 0, lambda p: None)
    up_loop(4, EARLY, 1, 0, lambda p: pair_group(p - 4, 1, p - 4))
    make_z(0)
    up_loop(0, 2, FIRST, EARLY, flush)
    up_loop(2, LAG, FIRST, EARLY, lambda p: None)
    up_loop(LAG, EARLY, FIRST, EARLY, lambda p: pair_group(p - LAG, FIRST, p - LAG + EARLY))
    up_loop(EARLY, EARLY + LAG, WHOLE, EARLY, lambda p: pair_group(p - LAG, FIRST, p - LAG + EARLY))
    up_loop(EARLY + LAG, N, WHOLE, EARLY, late)
    for p in range(N - LAG, N):
        pair_sum(p)

    @pl.when(home == 0)
    def _():
        x_copy_of(NF, 2, a0).start()
        x_copy_of(NF + 2, 1, a0).start()
        x_copy_of(NF + 3, 1, a0).start()
        x_copy_of(NF + 4, 1, a0).start()
        x_copy_of(NF + 5, 1, a0).start()
        both_far().start()
        x_copy_of(last, 1, a0).start()

    with jax.named_scope('w_out_wait'):
        pltpu.make_async_copy(w_out_v, w_out_v, w_out_sem).wait()

    def y_copy(j, part):
        sem = y_rsem.at[b_index(j, part)] if part > 0 else y_rsem.at[j]
        return remote(part_of(hall, j, part), part_of(hall, NA + j, part), y_ssem, sem, y_next)

    def b_sem(j, part):
        return b_rsem.at[NB + j // 2] if part > 0 else b_rsem.at[j]

    def relay_copy(j, part):
        return remote(part_of(hall, NA + j, part), part_of(hall, 2 * NA + j, part), b_ssem, b_sem(j, part), x_next)

    def back_copy(j, part):
        return remote(part_of(hall, 2 * NA + j, part), part_of(hall, 2 * NA + j, part), b_ssem, b_sem(j, part), y_next)

    def put_h(j, part, left, right):
        rows = rows_of(part)
        for c in range(max(part, 1)):
            total = left(c)[rows, :] + right(c)[rows, :]
            hall[j + c, rows, :] = jax.nn.gelu(total, approximate=True).astype(BF16)

    def make_h(j, part, first, send=True):
        with jax.named_scope('x_wait'):
            x_copy_of(j, part, 0).wait_recv()
        put_h(j, part, lambda c: own.at[first + j + c], lambda c: x_recv.at[j + c])
        if send:
            y_copy(j, part).start()

    def make_h_c(j, part, first=False):
        with jax.named_scope('c_wait'):
            if first:
                own_part = c_recv.at[0, pl.ds(0, NC)]
                remote(own_part, own_part, c_ssem, c_rsem.at[NC], y_next).wait_recv()
            c_relay(j, part).wait_recv()
        put_h(c0 + j, part, lambda c: c_recv.at[0, j + c], lambda c: c_recv.at[1, j + c])
        yc_copy(j, part).start()

    def yc_copy(j, part):
        sem = y_rsem.at[NA + j // 3] if part > 0 else y_rsem.at[c0 + j]
        return remote(part_of(hall, c0 + j, part), part_of(hall, NA + c0 + j, part), y_ssem, sem, y_next)

    def down(slot, i, part):
        rows = rows_of(part)
        parts = [jnp.dot(hall[slot + c, rows, :], w_out_v[i + c], preferred_element_type=F32)
                 for c in range(max(part, 1))]
        acc[rows, :] += sum(parts[1:], parts[0])

    e_recv, f_send, f_recv = (ea_recv, eb_recv), (fa_send, fb_send), (fa_recv, fb_recv)

    def token_rows(group, r):
        n, base = ((TA, 0), (tb, rows_a))[group]
        return pl.ds(pl.multiple_of(base + n * r, 8), n)

    def e_copy(group, s):
        r = 2 * (s * x + (1 - s) * (1 - x)) + 1 - k
        return remote(acc.at[token_rows(group, r)], e_recv[group].at[s], e_ssem, e_rsem.at[group], sibling)

    def f_copy(group):
        return remote(f_send[group], f_recv[group], f_ssem, f_rsem.at[group], x_next)

    def end_start(group):
        e_copy(group, 0).start()
        e_copy(group, 1).start()

    def end_send(group):
        with jax.named_scope('e0_wait'):
            remote(e_recv[group], e_recv[group], e_ssem, e_rsem.at[group], sibling).wait_recv()
        f_send[group][...] = acc[token_rows(group, 2 * (1 - x) + k), :] + e_recv[group][0]
        f_copy(group).start()

    def end_send_from(core):
        @pl.when(k == core)
        def _():
            end_send(0)

    def end_sum(group):
        with jax.named_scope('f_wait'):
            f_copy(group).wait_recv()
        total = acc[token_rows(group, row), :] + e_recv[group][1] + f_recv[group][...]
        t0, n = ((0, TA), (TA, tb))[group]
        out_v[t0:t0 + n, :] = ((xa_v, xb_v)[group][...].astype(F32) + total).astype(BF16)

    def loop(lo, hi, step):
        def body(i, _):
            step(i)
            return 0
        lax.fori_loop(lo, hi, body, 0)

    @pl.when(home == 1)
    def _():
        def relay(i, part):
            with jax.named_scope('relay_wait'):
                y_copy(i, part).wait_recv()
            relay_copy(i, part).start()

        def b_step(i, part):
            with jax.named_scope('b_wait'):
                back_copy(i, part).wait_recv()
            down(2 * NA + i, i, part)

        def c_step(i, part):
            with jax.named_scope('ch_wait'):
                yc_copy(i, part).wait_recv()
            down(NA + c0 + i, c0 + i, part)

        def a_step(j, part):
            make_h(j, part, a0)
            down(j, a0 + j, part)

        pass_c(1)
        both_home().start()

        def step(j):
            @pl.when(j == 2)
            def _():
                pass_c(2)
            a_step(j, WHOLE)

        loop(0, NF, step)

        def step(j):
            for t, i in ((4, 3), (6, 4)):
                @pl.when(j == t)
                def _():
                    pass_c(i)

            @pl.when(j == 7)
            def _():
                relay(0, FIRST)
                relay(1, FIRST)
            a_step(j, FIRST)

        loop(NF, 8, step)
        relay(2, FIRST)
        relay(3, FIRST)
        c_relay(0, 3).start()
        c_relay(3, 2).start()

        def step(t):
            a_step(8 + t, FIRST)

            @pl.when(t == 0)
            def _():
                relay(0, 2)
                relay(2, 2)

            @pl.when(t == 1)
            def _():
                c_step(1, FIRST)
            c_step(2 * t, FIRST)

        loop(0, 2, step)
        a_step(10, FIRST)
        loop(3, 5, lambda i: c_step(i, FIRST))
        a_step(NF, 2)
        loop(0, 2, lambda i: b_step(i, FIRST))
        make_h(NF + 2, 1, a0)
        make_h(NF + 3, 1, a0)
        down(NF + 2, a0 + NF + 2, 2)
        b_step(2, FIRST)
        b_step(NB - 1, FIRST)
        end_start(0)
        make_h(NF + 4, 1, a0)
        make_h(NF + 5, 1, a0)
        end_send_from(0)
        down(NF + 4, a0 + NF + 4, 2)
        c_step(0, 3)
        end_send_from(1)
        make_h(last, 1, a0, send=False)
        down(last, a0 + last, 1)
        c_step(3, 2)
        loop(0, 2, lambda m: b_step(2 * m, 2))

    @pl.when(home == 0)
    def _():
        def a_step(j, part):
            with jax.named_scope('a_wait'):
                y_copy(j, part).wait_recv()
            down(NA + j, a0 + j, part)

        def b_pass(i, part):
            with jax.named_scope('b_wait'):
                relay_copy(i, part).wait_recv()
            back_copy(i, part).start()

        def b_step(i, part):
            b_pass(i, part)
            down(2 * NA + i, i, part)

        def c_step(i, part, first=False):
            make_h_c(i, part, first)
            down(c0 + i, c0 + i, part)

        loop(0, NB, lambda j: make_h(j, FIRST, 0))
        loop(0, NB // 2, lambda m: make_h(2 * m, 2, 0))
        c_step(0, FIRST, first=True)

        def step(t):
            c_step(1 + t, FIRST)
            a_step(t, WHOLE)

        loop(0, NF, step)

        def step(t):
            b_step(t, FIRST)
            a_step(NF + t, FIRST)

        loop(0, 4, step)
        loop(8, 10, lambda j: a_step(j, FIRST))
        c_step(0, 3)
        a_step(10, FIRST)
        end_start(0)
        end_send_from(0)
        c_step(3, 2)
        b_pass(0, 2)
        b_pass(2, 2)
        down(2 * NA, 0, 4)
        a_step(NF, 2)
        end_send_from(1)
        with jax.named_scope('both_wait'):
            both_home().wait_recv()
            both_far().wait_recv()
        put_h(c0 + NC, 1, lambda c: c_recv.at[0, NC + c], lambda c: c_recv.at[1, NC + c])
        down(c0 + NC, a0 + last, 1)
        with jax.named_scope('a_wait'):
            y_copy(NF + 2, 1).wait_recv()
            y_copy(NF + 3, 1).wait_recv()
        down(NA + NF + 2, a0 + NF + 2, 2)
        with jax.named_scope('a_wait'):
            y_copy(NF + 4, 1).wait_recv()
            y_copy(NF + 5, 1).wait_recv()
        down(NA + NF + 4, a0 + NF + 4, 2)

    end_start(1)
    end_send(1)

    def sent(ref, sem):
        remote(ref, ref, sem, sem, y_next).wait_send()

    with jax.named_scope('drain'):
        sent(stat_g.at[pl.ds(0, 7)], stat_ssem)
        sent(d_send, d_ssem)
        sent(hall.at[pl.ds(0, NB)], b_ssem)
        sent(c_recv.at[0, pl.ds(0, NC)], c_ssem)
        sent(part_of(own, 0, 1), c_ssem)
        sent(ea_recv, e_ssem)
        sent(eb_recv, e_ssem)

        @pl.when(home == 0)
        def _():
            sent(x_ga, z_ssem)
            sent(x_gb, z_ssem)
            sent(own.at[pl.ds(0, NA)], x_ssem)
            sent(hall.at[pl.ds(0, NB + NC)], y_ssem)

        @pl.when(home == 1)
        def _():
            gain_cp.wait_send()
            sent(x_ga, z_ssem)
            sent(x_gb.at[pl.ds(0, 3)], z_ssem)
            sent(own.at[pl.ds(0, NB)], x_ssem)
            sent(c_recv.at[1, pl.ds(0, NC)], c_ssem)
            sent(hall.at[pl.ds(0, last)], y_ssem)
            sent(part_of(hall, 0, FIRST), y_ssem)

    end_sum(0)
    end_sum(1)
    sent(fa_send, f_ssem)
    sent(fb_send, f_ssem)


def solution(mesh):
    def body(x_blk, gain_blk, w_in_blk, w_out_blk):
        tok, half = x_blk.shape
        feat = w_in_blk.shape[0]
        tokens = 4 * tok
        dma = pltpu.SemaphoreType.DMA
        return pl.pallas_call(
            kernel,
            out_shape=pltpu.VMEM((tok, half), BF16),
            in_specs=[pl.BlockSpec(memory_space=pl.ANY)] * 4,
            out_specs=pl.BlockSpec(memory_space=pltpu.VMEM),
            scratch_shapes=[
                pltpu.VMEM((TA, half), BF16),
                pltpu.VMEM((tok - TA, half), BF16),
                pltpu.VMEM((2, half), F32),
                pltpu.VMEM((8, 2, 128), F32),
                pltpu.VMEM((4, TA, feat), BF16),
                pltpu.VMEM((4, tok - TA, feat), BF16),
                pltpu.VMEM((TA, feat), BF16),
                pltpu.VMEM((tokens, feat), BF16),
                pltpu.VMEM((N, feat, 2 * C), BF16),
                pltpu.VMEM((N, C, half), BF16),
                pltpu.VMEM((N, tokens, C), F32),
                pltpu.VMEM((N, tokens, C), F32),
                pltpu.VMEM((N, tokens, C), F32),
                pltpu.VMEM((NA, tokens, C), F32),
                pltpu.VMEM((2, NC + 1, tokens, C), F32),
                pltpu.VMEM((2 * NA + NB, tokens, C), BF16),
                pltpu.VMEM((tokens, half), F32),
                pltpu.VMEM((2, TA, half), F32),
                pltpu.VMEM((2, tok - TA, half), F32),
                pltpu.VMEM((TA, half), F32),
                pltpu.VMEM((TA, half), F32),
                pltpu.VMEM((tok - TA, half), F32),
                pltpu.VMEM((tok - TA, half), F32),
                dma((9,)),
                dma((N // GROUP,)),
                dma((2,)),
                dma((RING,)),
                dma((NA + 6,)),
                dma((NA + 6,)),
                dma((NB + NB // 2,)),
                dma((NC + 5,)),
                dma((2,)),
                dma((2,)),
            ],
            compiler_params=pltpu.CompilerParams(
                collective_id=0, has_side_effects=True, vmem_limit_bytes=66_500_000
            ),
        )(x_blk, gain_blk, w_in_blk, w_out_blk)

    return jax.shard_map(
        body,
        mesh=mesh,
        in_specs=(P(("dp", "row"), "col"), P("col"), P("row", "col"), P("row", "col")),
        out_specs=P(("dp", "row"), "col"),
        check_vma=False,
    )
```
